32 devices in a mesh: gx: 8 (over y, x, core), gy: 4 (over z).
Axes of the slice: x: 2, y: 2, z: 4, core: 2. Of those that a mesh axis runs over, the one named last changes fastest.
Arguments:
- fields: float32 [5, 128, 128, 128], P(None, 'gx', 'gy'), may hold values from -6 to 6
- patch_weight: bfloat16 [2560, 512], replicated, may hold values from -0.125 to 0.125
- trainer_of: int32 [2048, 1], P(('gx', 'gy')), may hold values from 0 to 31; in each aligned block of 64 rows (0 to 63, 64 to 127, ...) at most 4 rows name the same one
- lag_index: int32 [16, 16, 16], P('gx', 'gy'), may hold values from 0 to 1
- w_in: bfloat16 [32, 512, 2048], P(('gx', 'gy')), may hold values from -0.25 to 0.25
- b_in: float32 [32, 2048], P(('gx', 'gy')), may hold values from -3 to 3
- w_out: bfloat16 [32, 2048, 512], P(('gx', 'gy')), may hold values from -0.125 to 0.125
- b_out: float32 [32, 512], P(('gx', 'gy')), may hold values from -3 to 3
Outputs:
- new_fields: float32 [5, 128, 128, 128], P(None, 'gx', 'gy')
- patch_gradient: float32 [2560, 512], replicated
- w_in_gradient: float32 [32, 512, 2048], P(('gx', 'gy'))
- b_in_gradient: float32 [32, 2048], P(('gx', 'gy'))
- w_out_gradient: float32 [32, 2048, 512], P(('gx', 'gy'))
- b_out_gradient: float32 [32, 512], P(('gx', 'gy'))
The draws below stay inside these ranges and needn't reach their ends.
Inputs may be any that keep to these rules, and one draw needn't show every extreme that they name: `trainer_of`: among the 64 rows of one brick, no trainer is named more than 4 times.
All inputs are finite; a program needn't handle non-finite values.
Results may differ from the reference program's by a relative error of at most 0.0062.
Values may be sent and summed in bfloat16 or wider, within the bound.
A program may use at most 128 MiB of HBM per device.

```python
import math
import jax
import jax.numpy as jnp
import numpy as np
from jax import lax

FIELDS = 5
PATCH = 8
CX = 16
CY = 32
CZ = 128
STEPS = 3
EMBED = 512
HIDDEN_SIZE = 2048
BLOCK_ROWS = 2
FEAT = 2560
NX = 128
NY = 128
NBLOCK = 64
TRAINERS = 32
SLOTS = 4
ROWS = 4096
N_GX = 8
N_GY = 4
DEVICES = 32


def with_ends(result, key, low, top_value):
    place = [jax.random.randint(jax.random.fold_in(key, axis), (), 0, length) for axis, length in enumerate(result.shape)]
    main_axis = result.shape.index(max(result.shape))
    beside = place[:main_axis] + [(place[main_axis] + 1) % result.shape[main_axis]] + place[main_axis + 1:]
    return result.at[tuple(place)].set(low).at[tuple(beside)].set(top_value)


def levels(rng, dims, pieces, least, high):
    gain, own = 1.0, jax.random.fold_in(rng, 6)
    for dim, parts in pieces:
        heights = jnp.exp(jax.random.uniform(jax.random.fold_in(own, dim), (parts,), jnp.float32, least / len(pieces), high / len(pieces)))
        gain = gain * jnp.repeat(heights, dims[dim] // parts).reshape([-1 if axis == dim else 1 for axis in range(len(dims))])
    return gain


def shared_out(stream_key, own, number, rows, count, top, reach, lean):
    sequence = jax.random.permutation(stream_key, count)
    heavy_load, common = shares(count, rows * top, reach, lean, True), shares(count, rows * top, reach, lean, False)
    places = jnp.arange(count)

    def named(sizes, turn):
        used = int((sizes > 0).sum())
        fixed = max(1, used // 4)
        moved = fixed + (places - fixed + turn * (used - fixed)) % max(1, count - fixed)
        return jnp.zeros((count,), jnp.int32).at[sequence[jnp.where(places < fixed, places, moved)]].set(jnp.asarray(sizes, jnp.int32))

    sizes = jnp.where(number % 4 == 0, named(heavy_load, number // 4), named(common, number - number // 4 - 1))
    mixed = jax.random.permutation(jax.random.fold_in(own, 3), count)
    donor, sink = mixed[0:count // 2 * 2:2], mixed[1:count // 2 * 2:2]
    slack = jnp.minimum(sizes[donor] - 1, reach - sizes[sink]) // 2
    slack = jnp.where((donor == sequence[0]) | (sink == sequence[0]) | (sizes[sink] == 0), 0, jnp.maximum(slack, 0))
    moved = jax.random.randint(jax.random.fold_in(own, 4), (count // 2,), 0, 1 << 20) % (slack + 1)
    sizes = sizes.at[donor].add(-moved).at[sink].add(moved)
    members = jnp.searchsorted(jnp.cumsum(sizes), jnp.arange(rows * top), side="right").astype(jnp.int32)
    listing = members.reshape(top, rows).T
    listing = listing[jax.random.permutation(jax.random.fold_in(own, 1), rows)]
    turn = jax.random.randint(jax.random.fold_in(own, 2), (rows, 1), 0, top)
    return jnp.take_along_axis(listing, (jnp.arange(top)[None, :] + turn) % top, axis=1)


def shares(number_of, total, reach, lean, full):
    portions = [(1 << 20) // math.isqrt(rank ** lean) + 1 for rank in range(1, number_of + 1)]
    largest = reach if full else min(reach, max(-(-total // number_of), total * portions[0] // sum(portions)))
    least = 1 if total - largest >= number_of - 1 else 0
    counts, spare = [largest] + [least] * (number_of - 1), total - largest - least * (number_of - 1)
    while spare > 0:
        movable = [i for i in range(1, number_of) if counts[i] < largest] or [i for i in range(1, number_of) if counts[i] < reach]
        mass, remaining = sum([portions[i] for i in movable]), spare
        for i in movable:
            more = min(reach - counts[i], max(1, remaining * portions[i] // mass), spare)
            counts[i] = counts[i] + more
            spare = spare - more
    return np.array(counts)


def centred(own_key, dims, deviation, most, shards=(), kind=jnp.bfloat16):
    entries = jax.random.normal(own_key, dims, jnp.float32) * deviation
    if len(shards) > 0:
        entries = levels(own_key, dims, shards, -0.22, 0.18) * entries
    return jnp.clip(entries, min=-most, max=most).astype(kind)


def setup_inputs(seed: int = 0) -> dict:
    splits = jax.random.split(jax.random.key(seed), 9)
    fields = centred(splits[0], (FIELDS, NX, NY, CZ), 1.0, 6.0, ((1, 8), (2, 4)), jnp.float32)
    patch_weight = centred(splits[1], (FEAT, EMBED), FEAT ** -0.5, 0.125)
    trainer_of_keys = jax.random.split(jax.random.fold_in(splits[2], 1), (TRAINERS * NBLOCK) // NBLOCK)
    trainer_of_turns = jax.random.permutation(jax.random.fold_in(splits[2], 3), (TRAINERS * NBLOCK) // NBLOCK)
    trainer_of = jax.vmap(lambda own, number: shared_out(jax.random.fold_in(splits[2], 2), own, number, NBLOCK, TRAINERS, 1, SLOTS, 2))(trainer_of_keys, trainer_of_turns).reshape((TRAINERS * NBLOCK, 1))
    lag_index = with_ends(jax.random.randint(splits[3], (NX // PATCH, NY // PATCH, CZ // PATCH), 0, STEPS - 1), jax.random.fold_in(splits[3], 1), 0, (STEPS - 1) - 1).astype(jnp.int32)
    w_in = centred(splits[4], (TRAINERS, EMBED, HIDDEN_SIZE), EMBED ** -0.5, 0.25, ((0, 32),))
    b_in = centred(splits[5], (TRAINERS, HIDDEN_SIZE), 0.5, 3.0, ((0, 32),), jnp.float32)
    w_out = centred(splits[6], (TRAINERS, HIDDEN_SIZE, EMBED), HIDDEN_SIZE ** -0.5, 0.125, ((0, 32),))
    b_out = centred(splits[7], (TRAINERS, EMBED), 0.5, 3.0, ((0, 32),), jnp.float32)
    return {"fields": fields, "patch_weight": patch_weight, "trainer_of": trainer_of, "lag_index": lag_index, "w_in": w_in, "b_in": b_in, "w_out": w_out, "b_out": b_out}


time_step = 0.2
viscosity = 0.5
drift_x = 0.6
drift_y = -0.4
drift_z = 0.3
error_weight = 0.0625


def shifted(padded, dimension, offset):
    window = [slice(None)]
    for other in (1, 2, 3):
        window.append(slice(2, padded.shape[other] - 2))
    window[dimension] = slice(2 + offset, padded.shape[dimension] - 2 + offset)
    return padded[tuple(window)]


def tendency(padded):
    gradients = []
    laplacian = 0.0
    for dimension in (1, 2, 3):
        back_two = shifted(padded, dimension, -2)
        back_one = shifted(padded, dimension, -1)
        middle = shifted(padded, dimension, 0)
        ahead_one = shifted(padded, dimension, 1)
        ahead_two = shifted(padded, dimension, 2)
        gradients.append((back_two - 8.0 * back_one + 8.0 * ahead_one - ahead_two) / 12.0)
        laplacian = laplacian + (-back_two + 16.0 * back_one - 30.0 * middle + 16.0 * ahead_one - ahead_two) / 12.0
    carried = drift_x * gradients[0] + drift_y * gradients[1] + drift_z * gradients[2]
    divergence = gradients[0][1] + gradients[1][2] + gradients[2][3]
    acoustic = jnp.stack([divergence, gradients[0][4], gradients[1][4], gradients[2][4], divergence])
    return viscosity * laplacian - carried - acoustic


def contract_rows(left, right):
    return lax.dot_general(left, right, (((0,), (0,)), ((), ())), preferred_element_type=jnp.float32)


def contract_cols(left, right):
    return lax.dot_general(left, right, (((1,), (1,)), ((), ())), preferred_element_type=jnp.float32)


def trainer_step(source, target, valid, w_first, b_first, w_second, b_second):
    pre = jnp.dot(source, w_first, preferred_element_type=jnp.float32) + b_first
    hidden = jax.nn.silu(pre).astype(jnp.bfloat16)
    predict = jnp.dot(hidden, w_second, preferred_element_type=jnp.float32) + b_second
    error = (error_weight * (predict - target.astype(jnp.float32)) * valid).astype(jnp.bfloat16)
    b_second_grad = jnp.sum(error.astype(jnp.float32), axis=0)
    w_second_grad = contract_rows(hidden, error)
    back = contract_cols(error, w_second)
    sigma = jax.nn.sigmoid(pre)
    pre_grad = (back * sigma * (1.0 + pre * (1.0 - sigma))).astype(jnp.bfloat16)
    b_first_grad = jnp.sum(pre_grad.astype(jnp.float32), axis=0)
    w_first_grad = contract_rows(source, pre_grad)
    source_grad = contract_cols(pre_grad, w_first).astype(jnp.bfloat16)
    return source_grad, w_first_grad, b_first_grad, w_second_grad, b_second_grad


def patchify(state):
    shaped = state.reshape(FIELDS, N_GX, CX // PATCH, PATCH, N_GY, CY // PATCH, PATCH, CZ // PATCH, PATCH)
    return shaped.transpose(1, 4, 2, 5, 7, 0, 3, 6, 8).reshape(ROWS, FEAT)


def one_trainer(operands):
    return trainer_step(*operands)


def reference(fields, patch_weight, trainer_of, lag_index, w_in, b_in, w_out, b_out):
    current = fields
    states = []
    for counter in range(STEPS):
        padded = jnp.pad(current, ((0, 0), (2, 2), (2, 2), (2, 2)))
        current = current + time_step * tendency(padded)
        states.append(current)
    lag_rows = lag_index.reshape(N_GX, CX // PATCH, N_GY, CY // PATCH, CZ // PATCH)
    lag_rows = lag_rows.transpose(0, 2, 1, 3, 4).reshape(ROWS, 1)
    picked = patchify(states[0].astype(jnp.bfloat16))
    for counter in range(1, STEPS - 1):
        picked = jnp.where(lag_rows == counter, patchify(states[counter].astype(jnp.bfloat16)), picked)
    source = jnp.dot(picked, patch_weight, preferred_element_type=jnp.float32).astype(jnp.bfloat16)
    target = jnp.dot(patchify(current.astype(jnp.bfloat16)), patch_weight,
                     preferred_element_type=jnp.float32).astype(jnp.bfloat16)
    owners = trainer_of[:, 0].reshape(DEVICES, NBLOCK)
    onehot = (owners[:, :, None] == jnp.arange(TRAINERS, dtype=jnp.int32)[None, None, :]).astype(jnp.int32)
    within_rank = jnp.sum((jnp.cumsum(onehot, axis=1) - onehot) * onehot, axis=2)
    senders = jnp.arange(DEVICES, dtype=jnp.int32)[:, None]
    slot_block = (owners * DEVICES + senders) * SLOTS + within_rank
    slot_row = (slot_block[:, :, None] * BLOCK_ROWS + jnp.arange(BLOCK_ROWS, dtype=jnp.int32)[None, None, :])
    slot_row = slot_row.reshape(ROWS).astype(jnp.int32)
    capacity = TRAINERS * DEVICES * SLOTS * BLOCK_ROWS
    per_trainer = DEVICES * SLOTS * BLOCK_ROWS
    packed_source = jnp.zeros((capacity, EMBED), source.dtype).at[slot_row].set(source)
    packed_target = jnp.zeros((capacity, EMBED), target.dtype).at[slot_row].set(target)
    packed_valid = jnp.zeros((capacity, 1), jnp.float32).at[slot_row].set(1.0)
    results = lax.map(one_trainer, (packed_source.reshape(TRAINERS, per_trainer, EMBED),
                                    packed_target.reshape(TRAINERS, per_trainer, EMBED),
                                    packed_valid.reshape(TRAINERS, per_trainer, 1),
                                    w_in, b_in, w_out, b_out))
    source_grad = results[0].reshape(capacity, EMBED)[slot_row]
    patch_gradient = contract_rows(picked, source_grad)
    return current, patch_gradient, results[1], results[2], results[3], results[4]
```

```python
import functools

import jax
import jax.numpy as jnp
from jax import lax
from jax.experimental import pallas as pl
from jax.experimental.pallas import tpu as pltpu
from jax.sharding import PartitionSpec as P

FIELDS = 5
PATCH = 8
STEPS = 3
EMBED = 512
BLOCK_ROWS = 2


time_step = 0.2
viscosity = 0.5
drift_x = 0.6
drift_y = -0.4
drift_z = 0.3
error_weight = 0.0625


def with_halo(cells, sides, width):
    for axis, dim in sides:
        count = lax.axis_size(axis)
        ends = count - 1
        head = lax.slice_in_dim(cells, 0, width, axis=dim)
        tail = lax.slice_in_dim(cells, cells.shape[dim] - width, cells.shape[dim], axis=dim)
        cells = jnp.concatenate(
            [
                lax.ppermute(tail, axis, [(i, (i + 1) % count) for i in range(ends)]),
                cells,
                lax.ppermute(head, axis, [((i + 1) % count, i) for i in range(ends)]),
            ],
            axis=dim,
        )
    return cells


def shifted(padded, dimension, offset):
    window = [slice(None)]
    for other in (1, 2, 3):
        window.append(slice(2, padded.shape[other] - 2))
    window[dimension] = slice(2 + offset, padded.shape[dimension] - 2 + offset)
    return padded[tuple(window)]


def tendency(padded):
    gradients = []
    laplacian = 0.0
    for dimension in (1, 2, 3):
        back_two = shifted(padded, dimension, -2)
        back_one = shifted(padded, dimension, -1)
        middle = shifted(padded, dimension, 0)
        ahead_one = shifted(padded, dimension, 1)
        ahead_two = shifted(padded, dimension, 2)
        gradients.append((back_two - 8.0 * back_one + 8.0 * ahead_one - ahead_two) / 12.0)
        laplacian = (
            laplacian
            + (-back_two + 16.0 * back_one - 30.0 * middle + 16.0 * ahead_one - ahead_two) / 12.0
        )
    carried = drift_x * gradients[0] + drift_y * gradients[1] + drift_z * gradients[2]
    divergence = gradients[0][1] + gradients[1][2] + gradients[2][3]
    acoustic = jnp.stack(
        [divergence, gradients[0][4], gradients[1][4], gradients[2][4], divergence]
    )
    return viscosity * laplacian - carried - acoustic


def contract_rows(left, right):
    return lax.dot_general(
        left, right, (((0,), (0,)), ((), ())), preferred_element_type=jnp.float32
    )


def contract_cols(left, right):
    return lax.dot_general(
        left, right, (((1,), (1,)), ((), ())), preferred_element_type=jnp.float32
    )


def trainer_step(source, target, valid, w_first, b_first, w_second, b_second):
    pre = jnp.dot(source, w_first, preferred_element_type=jnp.float32) + b_first
    hidden = jax.nn.silu(pre).astype(jnp.bfloat16)
    predict = jnp.dot(hidden, w_second, preferred_element_type=jnp.float32) + b_second
    error = (error_weight * (predict - target.astype(jnp.float32)) * valid).astype(jnp.bfloat16)
    b_second_grad = jnp.sum(error.astype(jnp.float32), axis=0)
    w_second_grad = contract_rows(hidden, error)
    back = contract_cols(error, w_second)
    sigma = jax.nn.sigmoid(pre)
    pre_grad = (back * sigma * (1.0 + pre * (1.0 - sigma))).astype(jnp.bfloat16)
    b_first_grad = jnp.sum(pre_grad.astype(jnp.float32), axis=0)
    w_first_grad = contract_rows(source, pre_grad)
    source_grad = contract_cols(pre_grad, w_first).astype(jnp.bfloat16)
    return (source_grad, w_first_grad, b_first_grad, w_second_grad, b_second_grad)


def patch_kernel(cells_ref, rows_ref, *turned):
    count, inner, lanes = rows_ref.shape[0], cells_ref.shape[1], turned[0].shape[1]
    for part, piece in enumerate(turned):
        cells = cells_ref[0, part * lanes : min(inner, (part + 1) * lanes), :]
        if cells.shape[0] < lanes:
            cells = jnp.concatenate(
                [cells, jnp.zeros((lanes - cells.shape[0], cells.shape[1]), cells.dtype)], axis=0
            )
        piece[...] = cells.T
    parts = []
    for offset in range(PATCH):
        for part, piece in enumerate(turned):
            rows = piece[pl.ds(offset, count, stride=PATCH), :]
            parts.append(rows[:, : min(lanes, inner - part * lanes)])
    rows_ref[...] = jnp.concatenate(parts, axis=1).astype(rows_ref.dtype)


def patchify(state):
    width_x, width_y, width_z = (state.shape[1], state.shape[2], state.shape[3])
    shaped = state.reshape(FIELDS, width_x // PATCH, PATCH, width_y // PATCH, PATCH, width_z)
    cells = shaped.transpose(1, 3, 0, 2, 4, 5).reshape(-1, FIELDS * PATCH * PATCH, width_z)
    columns, inner = cells.shape[0], cells.shape[1]
    count = width_z // PATCH
    return pl.pallas_call(
        patch_kernel,
        grid=(columns,),
        out_shape=jax.ShapeDtypeStruct((columns * count, inner * PATCH), jnp.bfloat16),
        in_specs=[pl.BlockSpec((1, inner, width_z), lambda i: (i, 0, 0))],
        out_specs=pl.BlockSpec((count, inner * PATCH), lambda i: (i, 0)),
        scratch_shapes=[pltpu.VMEM((width_z, 128), jnp.float32)] * pl.cdiv(inner, 128),
        cost_estimate=pl.CostEstimate(
            flops=8 * cells.size, bytes_accessed=6 * cells.size, transcendentals=0
        ),
    )(cells)


def pick(first, second, lag_index):
    count_x, count_y, count_z = lag_index.shape
    lag = jnp.repeat(lag_index, PATCH, axis=2)
    lag = lag.reshape(1, count_x, 1, count_y, 1, count_z * PATCH)
    shape = (FIELDS, count_x, PATCH, count_y, PATCH, count_z * PATCH)
    return jnp.where(lag == 1, second.reshape(shape), first.reshape(shape)).reshape(first.shape)


def pad_third(current):
    return jnp.pad(current, ((0, 0), (0, 0), (0, 0), (2, 2)))


def advance(fields):
    states = []
    current = fields
    for counter in range(STEPS):
        padded = with_halo(current, (("gx", 1), ("gy", 2)), 2)
        current = current + time_step * tendency(pad_third(padded))
        states.append(current)
    return states


def my_place():
    return lax.axis_index("gx"), lax.axis_index("gy")


def remote(src, dst, send_sem, recv_sem, gx, gy):
    return pltpu.make_async_remote_copy(
        src_ref=src,
        dst_ref=dst,
        send_sem=send_sem,
        recv_sem=recv_sem,
        device_id=(gx, gy),
        device_id_type=pl.DeviceIdType.MESH,
    )


def greet_all(gx_n, gy_n):
    gx, gy = my_place()
    me = gx * gy_n + gy
    devices = gx_n * gy_n
    barrier = pltpu.get_barrier_semaphore()

    def greet(step, carry):
        other = lax.rem(me + step, devices)
        pl.semaphore_signal(
            barrier,
            inc=1,
            device_id=(other // gy_n, lax.rem(other, gy_n)),
            device_id_type=pl.DeviceIdType.MESH,
        )
        return carry

    lax.fori_loop(1, devices, greet, 0)
    pl.semaphore_wait(barrier, devices - 1)


def gradient_kernel(
    gx_n,
    gy_n,
    grad_ref,
    unplace_ref,
    feat_ref,
    out_ref,
    back,
    feats,
    shared,
    parts,
    landed,
    back_send,
    back_recv,
    feat_send,
    feat_recv,
    share_send,
    share_recv,
    part_send,
    part_recv,
    line_send,
    plane_send,
    pair_send,
    out_recv,
):
    gx, gy = my_place()
    me = gx * gy_n + gy
    devices = gx_n * gy_n
    chips = gx_n // 2
    chip, core = gx // 2, lax.rem(gx, 2)
    partner = gx + 1 - 2 * core
    rows, embed = shared.shape[1], shared.shape[2]

    def chip_at(step):
        return lax.rem(chip + step, chips) * 2 + core

    greet_all(gx_n, gy_n)

    def back_copy(step):
        other = lax.rem(me + step, devices)
        return remote(
            grad_ref.at[other],
            back.at[me],
            back_send.at[step],
            back_recv.at[step],
            other // gy_n,
            lax.rem(other, gy_n),
        )

    def start_back(step, carry):
        back_copy(step).start()
        return carry

    lax.fori_loop(1, devices, start_back, 0)

    def feat_copy(step):
        other = lax.rem(gx + step, gx_n)
        return remote(
            feat_ref.at[other], feats.at[gx], feat_send.at[step], feat_recv.at[step], other, gy
        )

    for step in range(1, gx_n):
        feat_copy(step).start()
    feats[gx] = feat_ref[gx]
    back[me] = grad_ref[me]

    def wait_back(step, carry):
        back_copy(step).wait()
        return carry

    lax.fori_loop(1, devices, wait_back, 0)
    packed = back[...].astype(jnp.float32).reshape(-1, embed).astype(jnp.bfloat16)
    mine = jnp.dot(unplace_ref[...], packed, preferred_element_type=jnp.float32)
    shared[gx] = mine.astype(jnp.bfloat16)

    def share_copy(origin, target, slot):
        return remote(
            shared.at[origin], shared.at[origin], share_send.at[slot], share_recv.at[origin], target, gy
        )

    share_sends = []
    for step in range(1, chips):
        copy = share_copy(gx, chip_at(step), step)
        copy.start()
        share_sends.append(copy)
    copy = share_copy(gx, partner, 0)
    copy.start()
    share_sends.append(copy)
    for step in range(1, chips):
        origin = chip_at(chips - step)
        share_copy(origin, partner, chips + step).wait_recv()
        copy = share_copy(origin, partner, chips + step)
        copy.start()
        share_sends.append(copy)
    for step in range(chips):
        share_copy(chip_at(step) + 1 - 2 * core, partner, 0).wait_recv()
    for step in range(1, gx_n):
        feat_copy(step).wait()

    def part_of(block):
        total = jnp.zeros((parts.shape[1], embed), jnp.float32)
        for origin in range(gx_n):
            total = total + jnp.dot(
                feats[origin, block], shared[origin], preferred_element_type=jnp.float32
            )
        return total

    def part_copy(step):
        other = lax.rem(gy + step, gy_n)
        return remote(
            parts.at[other], landed.at[step], part_send.at[step], part_recv.at[step], gx, other
        )

    for step in range(1, gy_n):
        other = lax.rem(gy + step, gy_n)
        parts[other] = part_of(other).astype(jnp.bfloat16)
        part_copy(step).start()
    total = part_of(gy)
    for step in range(1, gy_n):
        part_copy(step).wait()
        total = total + landed[step].astype(jnp.float32)
    out_ref[gx, gy] = total.astype(jnp.bfloat16)

    def out_copy(block_x, block_y, send_sem, target_x, target_y):
        block = out_ref.at[block_x, block_y]
        return remote(block, block, send_sem, out_recv.at[block_x, block_y], target_x, target_y)

    sends = []

    def send(*args):
        copy = out_copy(*args)
        copy.start()
        sends.append(copy)

    for step in range(1, gy_n):
        send(gx, gy, line_send.at[step], gx, lax.rem(gy + step, gy_n))
    for line in range(gy_n):
        block_y = lax.rem(gy + line, gy_n)
        if line > 0:
            out_copy(gx, block_y, line_send.at[0], gx, block_y).wait_recv()
        for step in range(1, chips):
            send(gx, block_y, plane_send.at[line, step], chip_at(step), gy)
        send(gx, block_y, pair_send.at[line, 0], partner, gy)
    for line in range(gy_n):
        block_y = lax.rem(gy + line, gy_n)
        for step in range(1, chips):
            block_x = chip_at(step)
            out_copy(block_x, block_y, line_send.at[0], partner, gy).wait_recv()
            send(block_x, block_y, pair_send.at[line, step], partner, gy)
    for line in range(gy_n):
        for step in range(chips):
            block_x = chip_at(step) + 1 - 2 * core
            out_copy(block_x, line, line_send.at[0], partner, gy).wait_recv()
    for copy in share_sends + sends:
        copy.wait_send()


def patch_gradient_sum(grad_slots, unplace, feat):
    gx_n, gy_n = lax.axis_size("gx"), lax.axis_size("gy")
    devices, slot_rows, embed = grad_slots.shape
    rows = unplace.shape[0]
    part_rows = feat.shape[2]
    chips = gx_n // 2
    bf16 = jnp.bfloat16
    dma = pltpu.SemaphoreType.DMA
    whole = pl.BlockSpec(memory_space=pltpu.VMEM)
    return pl.pallas_call(
        functools.partial(gradient_kernel, gx_n, gy_n),
        out_shape=jax.ShapeDtypeStruct((gx_n, gy_n, part_rows, embed), bf16),
        in_specs=[whole] * 3,
        out_specs=whole,
        scratch_shapes=[
            pltpu.VMEM((devices, slot_rows, embed), bf16),
            pltpu.VMEM(feat.shape, bf16),
            pltpu.VMEM((gx_n, rows, embed), bf16),
            pltpu.VMEM((gy_n, part_rows, embed), bf16),
            pltpu.VMEM((gy_n, part_rows, embed), bf16),
            dma((devices,)),
            dma((devices,)),
            dma((gx_n,)),
            dma((gx_n,)),
            dma((2 * chips,)),
            dma((gx_n,)),
            dma((gy_n,)),
            dma((gy_n,)),
            dma((gy_n,)),
            dma((gy_n, chips)),
            dma((gy_n, chips)),
            dma((gx_n, gy_n)),
        ],
        compiler_params=pltpu.CompilerParams(collective_id=1, has_side_effects=True),
    )(grad_slots, unplace, feat)


def per_device(fields, patch_weight, trainer_of, lag_index, w_in, b_in, w_out, b_out):
    states = advance(fields)
    gx_n, gy_n = lax.axis_size("gx"), lax.axis_size("gy")
    devices = gx_n * gy_n
    picked = patchify(pick(states[0], states[1], lag_index))
    embed = patch_weight.shape[1]
    weight = patch_weight.reshape(-1, PATCH, embed).transpose(1, 0, 2).reshape(-1, embed)
    source = jnp.dot(picked, weight, preferred_element_type=jnp.float32).astype(jnp.bfloat16)
    target = jnp.dot(
        patchify(states[-1]), weight, preferred_element_type=jnp.float32
    ).astype(jnp.bfloat16)
    patch_count = picked.shape[0]
    block_count = patch_count // BLOCK_ROWS
    slot_count = max(8 // BLOCK_ROWS, 2 * block_count // devices)
    owners = trainer_of[:, 0]
    onehot = (owners[:, None] == jnp.arange(devices, dtype=jnp.int32)[None, :]).astype(jnp.int32)
    within_rank = jnp.sum((jnp.cumsum(onehot, axis=0) - onehot) * onehot, axis=1)
    block_slot = owners * slot_count + within_rank

    patch_slot = jnp.repeat(block_slot, BLOCK_ROWS) * BLOCK_ROWS
    patch_slot = patch_slot + jnp.arange(patch_count, dtype=jnp.int32) % BLOCK_ROWS
    slot_rows = slot_count * BLOCK_ROWS
    slots = jnp.arange(devices * slot_rows, dtype=jnp.int32)
    place = (slots[:, None] == patch_slot[None, :]).astype(jnp.bfloat16)
    unplace = (patch_slot[:, None] == slots[None, :]).astype(jnp.bfloat16)

    rows = jnp.concatenate([source, target, jnp.ones((patch_count, 128), jnp.bfloat16)], 1)
    packed = jnp.dot(place, rows, preferred_element_type=jnp.float32).astype(jnp.bfloat16)
    packed = packed.reshape(devices, slot_rows, rows.shape[1])
    got = lax.all_to_all(packed, ("gx", "gy"), split_axis=0, concat_axis=0, tiled=True)
    got = got.reshape(devices * slot_rows, rows.shape[1])
    valid_rows = got[:, 2 * embed : 2 * embed + 1].astype(jnp.float32)
    results = trainer_step(
        got[:, :embed], got[:, embed : 2 * embed], valid_rows, w_in[0], b_in[0], w_out[0], b_out[0]
    )
    feat = picked.T.reshape(gx_n, gy_n, -1, patch_count)
    summed = patch_gradient_sum(
        results[0].reshape(devices, slot_rows, embed), unplace, feat
    )
    summed = summed.reshape(PATCH, -1, embed).transpose(1, 0, 2).reshape(-1, embed)
    patch_gradient = summed.astype(jnp.float32)
    return (
        states[-1],
        patch_gradient,
        results[1][None],
        results[2][None],
        results[3][None],
        results[4][None],
    )


def solution(mesh):
    in_specs = (
        P(None, "gx", "gy", None),
        P(),
        P(("gx", "gy"), None),
        P("gx", "gy", None),
        P(("gx", "gy"), None, None),
        P(("gx", "gy"), None),
        P(("gx", "gy"), None, None),
        P(("gx", "gy"), None),
    )
    out_specs = (
        P(None, "gx", "gy", None),
        P(),
        P(("gx", "gy"), None, None),
        P(("gx", "gy"), None),
        P(("gx", "gy"), None, None),
        P(("gx", "gy"), None),
    )
    return jax.shard_map(
        per_device, mesh=mesh, in_specs=in_specs, out_specs=out_specs, check_vma=False
    )
```

```python
import functools

import jax
import jax.numpy as jnp
from jax import lax
from jax.experimental import pallas as pl
from jax.experimental.pallas import tpu as pltpu
from jax.sharding import PartitionSpec as P

FIELDS = 5
PATCH = 8
STEPS = 3
EMBED = 512
BLOCK_ROWS = 2


time_step = 0.2
viscosity = 0.5
drift_x = 0.6
drift_y = -0.4
drift_z = 0.3
error_weight = 0.0625
PAD = 8


def contract_rows(left, right):
    return lax.dot_general(
        left, right, (((0,), (0,)), ((), ())), preferred_element_type=jnp.float32
    )


def contract_cols(left, right):
    return lax.dot_general(
        left, right, (((1,), (1,)), ((), ())), preferred_element_type=jnp.float32
    )


def trainer_step(source, target, valid, w_first, b_first, w_second, b_second):
    pre = jnp.dot(source, w_first, preferred_element_type=jnp.float32) + b_first
    hidden = jax.nn.silu(pre).astype(jnp.bfloat16)
    predict = jnp.dot(hidden, w_second, preferred_element_type=jnp.float32) + b_second
    error = (error_weight * (predict - target.astype(jnp.float32)) * valid).astype(jnp.bfloat16)
    b_second_grad = jnp.sum(error.astype(jnp.float32), axis=0)
    w_second_grad = contract_rows(hidden, error)
    back = contract_cols(error, w_second)
    sigma = jax.nn.sigmoid(pre)
    pre_grad = (back * sigma * (1.0 + pre * (1.0 - sigma))).astype(jnp.bfloat16)
    b_first_grad = jnp.sum(pre_grad.astype(jnp.float32), axis=0)
    w_first_grad = contract_rows(source, pre_grad)
    source_grad = contract_cols(pre_grad, w_first).astype(jnp.bfloat16)
    return (source_grad, w_first_grad, b_first_grad, w_second_grad, b_second_grad)


def my_place():
    return lax.axis_index("gx"), lax.axis_index("gy")


def remote(src, dst, send_sem, recv_sem, gx, gy):
    return pltpu.make_async_remote_copy(
        src_ref=src,
        dst_ref=dst,
        send_sem=send_sem,
        recv_sem=recv_sem,
        device_id=(gx, gy),
        device_id_type=pl.DeviceIdType.MESH,
    )


def greet_all(gx_n, gy_n):
    gx, gy = my_place()
    me = gx * gy_n + gy
    devices = gx_n * gy_n
    barrier = pltpu.get_barrier_semaphore()

    def greet(step, carry):
        other = lax.rem(me + step, devices)
        pl.semaphore_signal(
            barrier,
            inc=1,
            device_id=(other // gy_n, lax.rem(other, gy_n)),
            device_id_type=pl.DeviceIdType.MESH,
        )
        return carry

    lax.fori_loop(1, devices, greet, 0)
    pl.semaphore_wait(barrier, devices - 1)


def gradient_kernel(
    gx_n,
    gy_n,
    grad_ref,
    unplace_ref,
    feat_ref,
    out_ref,
    back,
    feats,
    shared,
    parts,
    landed,
    back_send,
    back_recv,
    feat_send,
    feat_recv,
    share_send,
    share_recv,
    part_send,
    part_recv,
    line_send,
    plane_send,
    pair_send,
    out_recv,
):
    gx, gy = my_place()
    me = gx * gy_n + gy
    devices = gx_n * gy_n
    chips = gx_n // 2
    chip, core = gx // 2, lax.rem(gx, 2)
    partner = gx + 1 - 2 * core
    rows, embed = shared.shape[1], shared.shape[2]

    def chip_at(step):
        return lax.rem(chip + step, chips) * 2 + core

    greet_all(gx_n, gy_n)

    def back_copy(step):
        other = lax.rem(me + step, devices)
        return remote(
            grad_ref.at[other],
            back.at[me],
            back_send.at[step],
            back_recv.at[step],
            other // gy_n,
            lax.rem(other, gy_n),
        )

    def start_back(step, carry):
        back_copy(step).start()
        return carry

    lax.fori_loop(1, devices, start_back, 0)

    def feat_copy(step):
        other = lax.rem(gx + step, gx_n)
        return remote(
            feat_ref.at[other], feats.at[gx], feat_send.at[step], feat_recv.at[step], other, gy
        )

    for step in range(1, gx_n):
        feat_copy(step).start()
    feats[gx] = feat_ref[gx]
    back[me] = grad_ref[me]

    def wait_back(step, carry):
        back_copy(step).wait()
        return carry

    lax.fori_loop(1, devices, wait_back, 0)
    packed = back[...].astype(jnp.float32).reshape(-1, embed).astype(jnp.bfloat16)
    mine = jnp.dot(unplace_ref[...], packed, preferred_element_type=jnp.float32)
    shared[gx] = mine.astype(jnp.bfloat16)

    def share_copy(origin, target, slot):
        return remote(
            shared.at[origin], shared.at[origin], share_send.at[slot], share_recv.at[origin], target, gy
        )

    share_sends = []
    for step in range(1, chips):
        copy = share_copy(gx, chip_at(step), step)
        copy.start()
        share_sends.append(copy)
    copy = share_copy(gx, partner, 0)
    copy.start()
    share_sends.append(copy)
    for step in range(1, chips):
        origin = chip_at(chips - step)
        share_copy(origin, partner, chips + step).wait_recv()
        copy = share_copy(origin, partner, chips + step)
        copy.start()
        share_sends.append(copy)
    for step in range(chips):
        share_copy(chip_at(step) + 1 - 2 * core, partner, 0).wait_recv()
    for step in range(1, gx_n):
        feat_copy(step).wait()

    def part_of(block):
        total = jnp.zeros((parts.shape[1], embed), jnp.float32)
        for origin in range(gx_n):
            total = total + jnp.dot(
                feats[origin, block], shared[origin], preferred_element_type=jnp.float32
            )
        return total

    def part_copy(step):
        other = lax.rem(gy + step, gy_n)
        return remote(
            parts.at[other], landed.at[step], part_send.at[step], part_recv.at[step], gx, other
        )

    for step in range(1, gy_n):
        other = lax.rem(gy + step, gy_n)
        parts[other] = part_of(other).astype(jnp.bfloat16)
        part_copy(step).start()
    total = part_of(gy)
    for step in range(1, gy_n):
        part_copy(step).wait()
        total = total + landed[step].astype(jnp.float32)
    out_ref[gx, gy] = total.astype(jnp.bfloat16)

    def out_copy(block_x, block_y, send_sem, target_x, target_y):
        block = out_ref.at[block_x, block_y]
        return remote(block, block, send_sem, out_recv.at[block_x, block_y], target_x, target_y)

    sends = []

    def send(*args):
        copy = out_copy(*args)
        copy.start()
        sends.append(copy)

    for step in range(1, gy_n):
        send(gx, gy, line_send.at[step], gx, lax.rem(gy + step, gy_n))
    for line in range(gy_n):
        block_y = lax.rem(gy + line, gy_n)
        if line > 0:
            out_copy(gx, block_y, line_send.at[0], gx, block_y).wait_recv()
        for step in range(1, chips):
            send(gx, block_y, plane_send.at[line, step], chip_at(step), gy)
        send(gx, block_y, pair_send.at[line, 0], partner, gy)
    for line in range(gy_n):
        block_y = lax.rem(gy + line, gy_n)
        for step in range(1, chips):
            block_x = chip_at(step)
            out_copy(block_x, block_y, line_send.at[0], partner, gy).wait_recv()
            send(block_x, block_y, pair_send.at[line, step], partner, gy)
    for line in range(gy_n):
        for step in range(chips):
            block_x = chip_at(step) + 1 - 2 * core
            out_copy(block_x, line, line_send.at[0], partner, gy).wait_recv()
    for copy in share_sends + sends:
        copy.wait_send()


def patch_gradient_sum(grad_slots, unplace, feat):
    gx_n, gy_n = lax.axis_size("gx"), lax.axis_size("gy")
    devices, slot_rows, embed = grad_slots.shape
    rows = unplace.shape[0]
    part_rows = feat.shape[2]
    chips = gx_n // 2
    bf16 = jnp.bfloat16
    dma = pltpu.SemaphoreType.DMA
    whole = pl.BlockSpec(memory_space=pltpu.VMEM)
    return pl.pallas_call(
        functools.partial(gradient_kernel, gx_n, gy_n),
        out_shape=jax.ShapeDtypeStruct((gx_n, gy_n, part_rows, embed), bf16),
        in_specs=[whole] * 3,
        out_specs=whole,
        scratch_shapes=[
            pltpu.VMEM((devices, slot_rows, embed), bf16),
            pltpu.VMEM(feat.shape, bf16),
            pltpu.VMEM((gx_n, rows, embed), bf16),
            pltpu.VMEM((gy_n, part_rows, embed), bf16),
            pltpu.VMEM((gy_n, part_rows, embed), bf16),
            dma((devices,)),
            dma((devices,)),
            dma((gx_n,)),
            dma((gx_n,)),
            dma((2 * chips,)),
            dma((gx_n,)),
            dma((gy_n,)),
            dma((gy_n,)),
            dma((gy_n,)),
            dma((gy_n, chips)),
            dma((gy_n, chips)),
            dma((gx_n, gy_n)),
        ],
        compiler_params=pltpu.CompilerParams(collective_id=1, has_side_effects=True),
    )(grad_slots, unplace, feat)


def flow_kernel(
    gx_n,
    gy_n,
    fields_ref,
    mask_ref,
    weight_ref,
    place_ref,
    out_ref,
    source_ref,
    target_ref,
    turned_ref,
    state_0,
    state_1,
    state_2,
    face_out,
    face_in,
    swap,
    cells,
    turned,
    source_out,
    target_out,
    halo_send,
    halo_recv,
    source_send,
    source_recv,
    target_send,
    target_recv,
):
    gx, gy = my_place()
    me = gx * gy_n + gy
    devices = gx_n * gy_n
    states = (state_0, state_1, state_2)
    _, size_x, size_y, size_z = fields_ref.shape
    inner = pl.ds(PAD, size_y)
    columns, embed = mask_ref.shape[0], weight_ref.shape[1]
    slot_rows = source_out.shape[1]
    count_y = size_y // PATCH
    kinds = FIELDS * PATCH * PATCH
    rows = turned.shape[1]
    count_z = size_z // PATCH

    edges = ((gx > 0, 0), (gx < gx_n - 1, 1), (gy > 0, 2), (gy < gy_n - 1, 3))
    for state in states:
        for inside, side in edges:
            @pl.when(jnp.logical_not(inside))
            def _():
                if side < 2:
                    plane = pl.ds(0 if side == 0 else size_x + 2, 2)
                    state[:, plane, inner, :] = jnp.zeros((FIELDS, 2, size_y, size_z), jnp.float32)
                else:
                    strip = pl.ds(0 if side == 2 else PAD + size_y, PAD)
                    state[:, pl.ds(2, size_x), strip, :] = jnp.zeros(
                        (FIELDS, size_x, PAD, size_z), jnp.float32
                    )

    barrier = pltpu.get_barrier_semaphore()

    def greet(step, carry):
        other = lax.rem(me + step, devices)
        pl.semaphore_signal(
            barrier,
            inc=1,
            device_id=(other // gy_n, lax.rem(other, gy_n)),
            device_id_type=pl.DeviceIdType.MESH,
        )
        return carry

    lax.fori_loop(1, devices, greet, 0)
    state_0[:, pl.ds(2, size_x), inner, :] = fields_ref[...]
    place_of = lax.broadcasted_iota(jnp.int32, (size_z, PATCH * rows), 1)
    column_of = lax.rem(place_of, rows) // count_z
    cell_of = column_of * size_z + lax.rem(place_of, count_z) * PATCH + place_of // rows
    for column in range(columns):
        row_of = lax.broadcasted_iota(jnp.int32, (size_z, PATCH * rows), 0) + column * size_z
        swap[pl.ds(column * size_z, size_z), :] = jnp.where(row_of == cell_of, 1.0, 0.0).astype(
            jnp.bfloat16
        )
    pl.semaphore_wait(barrier, devices - 1)

    def halo_copy(step, side):
        state = states[step]
        if side == 0:
            src, dst = state.at[:, pl.ds(2, 2), inner], state.at[:, pl.ds(size_x + 2, 2), inner]
            target = (gx - 1, gy)
        elif side == 1:
            src, dst = state.at[:, pl.ds(size_x, 2), inner], state.at[:, pl.ds(0, 2), inner]
            target = (gx + 1, gy)
        else:
            src, dst = face_out.at[step, side - 2], face_in.at[step, 3 - side]
            target = (gx, gy - 1 if side == 2 else gy + 1)
        return remote(
            src, dst, halo_send.at[step, side], halo_recv.at[step, side ^ 1], *target
        )

    def halo_start(step):
        state = states[step]
        for side in (2, 3):
            first = PAD if side == 2 else PAD + size_y - 2
            face_out[step, side - 2] = state[:, pl.ds(2, size_x), pl.ds(first, 2), :]
        for inside, side in edges:
            @pl.when(inside)
            def _():
                halo_copy(step, side).start()

    def halo_wait(step):
        state = states[step]
        for inside, side in edges:
            @pl.when(inside)
            def _():
                copy = halo_copy(step, side)
                copy.wait_send()
                remote(
                    face_in.at[step, 0] if side > 1 else state.at[:, pl.ds(0, 2), inner],
                    face_in.at[step, 0] if side > 1 else state.at[:, pl.ds(0, 2), inner],
                    halo_send.at[step, side],
                    halo_recv.at[step, side],
                    gx,
                    gy,
                ).wait_recv()
                if side > 1:
                    first = PAD - 2 if side == 2 else PAD + size_y
                    state[:, pl.ds(2, size_x), pl.ds(first, 2), :] = face_in[step, side - 2]

    lane = lax.broadcasted_iota(jnp.int32, (size_y, size_z), 1)

    def advance_state(step):
        state = states[step]

        def plane(i, carry):
            def pieces(field):
                middle = state[field, i + 2, inner, :]
                around = []
                around.append([state[field, i + k, inner, :] for k in (0, 1, 3, 4)])
                around.append(
                    [state[field, i + 2, pl.ds(PAD + k, size_y), :] for k in (-2, -1, 1, 2)]
                )
                around.append(
                    [
                        jnp.where(lane < 2, 0.0, pltpu.roll(middle, 2, 1)),
                        jnp.where(lane < 1, 0.0, pltpu.roll(middle, 1, 1)),
                        jnp.where(lane >= size_z - 1, 0.0, pltpu.roll(middle, size_z - 1, 1)),
                        jnp.where(lane >= size_z - 2, 0.0, pltpu.roll(middle, size_z - 2, 1)),
                    ]
                )
                slopes = [(a - d) + 8.0 * (c - b) for a, b, c, d in around]
                near = sum(b + c for a, b, c, d in around)
                far = sum(a + d for a, b, c, d in around)
                change = viscosity * (16.0 * near - far - 90.0 * middle)
                change = change - (
                    drift_x * slopes[0] + drift_y * slopes[1] + drift_z * slopes[2]
                )
                return middle, slopes, change

            def put(field, value):
                if step < STEPS - 1:
                    states[step + 1][field, i + 2, inner, :] = value
                else:
                    out_ref[field, i] = value

            scale = time_step / 12.0
            middle_p, slopes_p, change_p = pieces(4)
            spread = 0.0
            for axis in range(3):
                middle, slopes, change = pieces(1 + axis)
                spread = spread + slopes[axis]
                put(1 + axis, middle + scale * (change - slopes_p[axis]))
            put(4, middle_p + scale * (change_p - spread))
            middle, slopes, change = pieces(0)
            put(0, middle + scale * (change - spread))
            return carry

        lax.fori_loop(0, size_x, plane, 0)

    def column_cells(state, offset_x, offset_y, column):
        first_x = offset_x + column // count_y * PATCH
        first_y = offset_y + column % count_y * PATCH
        return state[:, pl.ds(first_x, PATCH), pl.ds(first_y, PATCH), :].reshape(kinds, size_z)

    def embed_cells():
        for offset in range(PATCH):
            turned[pl.ds(offset, kinds, stride=PATCH), :] = jnp.dot(
                cells[...],
                swap[:, pl.ds(offset * rows, rows)],
                preferred_element_type=jnp.float32,
            )
        patches = turned[...].astype(jnp.bfloat16)
        return patches, contract_rows(patches, weight_ref[...]).astype(jnp.bfloat16)

    def scatter(step, stage, landing, send_sem, recv_sem):
        other = lax.rem(me + step, devices)
        return remote(
            stage.at[other],
            landing.at[me],
            send_sem.at[step],
            recv_sem.at[step],
            other // gy_n,
            lax.rem(other, gy_n),
        )

    def scatter_start(values, stage, landing, send_sem, recv_sem):
        packed = jnp.dot(place_ref[...], values, preferred_element_type=jnp.float32)
        stage[...] = packed.reshape(stage.shape).astype(jnp.bfloat16)

        def start(step, carry):
            scatter(step, stage, landing, send_sem, recv_sem).start()
            return carry

        lax.fori_loop(1, devices, start, 0)
        landing[me] = stage[me]

    def scatter_wait(*args):
        def wait(step, carry):
            scatter(step, *args).wait()
            return carry

        lax.fori_loop(1, devices, wait, 0)

    halo_start(0)
    halo_wait(0)
    advance_state(0)
    halo_start(1)
    halo_wait(1)
    advance_state(1)
    halo_start(2)
    for column in range(columns):
        first = column_cells(state_1, 2, PAD, column)
        second = column_cells(state_2, 2, PAD, column)
        chosen = jnp.where(mask_ref[pl.ds(column, 1), :] > 0.5, second, first)
        cells[:, pl.ds(column * size_z, size_z)] = chosen.astype(jnp.bfloat16)
    patches, source = embed_cells()
    turned_ref[...] = patches
    source_args = (source_out, source_ref, source_send, source_recv)
    ones = jnp.ones((rows, source_out.shape[2] - embed), jnp.bfloat16)
    scatter_start(jnp.concatenate([source, ones], axis=1), *source_args)
    halo_wait(2)
    advance_state(2)
    for column in range(columns):
        cells[:, pl.ds(column * size_z, size_z)] = column_cells(out_ref, 0, 0, column).astype(
            jnp.bfloat16
        )
    patches, target = embed_cells()
    target_args = (target_out, target_ref, target_send, target_recv)
    scatter_start(target, *target_args)
    scatter_wait(*source_args)
    scatter_wait(*target_args)


def flow(fields, mask, weight, place, slot_rows):
    gx_n, gy_n = lax.axis_size("gx"), lax.axis_size("gy")
    devices = gx_n * gy_n
    fields_n, size_x, size_y, size_z = fields.shape
    features, embed = weight.shape
    rows = place.shape[1]
    bf16, f32 = jnp.bfloat16, jnp.float32
    dma = pltpu.SemaphoreType.DMA
    whole = pl.BlockSpec(memory_space=pltpu.VMEM)
    padded = (fields_n, size_x + 4, size_y + 2 * PAD, size_z)
    faces = (STEPS, 2, fields_n, size_x, 2, size_z)
    source_shape = (devices, slot_rows, embed + 128)
    target_shape = (devices, slot_rows, embed)
    return pl.pallas_call(
        functools.partial(flow_kernel, gx_n, gy_n),
        out_shape=[
            jax.ShapeDtypeStruct(fields.shape, f32),
            jax.ShapeDtypeStruct(source_shape, bf16),
            jax.ShapeDtypeStruct(target_shape, bf16),
            jax.ShapeDtypeStruct((features, rows), bf16),
        ],
        in_specs=[whole] * 4,
        out_specs=[whole] * 4,
        scratch_shapes=[
            pltpu.VMEM(padded, f32),
            pltpu.VMEM(padded, f32),
            pltpu.VMEM(padded, f32),
            pltpu.VMEM(faces, f32),
            pltpu.VMEM(faces, f32),
            pltpu.VMEM((mask.shape[0] * size_z, PATCH * rows), bf16),
            pltpu.VMEM((features // PATCH, mask.shape[0] * size_z), bf16),
            pltpu.VMEM((features, rows), f32),
            pltpu.VMEM(source_shape, bf16),
            pltpu.VMEM(target_shape, bf16),
            dma((STEPS, 4)),
            dma((STEPS, 4)),
            dma((devices,)),
            dma((devices,)),
            dma((devices,)),
            dma((devices,)),
        ],
        compiler_params=pltpu.CompilerParams(
            collective_id=0, has_side_effects=True, vmem_limit_bytes=60 * 1024 * 1024
        ),
    )(fields, mask, weight, place)


def per_device(fields, patch_weight, trainer_of, lag_index, w_in, b_in, w_out, b_out):
    gx_n, gy_n = lax.axis_size("gx"), lax.axis_size("gy")
    devices = gx_n * gy_n
    embed = patch_weight.shape[1]
    patch_count = lag_index.size
    block_count = patch_count // BLOCK_ROWS
    slot_count = max(8 // BLOCK_ROWS, 2 * block_count // devices)
    owners = trainer_of[:, 0]
    onehot = (owners[:, None] == jnp.arange(devices, dtype=jnp.int32)[None, :]).astype(jnp.int32)
    within_rank = jnp.sum((jnp.cumsum(onehot, axis=0) - onehot) * onehot, axis=1)
    block_slot = owners * slot_count + within_rank

    patch_slot = jnp.repeat(block_slot, BLOCK_ROWS) * BLOCK_ROWS
    patch_slot = patch_slot + jnp.arange(patch_count, dtype=jnp.int32) % BLOCK_ROWS
    slot_rows = slot_count * BLOCK_ROWS
    slots = jnp.arange(devices * slot_rows, dtype=jnp.int32)
    place = (slots[:, None] == patch_slot[None, :]).astype(jnp.bfloat16)
    unplace = (patch_slot[:, None] == slots[None, :]).astype(jnp.bfloat16)
    mask = jnp.repeat(lag_index.reshape(-1, lag_index.shape[2]), PATCH, axis=1)
    mask = mask.astype(jnp.float32)

    new_fields, source, target, patches = flow(fields, mask, patch_weight, place, slot_rows)
    source = source.reshape(devices * slot_rows, -1)
    target = target.reshape(devices * slot_rows, -1)
    valid_rows = source[:, embed : embed + 1].astype(jnp.float32)
    results = trainer_step(
        source[:, :embed], target, valid_rows, w_in[0], b_in[0], w_out[0], b_out[0]
    )
    feat = patches.reshape(gx_n, gy_n, -1, patch_count)
    summed = patch_gradient_sum(results[0].reshape(devices, slot_rows, embed), unplace, feat)
    patch_gradient = summed.reshape(-1, embed).astype(jnp.float32)
    return (
        new_fields,
        patch_gradient,
        results[1][None],
        results[2][None],
        results[3][None],
        results[4][None],
    )


def solution(mesh):
    in_specs = (
        P(None, "gx", "gy", None),
        P(),
        P(("gx", "gy"), None),
        P("gx", "gy", None),
        P(("gx", "gy"), None, None),
        P(("gx", "gy"), None),
        P(("gx", "gy"), None, None),
        P(("gx", "gy"), None),
    )
    out_specs = (
        P(None, "gx", "gy", None),
        P(),
        P(("gx", "gy"), None, None),
        P(("gx", "gy"), None),
        P(("gx", "gy"), None, None),
        P(("gx", "gy"), None),
    )
    return jax.shard_map(
        per_device, mesh=mesh, in_specs=in_specs, out_specs=out_specs, check_vma=False
    )
```

```python
import functools

import jax
import jax.numpy as jnp
from jax import lax
from jax.experimental import pallas as pl
from jax.experimental.pallas import tpu as pltpu
from jax.sharding import PartitionSpec as P

FIELDS = 5
PATCH = 8
STEPS = 3
BLOCK_ROWS = 2
PAD = 8
CHUNKS = 2
HIDDEN_TILE = 512


time_step = 0.2
viscosity = 0.5
drift_x = 0.6
drift_y = -0.4
drift_z = 0.3
error_weight = 0.0625


def contract_rows(left, right):
    return lax.dot_general(
        left, right, (((0,), (0,)), ((), ())), preferred_element_type=jnp.float32
    )


def contract_cols(left, right):
    return lax.dot_general(
        left, right, (((1,), (1,)), ((), ())), preferred_element_type=jnp.float32
    )


def my_place():
    return lax.axis_index("gx"), lax.axis_index("gy")


def remote(src, dst, send_sem, recv_sem, gx, gy):
    return pltpu.make_async_remote_copy(
        src_ref=src,
        dst_ref=dst,
        send_sem=send_sem,
        recv_sem=recv_sem,
        device_id=(gx, gy),
        device_id_type=pl.DeviceIdType.MESH,
    )


def step_kernel(
    gx_n,
    gy_n,
    fields_hbm,
    weight_hbm,
    owner_ref,
    lag_ref,
    first_hbm,
    first_bias_ref,
    second_hbm,
    second_bias_ref,
    out_ref,
    summed_ref,
    source_hbm,
    hidden_hbm,
    error_hbm,
    slope_hbm,
    state_0,
    state_1,
    state_2,
    face_out,
    face_in,
    swap,
    cells,
    turned,
    place,
    weight,
    first,
    second,
    source_out,
    source_in,
    target_out,
    target_in,
    feat_out,
    feats,
    source_rows,
    hidden,
    steep,
    error,
    slope,
    grad_out,
    back,
    shared,
    parts,
    landed,
    load_sem,
    save_sem,
    halo_send,
    halo_recv,
    source_send,
    source_recv,
    target_send,
    target_recv,
    feat_send,
    feat_recv,
    back_send,
    back_recv,
    share_send,
    share_recv,
    part_send,
    part_recv,
    line_send,
    plane_send,
    pair_send,
    out_recv,
):
    gx, gy = my_place()
    me = gx * gy_n + gy
    devices = gx_n * gy_n
    chips = gx_n // 2
    chip, core = gx // 2, lax.rem(gx, 2)
    partner = gx + 1 - 2 * core
    states = (state_0, state_1, state_2)
    _, size_x, size_y, size_z = fields_hbm.shape
    inner = pl.ds(PAD, size_y)
    embed = weight.shape[1]
    slot_rows = source_out.shape[1]
    count_x, count_y, count_z = lag_ref.shape
    columns = count_x * count_y
    kinds = FIELDS * PATCH * PATCH
    rows = turned.shape[1]
    hidden_n = hidden.shape[1]
    width = embed // CHUNKS
    f32, bf16 = jnp.float32, jnp.bfloat16

    loads = [
        pltpu.make_async_copy(
            fields_hbm, state_0.at[:, pl.ds(2, size_x), inner, :], load_sem.at[0]
        ),
        pltpu.make_async_copy(weight_hbm, weight, load_sem.at[1]),
        pltpu.make_async_copy(first_hbm.at[0], first, load_sem.at[2]),
        pltpu.make_async_copy(second_hbm.at[0], second, load_sem.at[3]),
    ]
    for load in loads:
        load.start()

    edges = ((gx > 0, 0), (gx < gx_n - 1, 1), (gy > 0, 2), (gy < gy_n - 1, 3))
    for state in states:
        for inside, side in edges:
            @pl.when(jnp.logical_not(inside))
            def _():
                if side < 2:
                    plane = pl.ds(0 if side == 0 else size_x + 2, 2)
                    state[:, plane, inner, :] = jnp.zeros((FIELDS, 2, size_y, size_z), jnp.float32)
                else:
                    strip = pl.ds(0 if side == 2 else PAD + size_y, PAD)
                    state[:, pl.ds(2, size_x), strip, :] = jnp.zeros(
                        (FIELDS, size_x, PAD, size_z), jnp.float32
                    )

    barrier = pltpu.get_barrier_semaphore()

    def greet(step, carry):
        other = lax.rem(me + step, devices)
        pl.semaphore_signal(
            barrier,
            inc=1,
            device_id=(other // gy_n, lax.rem(other, gy_n)),
            device_id_type=pl.DeviceIdType.MESH,
        )
        return carry

    lax.fori_loop(1, devices, greet, 0)
    place_of = lax.broadcasted_iota(jnp.int32, (size_z, PATCH * rows), 1)
    column_of = lax.rem(place_of, rows) // count_z
    cell_of = column_of * size_z + lax.rem(place_of, count_z) * PATCH + place_of // rows
    for column in range(columns):
        row_of = lax.broadcasted_iota(jnp.int32, (size_z, PATCH * rows), 0) + column * size_z
        swap[pl.ds(column * size_z, size_z), :] = jnp.where(row_of == cell_of, 1.0, 0.0).astype(
            jnp.bfloat16
        )

    owner = owner_ref[...].astype(f32)
    blocks = owner.shape[1]
    tall = lax.broadcasted_iota(jnp.int32, (devices, blocks), 0).astype(f32)
    onehot = jnp.where(owner == tall, 1.0, 0.0)
    before = jnp.where(
        lax.broadcasted_iota(jnp.int32, (blocks, blocks), 0)
        < lax.broadcasted_iota(jnp.int32, (blocks, blocks), 1),
        1.0,
        0.0,
    )
    ahead = jnp.dot(onehot.astype(bf16), before.astype(bf16), preferred_element_type=f32)
    rank = jnp.sum(ahead * onehot, axis=0, keepdims=True)
    block_slot = owner * float(slot_rows // BLOCK_ROWS) + rank
    slots = place.shape[0]
    slot_block = lax.broadcasted_iota(jnp.int32, (slots, blocks), 0) // BLOCK_ROWS
    block_place = jnp.where(block_slot == slot_block.astype(f32), 1.0, 0.0)
    spread_rows = jnp.where(
        lax.broadcasted_iota(jnp.int32, (blocks, rows), 1) // BLOCK_ROWS
        == lax.broadcasted_iota(jnp.int32, (blocks, rows), 0),
        1.0,
        0.0,
    )
    row_place = jnp.dot(
        block_place.astype(bf16), spread_rows.astype(bf16), preferred_element_type=f32
    )
    same = lax.rem(lax.broadcasted_iota(jnp.int32, (slots, rows), 0), BLOCK_ROWS) == lax.rem(
        lax.broadcasted_iota(jnp.int32, (slots, rows), 1), BLOCK_ROWS
    )
    place[...] = jnp.where(same, row_place, 0.0).astype(bf16)
    pl.semaphore_wait(barrier, devices - 1)

    def halo_copy(step, side):
        state = states[step]
        if side == 0:
            src, dst = state.at[:, pl.ds(2, 2), inner], state.at[:, pl.ds(size_x + 2, 2), inner]
            target = (gx - 1, gy)
        elif side == 1:
            src, dst = state.at[:, pl.ds(size_x, 2), inner], state.at[:, pl.ds(0, 2), inner]
            target = (gx + 1, gy)
        else:
            src, dst = face_out.at[step, side - 2], face_in.at[step, 3 - side]
            target = (gx, gy - 1 if side == 2 else gy + 1)
        return remote(
            src, dst, halo_send.at[step, side], halo_recv.at[step, side ^ 1], *target
        )

    def halo_start(step):
        state = states[step]
        for side in (2, 3):
            first = PAD if side == 2 else PAD + size_y - 2
            face_out[step, side - 2] = state[:, pl.ds(2, size_x), pl.ds(first, 2), :]
        for inside, side in edges:
            @pl.when(inside)
            def _():
                halo_copy(step, side).start()

    def halo_wait(step):
        state = states[step]
        for inside, side in edges:
            @pl.when(inside)
            def _():
                copy = halo_copy(step, side)
                copy.wait_send()
                remote(
                    face_in.at[step, 0] if side > 1 else state.at[:, pl.ds(0, 2), inner],
                    face_in.at[step, 0] if side > 1 else state.at[:, pl.ds(0, 2), inner],
                    halo_send.at[step, side],
                    halo_recv.at[step, side],
                    gx,
                    gy,
                ).wait_recv()
                if side > 1:
                    first = PAD - 2 if side == 2 else PAD + size_y
                    state[:, pl.ds(2, size_x), pl.ds(first, 2), :] = face_in[step, side - 2]

    lane = lax.broadcasted_iota(jnp.int32, (size_y, size_z), 1)

    def advance_state(step):
        state = states[step]

        def plane(i, carry):
            def pieces(field):
                middle = state[field, i + 2, inner, :]
                around = []
                around.append([state[field, i + k, inner, :] for k in (0, 1, 3, 4)])
                around.append(
                    [state[field, i + 2, pl.ds(PAD + k, size_y), :] for k in (-2, -1, 1, 2)]
                )
                around.append(
                    [
                        jnp.where(lane < 2, 0.0, pltpu.roll(middle, 2, 1)),
                        jnp.where(lane < 1, 0.0, pltpu.roll(middle, 1, 1)),
                        jnp.where(lane >= size_z - 1, 0.0, pltpu.roll(middle, size_z - 1, 1)),
                        jnp.where(lane >= size_z - 2, 0.0, pltpu.roll(middle, size_z - 2, 1)),
                    ]
                )
                slopes = [(a - d) + 8.0 * (c - b) for a, b, c, d in around]
                near = sum(b + c for a, b, c, d in around)
                far = sum(a + d for a, b, c, d in around)
                change = viscosity * (16.0 * near - far - 90.0 * middle)
                change = change - (
                    drift_x * slopes[0] + drift_y * slopes[1] + drift_z * slopes[2]
                )
                return middle, slopes, change

            def put(field, value):
                if step < STEPS - 1:
                    states[step + 1][field, i + 2, inner, :] = value
                else:
                    out_ref[field, i] = value

            scale = time_step / 12.0
            middle_p, slopes_p, change_p = pieces(4)
            spread = 0.0
            for axis in range(3):
                middle, slopes, change = pieces(1 + axis)
                spread = spread + slopes[axis]
                put(1 + axis, middle + scale * (change - slopes_p[axis]))
            put(4, middle_p + scale * (change_p - spread))
            middle, slopes, change = pieces(0)
            put(0, middle + scale * (change - spread))
            return carry

        lax.fori_loop(0, size_x, plane, 0)


    def column_cells(state, offset_x, offset_y, column):
        first_x = offset_x + column // count_y * PATCH
        first_y = offset_y + column % count_y * PATCH
        return state[:, pl.ds(first_x, PATCH), pl.ds(first_y, PATCH), :].reshape(kinds, size_z)

    def turn_cells():
        for offset in range(PATCH):
            turned[pl.ds(offset, kinds, stride=PATCH), :] = jnp.dot(
                cells[...],
                swap[:, pl.ds(offset * rows, rows)],
                preferred_element_type=f32,
            )

    def embed_rows():
        return contract_rows(turned[...].astype(bf16), weight[...]).astype(bf16)

    def scatter(step, stage, landing, send_sem, recv_sem):
        other = lax.rem(me + step, devices)
        return remote(
            stage.at[other],
            landing.at[me],
            send_sem.at[step],
            recv_sem.at[step],
            other // gy_n,
            lax.rem(other, gy_n),
        )

    def scatter_start(stage, landing, *sems):
        def start(step, carry):
            scatter(step, stage, landing, *sems).start()
            return carry

        lax.fori_loop(1, devices, start, 0)
        landing[me] = stage[me]

    def scatter_wait(*args):
        def wait(step, carry):
            scatter(step, *args).wait()
            return carry

        lax.fori_loop(1, devices, wait, 0)

    def put_rows(values, stage):
        packed = jnp.dot(place[...], values, preferred_element_type=f32)
        stage[...] = packed.reshape(stage.shape).astype(bf16)

    loads[0].wait()
    halo_start(0)
    halo_wait(0)
    advance_state(0)
    halo_start(1)
    halo_wait(1)
    advance_state(1)
    halo_start(2)
    stretch = jnp.where(
        lax.broadcasted_iota(jnp.int32, (count_z, size_z), 1) // PATCH
        == lax.broadcasted_iota(jnp.int32, (count_z, size_z), 0),
        1.0,
        0.0,
    ).astype(bf16)
    for column_x in range(count_x):
        lag = lag_ref[column_x].astype(f32).astype(bf16)
        lag = jnp.dot(lag, stretch, preferred_element_type=f32)
        for column_y in range(count_y):
            column = column_x * count_y + column_y
            early = column_cells(state_1, 2, PAD, column)
            late = column_cells(state_2, 2, PAD, column)
            chosen = jnp.where(lag[column_y : column_y + 1, :] > 0.5, late, early)
            cells[:, pl.ds(column * size_z, size_z)] = chosen.astype(bf16)
    turn_cells()
    loads[1].wait()
    source = embed_rows()
    source_args = (source_out, source_in, source_send, source_recv)
    ones = jnp.ones((rows, source_out.shape[2] - embed), bf16)
    put_rows(jnp.concatenate([source, ones], axis=1), source_out)
    scatter_start(*source_args)

    part_rows = feats.shape[2]
    for block in range(devices):
        feat_out[block // gy_n, block % gy_n] = turned[
            pl.ds(block * part_rows, part_rows), :
        ].astype(bf16)

    def feat_copy(step):
        other = lax.rem(gx + step, gx_n)
        return remote(
            feat_out.at[other], feats.at[gx], feat_send.at[step], feat_recv.at[step], other, gy
        )

    for step in range(1, gx_n):
        feat_copy(step).start()
    feats[gx] = feat_out[gx]

    halo_wait(2)
    advance_state(2)
    for column in range(columns):
        cells[:, pl.ds(column * size_z, size_z)] = column_cells(out_ref, 0, 0, column).astype(bf16)
    turn_cells()
    target_args = (target_out, target_in, target_send, target_recv)
    put_rows(embed_rows(), target_out)
    scatter_start(*target_args)

    scatter_wait(*source_args)
    got = source_in[...].astype(f32).reshape(slots, source_in.shape[2])
    source_rows[...] = got[:, :embed].astype(bf16)
    valid = got[:, embed : embed + 1]
    loads[2].wait()
    loads[3].wait()
    predict = jnp.zeros((slots, embed), f32) + second_bias_ref[...]
    for tile in range(0, hidden_n, HIDDEN_TILE):
        part = pl.ds(tile, HIDDEN_TILE)
        pre = jnp.dot(source_rows[...], first[:, part], preferred_element_type=f32)
        pre = pre + first_bias_ref[:, part]
        sigma = jax.nn.sigmoid(pre)
        units = (pre * sigma).astype(bf16)
        hidden[:, part] = units
        steep[:, part] = sigma * (1.0 + pre * (1.0 - sigma))
        predict = predict + jnp.dot(units, second[part, :], preferred_element_type=f32)
    scatter_wait(*target_args)
    wanted = target_in[...].astype(f32).reshape(slots, embed)
    error[...] = (error_weight * (predict - wanted) * valid).astype(bf16)
    for tile in range(0, hidden_n, HIDDEN_TILE):
        part = pl.ds(tile, HIDDEN_TILE)
        slope[:, part] = (contract_cols(error[...], second[part, :]) * steep[:, part]).astype(bf16)
    for chunk in range(CHUNKS):
        grad = contract_cols(slope[...], first[pl.ds(chunk * width, width), :])
        grad_out[chunk] = grad.reshape(devices, slot_rows, width).astype(bf16)
        scatter_start(
            grad_out.at[chunk], back.at[chunk], back_send.at[chunk], back_recv.at[chunk]
        )
    saves = [
        pltpu.make_async_copy(source_rows, source_hbm, save_sem.at[0]),
        pltpu.make_async_copy(hidden, hidden_hbm, save_sem.at[1]),
        pltpu.make_async_copy(error, error_hbm, save_sem.at[2]),
        pltpu.make_async_copy(slope, slope_hbm, save_sem.at[3]),
    ]
    for save in saves:
        save.start()

    def chip_at(step):
        return lax.rem(chip + step, chips) * 2 + core

    sends = []

    def send(copy):
        copy.start()
        sends.append(copy)

    def share_copy(chunk, origin, target, slot):
        block = shared.at[chunk, origin]
        return remote(
            block, block, share_send.at[chunk, slot], share_recv.at[chunk, origin], target, gy
        )

    for chunk in range(CHUNKS):
        scatter_wait(
            grad_out.at[chunk], back.at[chunk], back_send.at[chunk], back_recv.at[chunk]
        )
        packed = back[chunk].astype(f32).reshape(slots, width).astype(bf16)
        mine = contract_rows(place[...], packed)
        shared[chunk, gx] = mine.astype(bf16)
        for step in range(1, chips):
            send(share_copy(chunk, gx, chip_at(step), step))
        send(share_copy(chunk, gx, partner, 0))

    for step in range(1, gx_n):
        feat_copy(step).wait()

    def part_of(chunk, block):
        total = jnp.zeros((part_rows, width), f32)
        for origin in range(gx_n):
            total = total + jnp.dot(
                feats[origin, block], shared[chunk, origin], preferred_element_type=f32
            )
        return total

    def part_copy(chunk, step):
        other = lax.rem(gy + step, gy_n)
        return remote(
            parts.at[chunk, other],
            landed.at[chunk, step],
            part_send.at[chunk, step],
            part_recv.at[chunk, step],
            gx,
            other,
        )

    own = []
    for chunk in range(CHUNKS):
        for step in range(1, chips):
            origin = chip_at(chips - step)
            share_copy(chunk, origin, partner, chips + step).wait_recv()
            send(share_copy(chunk, origin, partner, chips + step))
        for step in range(chips):
            share_copy(chunk, chip_at(step) + 1 - 2 * core, partner, 0).wait_recv()
        for step in range(1, gy_n):
            other = lax.rem(gy + step, gy_n)
            parts[chunk, other] = part_of(chunk, other).astype(bf16)
            part_copy(chunk, step).start()
        own.append(part_of(chunk, gy))

    def out_copy(chunk, block_x, block_y, send_sem, target_x, target_y):
        block = summed_ref.at[chunk, block_x, block_y]
        return remote(
            block, block, send_sem, out_recv.at[chunk, block_x, block_y], target_x, target_y
        )

    def out_wait(chunk, block_x, block_y):
        out_copy(chunk, block_x, block_y, line_send.at[0, 0], partner, gy).wait_recv()

    for chunk in range(CHUNKS):
        total = own[chunk]
        for step in range(1, gy_n):
            part_copy(chunk, step).wait()
            total = total + landed[chunk, step].astype(f32)
        summed_ref[chunk, gx, gy] = total.astype(bf16)
        for step in range(1, gy_n):
            other = lax.rem(gy + step, gy_n)
            send(out_copy(chunk, gx, gy, line_send.at[chunk, step], gx, other))
        for step in range(1, chips):
            send(out_copy(chunk, gx, gy, plane_send.at[chunk, 0, step], chip_at(step), gy))
        send(out_copy(chunk, gx, gy, pair_send.at[chunk, 0, 0], partner, gy))
    for chunk in range(CHUNKS):
        for line in range(1, gy_n):
            block_y = lax.rem(gy + line, gy_n)
            out_wait(chunk, gx, block_y)
            for step in range(1, chips):
                send(
                    out_copy(
                        chunk, gx, block_y, plane_send.at[chunk, line, step], chip_at(step), gy
                    )
                )
            send(out_copy(chunk, gx, block_y, pair_send.at[chunk, line, 0], partner, gy))
    for chunk in range(CHUNKS):
        for line in range(gy_n):
            block_y = lax.rem(gy + line, gy_n)
            for step in range(1, chips):
                block_x = chip_at(step)
                out_wait(chunk, block_x, block_y)
                send(
                    out_copy(
                        chunk, block_x, block_y, pair_send.at[chunk, line, step], partner, gy
                    )
                )
    for chunk in range(CHUNKS):
        for line in range(gy_n):
            for step in range(chips):
                out_wait(chunk, chip_at(step) + 1 - 2 * core, line)
    for copy in sends:
        copy.wait_send()
    for save in saves:
        save.wait()


def finish_kernel(source_ref, hidden_ref, error_ref, slope_ref, summed_ref, *outs):
    first_ref, first_bias_ref, second_ref, second_bias_ref, patch_ref = outs
    error, slope = error_ref[...], slope_ref[...]
    first_ref[0] = contract_rows(source_ref[...], slope)
    first_bias_ref[...] = jnp.sum(slope.astype(jnp.float32), axis=0, keepdims=True)
    second_ref[0] = contract_rows(hidden_ref[...], error)
    second_bias_ref[...] = jnp.sum(error.astype(jnp.float32), axis=0, keepdims=True)
    width = summed_ref.shape[2]
    for chunk in range(summed_ref.shape[0]):
        patch_ref[:, chunk * width : (chunk + 1) * width] = summed_ref[chunk].astype(jnp.float32)


def finish(source, hidden, error, slope, summed):
    slots, embed = source.shape
    hidden_n = hidden.shape[1]
    features, width = summed.shape[1], summed.shape[2]
    steps = hidden_n // HIDDEN_TILE
    f32 = jnp.float32
    return pl.pallas_call(
        finish_kernel,
        grid=(steps,),
        out_shape=[
            jax.ShapeDtypeStruct((1, embed, hidden_n), f32),
            jax.ShapeDtypeStruct((1, hidden_n), f32),
            jax.ShapeDtypeStruct((1, hidden_n, embed), f32),
            jax.ShapeDtypeStruct((1, embed), f32),
            jax.ShapeDtypeStruct((features, embed), f32),
        ],
        in_specs=[
            pl.BlockSpec((slots, embed), lambda i: (0, 0)),
            pl.BlockSpec((slots, HIDDEN_TILE), lambda i: (0, i)),
            pl.BlockSpec((slots, embed), lambda i: (0, 0)),
            pl.BlockSpec((slots, HIDDEN_TILE), lambda i: (0, i)),
            pl.BlockSpec((CHUNKS, features // steps, width), lambda i: (0, i, 0)),
        ],
        out_specs=[
            pl.BlockSpec((1, embed, HIDDEN_TILE), lambda i: (0, 0, i)),
            pl.BlockSpec((1, HIDDEN_TILE), lambda i: (0, i)),
            pl.BlockSpec((1, HIDDEN_TILE, embed), lambda i: (0, i, 0)),
            pl.BlockSpec((1, embed), lambda i: (0, 0)),
            pl.BlockSpec((features // steps, embed), lambda i: (i, 0)),
        ],
    )(source, hidden, error, slope, summed)


def per_device(fields, patch_weight, trainer_of, lag_index, w_in, b_in, w_out, b_out):
    gx_n, gy_n = lax.axis_size("gx"), lax.axis_size("gy")
    devices, chips = gx_n * gy_n, gx_n // 2
    fields_n, size_x, size_y, size_z = fields.shape
    features, embed = patch_weight.shape
    hidden_n = w_in.shape[2]
    rows = lag_index.size
    blocks = rows // BLOCK_ROWS
    slot_rows = max(8, 2 * blocks // devices * BLOCK_ROWS)
    slots = devices * slot_rows
    columns = lag_index.shape[0] * lag_index.shape[1]
    part_rows = features // devices
    width = embed // CHUNKS
    bf16, f32 = jnp.bfloat16, jnp.float32
    dma = pltpu.SemaphoreType.DMA
    vmem = pltpu.VMEM
    whole = pl.BlockSpec(memory_space=pltpu.VMEM)
    anywhere = pl.BlockSpec(memory_space=pl.ANY)
    padded = (fields_n, size_x + 4, size_y + 2 * PAD, size_z)
    faces = (STEPS, 2, fields_n, size_x, 2, size_z)
    source_shape = (devices, slot_rows, embed + 128)
    target_shape = (devices, slot_rows, embed)
    feat_shape = (gx_n, gy_n, part_rows, rows)
    block_shape = (CHUNKS, gx_n, gy_n, part_rows, width)
    new_fields, summed, source, hidden, error, slope = pl.pallas_call(
        functools.partial(step_kernel, gx_n, gy_n),
        out_shape=[
            jax.ShapeDtypeStruct(fields.shape, f32),
            jax.ShapeDtypeStruct(block_shape, bf16),
            jax.ShapeDtypeStruct((slots, embed), bf16),
            jax.ShapeDtypeStruct((slots, hidden_n), bf16),
            jax.ShapeDtypeStruct((slots, embed), bf16),
            jax.ShapeDtypeStruct((slots, hidden_n), bf16),
        ],
        in_specs=[anywhere, anywhere, whole, whole, anywhere, whole, anywhere, whole],
        out_specs=[whole, whole] + [anywhere] * 4,
        scratch_shapes=[
            vmem(padded, f32),
            vmem(padded, f32),
            vmem(padded, f32),
            vmem(faces, f32),
            vmem(faces, f32),
            vmem((columns * size_z, PATCH * rows), bf16),
            vmem((features // PATCH, columns * size_z), bf16),
            vmem((features, rows), f32),
            vmem((slots, rows), bf16),
            vmem((features, embed), bf16),
            vmem((embed, hidden_n), bf16),
            vmem((hidden_n, embed), bf16),
            vmem(source_shape, bf16),
            vmem(source_shape, bf16),
            vmem(target_shape, bf16),
            vmem(target_shape, bf16),
            vmem(feat_shape, bf16),
            vmem(feat_shape, bf16),
            vmem((slots, embed), bf16),
            vmem((slots, hidden_n), bf16),
            vmem((slots, hidden_n), f32),
            vmem((slots, embed), bf16),
            vmem((slots, hidden_n), bf16),
            vmem((CHUNKS, devices, slot_rows, width), bf16),
            vmem((CHUNKS, devices, slot_rows, width), bf16),
            vmem((CHUNKS, gx_n, rows, width), bf16),
            vmem((CHUNKS, gy_n, part_rows, width), bf16),
            vmem((CHUNKS, gy_n, part_rows, width), bf16),
            dma((4,)),
            dma((4,)),
            dma((STEPS, 4)),
            dma((STEPS, 4)),
            dma((devices,)),
            dma((devices,)),
            dma((devices,)),
            dma((devices,)),
            dma((gx_n,)),
            dma((gx_n,)),
            dma((CHUNKS, devices)),
            dma((CHUNKS, devices)),
            dma((CHUNKS, 2 * chips)),
            dma((CHUNKS, gx_n)),
            dma((CHUNKS, gy_n)),
            dma((CHUNKS, gy_n)),
            dma((CHUNKS, gy_n)),
            dma((CHUNKS, gy_n, chips)),
            dma((CHUNKS, gy_n, chips)),
            dma((CHUNKS, gx_n, gy_n)),
        ],
        compiler_params=pltpu.CompilerParams(
            collective_id=0, has_side_effects=True, vmem_limit_bytes=62 * 1024 * 1024
        ),
    )(fields, patch_weight, trainer_of.T, lag_index, w_in, b_in, w_out, b_out)
    first_grad, first_bias_grad, second_grad, second_bias_grad, patch_gradient = finish(
        source, hidden, error, slope, summed.reshape(CHUNKS, features, width)
    )
    return (
        new_fields,
        patch_gradient,
        first_grad,
        first_bias_grad,
        second_grad,
        second_bias_grad,
    )


def solution(mesh):
    in_specs = (
        P(None, "gx", "gy", None),
        P(),
        P(("gx", "gy"), None),
        P("gx", "gy", None),
        P(("gx", "gy"), None, None),
        P(("gx", "gy"), None),
        P(("gx", "gy"), None, None),
        P(("gx", "gy"), None),
    )
    out_specs = (
        P(None, "gx", "gy", None),
        P(),
        P(("gx", "gy"), None, None),
        P(("gx", "gy"), None),
        P(("gx", "gy"), None, None),
        P(("gx", "gy"), None),
    )
    return jax.shard_map(
        per_device, mesh=mesh, in_specs=in_specs, out_specs=out_specs, check_vma=False
    )
```

```python
import functools

import jax
import jax.numpy as jnp
from jax import lax
from jax.experimental import pallas as pl
from jax.experimental.pallas import tpu as pltpu
from jax.sharding import PartitionSpec as P

FIELDS = 5
PATCH = 8
STEPS = 3
BLOCK_ROWS = 2
PAD = 8
CHUNKS = 2
BACK_CHUNKS = 2
HIDDEN_TILE = 512


time_step = 0.2
viscosity = 0.5
drift_x = 0.6
drift_y = -0.4
drift_z = 0.3
error_weight = 0.0625


def contract_rows(left, right):
    return lax.dot_general(
        left, right, (((0,), (0,)), ((), ())), preferred_element_type=jnp.float32
    )


def contract_cols(left, right):
    return lax.dot_general(
        left, right, (((1,), (1,)), ((), ())), preferred_element_type=jnp.float32
    )


def my_place():
    return lax.axis_index("gx"), lax.axis_index("gy")


def across(place, step):
    bit = 1
    while bit <= step:
        if step & bit:
            place = place + bit - 2 * bit * lax.rem(place // bit, 2)
        bit *= 2
    return place


def remote(src, dst, send_sem, recv_sem, gx, gy):
    return pltpu.make_async_remote_copy(
        src_ref=src,
        dst_ref=dst,
        send_sem=send_sem,
        recv_sem=recv_sem,
        device_id=(gx, gy),
        device_id_type=pl.DeviceIdType.MESH,
    )


def step_kernel(
    gx_n,
    gy_n,
    fields_hbm,
    weight_hbm,
    owner_ref,
    lag_ref,
    first_hbm,
    first_bias_ref,
    second_hbm,
    second_bias_ref,
    fields_out_hbm,
    summed_hbm,
    source_hbm,
    hidden_hbm,
    error_hbm,
    slope_hbm,
    state_0,
    state_1,
    state_2,
    out_ref,
    summed_ref,
    valid_out,
    valid_in,
    face_out,
    face_in,
    swap,
    cells,
    turned,
    place,
    weight,
    first,
    second,
    source_out,
    source_in,
    target_out,
    target_in,
    feat_out,
    feats,
    source_rows,
    hidden,
    steep,
    error,
    slope,
    grad_out,
    back,
    shared,
    parts,
    landed,
    load_sem,
    save_sem,
    valid_sems,
    halo_send,
    halo_recv,
    source_sems,
    target_sems,
    feat_send,
    feat_recv,
    back_sems,
    share_send,
    share_recv,
    part_send,
    part_recv,
    line_send,
    plane_send,
    pair_send,
    out_recv,
):
    gx, gy = my_place()
    me = gx * gy_n + gy
    devices = gx_n * gy_n
    chips = gx_n // 2
    chip, core = gx // 2, lax.rem(gx, 2)
    partner = gx + 1 - 2 * core
    states = (state_0, state_1, state_2)
    _, size_x, size_y, size_z = fields_hbm.shape
    inner = pl.ds(PAD, size_y)
    embed = weight.shape[1]
    slot_rows = source_out.shape[1]
    count_x, count_y, count_z = lag_ref.shape
    columns = count_x * count_y
    kinds = FIELDS * PATCH * PATCH
    rows = turned.shape[1]
    hidden_n = hidden.shape[1]
    width = embed // CHUNKS
    f32, bf16 = jnp.float32, jnp.bfloat16

    loads = [
        pltpu.make_async_copy(
            fields_hbm, state_0.at[:, pl.ds(2, size_x), inner, :], load_sem.at[0]
        ),
        pltpu.make_async_copy(weight_hbm, weight, load_sem.at[1]),
        pltpu.make_async_copy(first_hbm.at[0], first, load_sem.at[2]),
        pltpu.make_async_copy(second_hbm.at[0], second, load_sem.at[3]),
    ]
    for load in loads:
        load.start()

    edges = ((gx > 0, 0), (gx < gx_n - 1, 1), (gy > 0, 2), (gy < gy_n - 1, 3))
    for state in states:
        for inside, side in edges:
            @pl.when(jnp.logical_not(inside))
            def _():
                if side < 2:
                    plane = pl.ds(0 if side == 0 else size_x + 2, 2)
                    state[:, plane, inner, :] = jnp.zeros((FIELDS, 2, size_y, size_z), jnp.float32)
                else:
                    strip = pl.ds(0 if side == 2 else PAD + size_y, PAD)
                    state[:, pl.ds(2, size_x), strip, :] = jnp.zeros(
                        (FIELDS, size_x, PAD, size_z), jnp.float32
                    )

    barrier = pltpu.get_barrier_semaphore()

    def greet(step, carry):
        other = lax.rem(me + step, devices)
        pl.semaphore_signal(
            barrier,
            inc=1,
            device_id=(other // gy_n, lax.rem(other, gy_n)),
            device_id_type=pl.DeviceIdType.MESH,
        )
        return carry

    lax.fori_loop(1, devices, greet, 0)
    place_of = lax.broadcasted_iota(jnp.int32, (size_z, PATCH * rows), 1)
    column_of = lax.rem(place_of, rows) // count_z
    cell_of = column_of * size_z + lax.rem(place_of, count_z) * PATCH + place_of // rows
    for column in range(columns):
        row_of = lax.broadcasted_iota(jnp.int32, (size_z, PATCH * rows), 0) + column * size_z
        swap[pl.ds(column * size_z, size_z), :] = jnp.where(row_of == cell_of, 1.0, 0.0).astype(
            jnp.bfloat16
        )

    owner = owner_ref[...].astype(f32)
    blocks = owner.shape[1]
    tall = lax.broadcasted_iota(jnp.int32, (devices, blocks), 0).astype(f32)
    onehot = jnp.where(owner == tall, 1.0, 0.0)
    before = jnp.where(
        lax.broadcasted_iota(jnp.int32, (blocks, blocks), 0)
        < lax.broadcasted_iota(jnp.int32, (blocks, blocks), 1),
        1.0,
        0.0,
    )
    ahead = jnp.dot(onehot.astype(bf16), before.astype(bf16), preferred_element_type=f32)
    rank = jnp.sum(ahead * onehot, axis=0, keepdims=True)
    block_slot = owner * float(slot_rows // BLOCK_ROWS) + rank
    slots = place.shape[0]
    slot_block = lax.broadcasted_iota(jnp.int32, (slots, blocks), 0) // BLOCK_ROWS
    block_place = jnp.where(block_slot == slot_block.astype(f32), 1.0, 0.0)
    spread_rows = jnp.where(
        lax.broadcasted_iota(jnp.int32, (blocks, rows), 1) // BLOCK_ROWS
        == lax.broadcasted_iota(jnp.int32, (blocks, rows), 0),
        1.0,
        0.0,
    )
    row_place = jnp.dot(
        block_place.astype(bf16), spread_rows.astype(bf16), preferred_element_type=f32
    )
    same = lax.rem(lax.broadcasted_iota(jnp.int32, (slots, rows), 0), BLOCK_ROWS) == lax.rem(
        lax.broadcasted_iota(jnp.int32, (slots, rows), 1), BLOCK_ROWS
    )
    place[...] = jnp.where(same, row_place, 0.0).astype(bf16)
    pl.semaphore_wait(barrier, devices - 1)

    def halo_copy(step, side):
        state = states[step]
        if side == 0:
            src, dst = state.at[:, pl.ds(2, 2), inner], state.at[:, pl.ds(size_x + 2, 2), inner]
            target = (gx - 1, gy)
        elif side == 1:
            src, dst = state.at[:, pl.ds(size_x, 2), inner], state.at[:, pl.ds(0, 2), inner]
            target = (gx + 1, gy)
        else:
            src, dst = face_out.at[step, side - 2], face_in.at[step, 3 - side]
            target = (gx, gy - 1 if side == 2 else gy + 1)
        return remote(
            src, dst, halo_send.at[step, side], halo_recv.at[step, side ^ 1], *target
        )

    def halo_start(step):
        state = states[step]
        for side in (2, 3):
            first = PAD if side == 2 else PAD + size_y - 2
            face_out[step, side - 2] = state[:, pl.ds(2, size_x), pl.ds(first, 2), :]
        for inside, side in edges:
            @pl.when(inside)
            def _():
                halo_copy(step, side).start()

    def halo_wait(step):
        state = states[step]
        for inside, side in edges:
            @pl.when(inside)
            def _():
                copy = halo_copy(step, side)
                copy.wait_send()
                remote(
                    face_in.at[step, 0] if side > 1 else state.at[:, pl.ds(0, 2), inner],
                    face_in.at[step, 0] if side > 1 else state.at[:, pl.ds(0, 2), inner],
                    halo_send.at[step, side],
                    halo_recv.at[step, side],
                    gx,
                    gy,
                ).wait_recv()
                if side > 1:
                    first = PAD - 2 if side == 2 else PAD + size_y
                    state[:, pl.ds(2, size_x), pl.ds(first, 2), :] = face_in[step, side - 2]

    def advance_part(step, first_plane, planes, first_row, count):
        state = states[step]
        lane = lax.broadcasted_iota(jnp.int32, (count, size_z), 1)
        here = pl.ds(PAD + first_row, count)

        def plane(i, carry):
            def pieces(field):
                middle = state[field, i + 2, here, :]
                around = []
                around.append([state[field, i + k, here, :] for k in (0, 1, 3, 4)])
                around.append(
                    [state[field, i + 2, pl.ds(PAD + first_row + k, count), :] for k in (-2, -1, 1, 2)]
                )
                around.append(
                    [
                        jnp.where(lane < 2, 0.0, pltpu.roll(middle, 2, 1)),
                        jnp.where(lane < 1, 0.0, pltpu.roll(middle, 1, 1)),
                        jnp.where(lane >= size_z - 1, 0.0, pltpu.roll(middle, size_z - 1, 1)),
                        jnp.where(lane >= size_z - 2, 0.0, pltpu.roll(middle, size_z - 2, 1)),
                    ]
                )
                slopes = [(a - d) + 8.0 * (c - b) for a, b, c, d in around]
                near = sum(b + c for a, b, c, d in around)
                far = sum(a + d for a, b, c, d in around)
                change = viscosity * (16.0 * near - far - 90.0 * middle)
                change = change - (
                    drift_x * slopes[0] + drift_y * slopes[1] + drift_z * slopes[2]
                )
                return middle, slopes, change

            def put(field, value):
                if step < STEPS - 1:
                    states[step + 1][field, i + 2, here, :] = value
                else:
                    out_ref[field, i, pl.ds(first_row, count), :] = value

            scale = time_step / 12.0
            middle_p, slopes_p, change_p = pieces(4)
            spread = 0.0
            for axis in range(3):
                middle, slopes, change = pieces(1 + axis)
                spread = spread + slopes[axis]
                put(1 + axis, middle + scale * (change - slopes_p[axis]))
            put(4, middle_p + scale * (change_p - spread))
            middle, slopes, change = pieces(0)
            put(0, middle + scale * (change - spread))
            return carry

        lax.fori_loop(first_plane, first_plane + planes, plane, 0)

    def advance_inside(step):
        advance_part(step, 2, size_x - 4, PAD, size_y - 2 * PAD)

    def advance_edges(step):
        advance_part(step, 0, 2, 0, size_y)
        advance_part(step, size_x - 2, 2, 0, size_y)
        advance_part(step, 2, size_x - 4, 0, PAD)
        advance_part(step, 2, size_x - 4, size_y - PAD, PAD)


    def column_cells(state, offset_x, offset_y, column):
        first_x = offset_x + column // count_y * PATCH
        first_y = offset_y + column % count_y * PATCH
        return state[:, pl.ds(first_x, PATCH), pl.ds(first_y, PATCH), :].reshape(kinds, size_z)

    def turn_cells():
        for offset in range(PATCH):
            turned[pl.ds(offset, kinds, stride=PATCH), :] = jnp.dot(
                cells[...],
                swap[:, pl.ds(offset * rows, rows)],
                preferred_element_type=f32,
            )

    def embed_rows():
        return contract_rows(turned[...].astype(bf16), weight[...]).astype(bf16)

    def scatter(step, stage, landing, sems):
        other = lax.rem(me + step, devices)
        return remote(
            stage.at[other],
            landing.at[me],
            sems.at[0],
            sems.at[1],
            other // gy_n,
            lax.rem(other, gy_n),
        )

    def scatter_start(stage, landing, sems):
        def start(step, carry):
            scatter(step, stage, landing, sems).start()
            return carry

        lax.fori_loop(1, devices, start, 0)
        landing[me] = stage[me]

    def scatter_all(stage, landing, sems):
        others = pl.ds(0, devices - 1)
        return remote(stage.at[others], landing.at[others], sems.at[0], sems.at[1], partner, gy)

    def scatter_wait(*args):
        scatter_all(*args).wait_recv()
        unsent.append(scatter_all(*args))

    unsent = []

    def put_rows(values, stage):
        packed = jnp.dot(place[...], values, preferred_element_type=f32)
        stage[...] = packed.reshape(stage.shape).astype(bf16)

    loads[0].wait()
    halo_start(0)
    filled = jnp.sum(place[...].astype(f32), axis=1, keepdims=True)
    filled = jnp.broadcast_to(filled, (slots, valid_out.shape[2]))
    valid_out[...] = filled.reshape(valid_out.shape).astype(bf16)
    valid_args = (valid_out, valid_in, valid_sems)
    scatter_start(*valid_args)
    halo_wait(0)
    advance_part(0, 0, size_x, 0, size_y)
    halo_start(1)
    halo_wait(1)
    advance_part(1, 0, size_x, 0, size_y)
    halo_start(2)
    stretch = jnp.where(
        lax.broadcasted_iota(jnp.int32, (count_z, size_z), 1) // PATCH
        == lax.broadcasted_iota(jnp.int32, (count_z, size_z), 0),
        1.0,
        0.0,
    ).astype(bf16)
    for column_x in range(count_x):
        lag = lag_ref[column_x].astype(f32).astype(bf16)
        lag = jnp.dot(lag, stretch, preferred_element_type=f32)
        for column_y in range(count_y):
            column = column_x * count_y + column_y
            early = column_cells(state_1, 2, PAD, column)
            late = column_cells(state_2, 2, PAD, column)
            chosen = jnp.where(lag[column_y : column_y + 1, :] > 0.5, late, early)
            cells[:, pl.ds(column * size_z, size_z)] = chosen.astype(bf16)
    turn_cells()
    loads[1].wait()
    source = embed_rows()
    source_args = (source_out, source_in, source_sems)
    put_rows(source, source_out)
    scatter_start(*source_args)

    part_rows = feats.shape[2]
    for block in range(devices):
        feat_out[block // gy_n, block % gy_n] = turned[
            pl.ds(block * part_rows, part_rows), :
        ].astype(bf16)

    def feat_copy(step):
        other = lax.rem(gx + step, gx_n)
        return remote(
            feat_out.at[other], feats.at[gx], feat_send.at[step], feat_recv.at[step], other, gy
        )

    halo_wait(2)
    advance_part(2, 0, size_x, 0, size_y)
    saves = [pltpu.make_async_copy(out_ref, fields_out_hbm, save_sem.at[4])]
    saves[0].start()
    for column in range(columns):
        cells[:, pl.ds(column * size_z, size_z)] = column_cells(out_ref, 0, 0, column).astype(bf16)
    turn_cells()
    target_args = (target_out, target_in, target_sems)
    put_rows(embed_rows(), target_out)
    scatter_start(*target_args)
    for step in range(1, gx_n):
        feat_copy(step).start()
    feats[gx] = feat_out[gx]

    scatter_wait(*source_args)
    source_rows[...] = source_in[...].astype(f32).reshape(slots, embed).astype(bf16)
    scatter_wait(*valid_args)
    valid = valid_in[...].astype(f32).reshape(slots, valid_in.shape[2])[:, 0:1]
    loads[2].wait()
    loads[3].wait()
    predict = jnp.zeros((slots, embed), f32) + second_bias_ref[...]
    for tile in range(0, hidden_n, HIDDEN_TILE):
        part = pl.ds(tile, HIDDEN_TILE)
        pre = jnp.dot(source_rows[...], first[:, part], preferred_element_type=f32)
        pre = pre + first_bias_ref[:, part]
        sigma = jax.nn.sigmoid(pre)
        units = (pre * sigma).astype(bf16)
        hidden[:, part] = units
        steep[:, part] = sigma * (1.0 + pre * (1.0 - sigma))
        predict = predict + jnp.dot(units, second[part, :], preferred_element_type=f32)
    scatter_wait(*target_args)
    wanted = target_in[...].astype(f32).reshape(slots, embed)
    error[...] = (error_weight * (predict - wanted) * valid).astype(bf16)
    for tile in range(0, hidden_n, HIDDEN_TILE):
        part = pl.ds(tile, HIDDEN_TILE)
        slope[:, part] = (contract_cols(error[...], second[part, :]) * steep[:, part]).astype(bf16)
    span = embed // BACK_CHUNKS
    for group in range(BACK_CHUNKS):
        grad = contract_cols(slope[...], first[pl.ds(group * span, span), :])
        grad_out[group] = grad.reshape(devices, slot_rows, span).astype(bf16)
        scatter_start(grad_out.at[group], back.at[group], back_sems.at[group])
    results = [
        pltpu.make_async_copy(source_rows, source_hbm, save_sem.at[0]),
        pltpu.make_async_copy(hidden, hidden_hbm, save_sem.at[1]),
        pltpu.make_async_copy(error, error_hbm, save_sem.at[2]),
        pltpu.make_async_copy(slope, slope_hbm, save_sem.at[3]),
    ]
    for save in results:
        save.start()
    saves = saves + results

    def chip_at(step):
        return across(chip, step) * 2 + core

    sends = []

    def send(copy):
        copy.start()
        sends.append(copy)

    def share_copy(chunk, origin, target, slot):
        block = shared.at[chunk, origin]
        return remote(
            block, block, share_send.at[chunk, slot], share_recv.at[chunk, origin], target, gy
        )

    def part_of(chunk, block):
        total = jnp.zeros((part_rows, width), f32)
        for origin in range(gx_n):
            total = total + jnp.dot(
                feats[origin, block], shared[chunk, origin], preferred_element_type=f32
            )
        return total

    def part_copy(chunk, step):
        other = across(gy, step)
        return remote(
            parts.at[chunk, other],
            landed.at[chunk, step],
            part_send.at[chunk, step],
            part_recv.at[chunk, step],
            gx,
            other,
        )

    def out_copy(chunk, block_x, block_y, send_sem, target_x, target_y):
        block = summed_ref.at[chunk, block_x, block_y]
        return remote(
            block, block, send_sem, out_recv.at[chunk, block_x, block_y], target_x, target_y
        )

    def out_wait(chunk, block_x, block_y):
        out_copy(chunk, block_x, block_y, line_send.at[0, 0], partner, gy).wait_recv()

    near = [chip_at(step) for step in range(1, chips)]
    own = {}

    def back_event(group):
        scatter_wait(grad_out.at[group], back.at[group], back_sems.at[group])
        packed = back[group].astype(f32).reshape(slots, span).astype(bf16)
        mine = contract_rows(place[...], packed).astype(bf16)
        for piece in range(span // width):
            chunk = group * (span // width) + piece
            shared[chunk, gx] = mine[:, piece * width : (piece + 1) * width]
            for step in range(1, chips):
                send(share_copy(chunk, gx, chip_at(step), step))
            send(share_copy(chunk, gx, partner, 0))

    def share_event(chunk):
        for step in range(1, chips):
            origin = chip_at(step)
            share_copy(chunk, origin, partner, chips + step).wait_recv()
            send(share_copy(chunk, origin, partner, chips + step))

    def part_event(chunk):
        for step in range(chips):
            share_copy(chunk, chip_at(step) + 1 - 2 * core, partner, 0).wait_recv()
        if chunk == 0:
            for step in range(1, gx_n):
                feat_copy(step).wait()
        for step in range(1, gy_n):
            other = across(gy, step)
            parts[chunk, other] = part_of(chunk, other).astype(bf16)
            part_copy(chunk, step).start()
        own[chunk] = part_of(chunk, gy)

    def spread(chunk, line):
        block_y = across(gy, line)
        for slot, target in enumerate(near):
            send(out_copy(chunk, gx, block_y, plane_send.at[chunk, line, slot], target, gy))
        send(out_copy(chunk, gx, block_y, pair_send.at[chunk, line, 0], partner, gy))

    def total_event(chunk):
        total = own[chunk]
        for step in range(1, gy_n):
            part_copy(chunk, step).wait()
            total = total + landed[chunk, step].astype(f32)
        summed_ref[chunk, gx, gy] = total.astype(bf16)
        for step in range(1, gy_n):
            other = across(gy, step)
            send(out_copy(chunk, gx, gy, line_send.at[chunk, step], gx, other))
        spread(chunk, 0)

    def line_event(chunk, line):
        out_wait(chunk, gx, across(gy, line))
        spread(chunk, line)

    def near_event(chunk, line):
        block_y = across(gy, line)
        for slot, block_x in enumerate(near):
            out_wait(chunk, block_x, block_y)
            send(
                out_copy(
                    chunk, block_x, block_y, pair_send.at[chunk, line, 1 + slot], partner, gy
                )
            )

    def pair_event(chunk):
        for line in range(gy_n):
            for step in range(chips):
                out_wait(chunk, chip_at(step) + 1 - 2 * core, line)
        save = pltpu.make_async_copy(
            summed_ref.at[chunk], summed_hbm.at[chunk], save_sem.at[5 + chunk]
        )
        save.start()
        saves.append(save)

    events = []
    for chunk in range(CHUNKS):
        if chunk * BACK_CHUNKS % CHUNKS == 0:
            group = chunk * BACK_CHUNKS // CHUNKS
            events.append((6.0 + 1.4 * chunk, back_event, group))
        events.append((9.8 + 1.6 * chunk, share_event, chunk))
        events.append((11.2 + 1.6 * chunk, part_event, chunk))
        base = 16.0 + 2.6 * chunk
        events.append((base, total_event, chunk))
        events.append((base + 3.2, near_event, chunk, 0))
        for line in range(1, gy_n):
            events.append((base + 3.0 + 0.5 * line, line_event, chunk, line))
            events.append((base + 6.0 + 0.5 * line, near_event, chunk, line))
        events.append((base + 12.0, pair_event, chunk))
    for event in sorted(events, key=lambda event: event[0]):
        event[1](*event[2:])
    for copy in sends + unsent:
        copy.wait_send()
    for save in saves:
        save.wait()


def finish_kernel(source_ref, hidden_ref, error_ref, slope_ref, summed_ref, *outs):
    first_ref, first_bias_ref, second_ref, second_bias_ref, patch_ref = outs
    error, slope = error_ref[...], slope_ref[...]
    first_ref[0] = contract_rows(source_ref[...], slope)
    first_bias_ref[...] = jnp.sum(slope.astype(jnp.float32), axis=0, keepdims=True)
    second_ref[0] = contract_rows(hidden_ref[...], error)
    second_bias_ref[...] = jnp.sum(error.astype(jnp.float32), axis=0, keepdims=True)
    width = summed_ref.shape[2]
    for chunk in range(summed_ref.shape[0]):
        patch_ref[:, chunk * width : (chunk + 1) * width] = summed_ref[chunk].astype(jnp.float32)


def finish(source, hidden, error, slope, summed):
    slots, embed = source.shape
    hidden_n = hidden.shape[1]
    features, width = summed.shape[1], summed.shape[2]
    steps = hidden_n // HIDDEN_TILE
    f32 = jnp.float32
    return pl.pallas_call(
        finish_kernel,
        grid=(steps,),
        out_shape=[
            jax.ShapeDtypeStruct((1, embed, hidden_n), f32),
            jax.ShapeDtypeStruct((1, hidden_n), f32),
            jax.ShapeDtypeStruct((1, hidden_n, embed), f32),
            jax.ShapeDtypeStruct((1, embed), f32),
            jax.ShapeDtypeStruct((features, embed), f32),
        ],
        in_specs=[
            pl.BlockSpec((slots, embed), lambda i: (0, 0)),
            pl.BlockSpec((slots, HIDDEN_TILE), lambda i: (0, i)),
            pl.BlockSpec((slots, embed), lambda i: (0, 0)),
            pl.BlockSpec((slots, HIDDEN_TILE), lambda i: (0, i)),
            pl.BlockSpec((CHUNKS, features // steps, width), lambda i: (0, i, 0)),
        ],
        out_specs=[
            pl.BlockSpec((1, embed, HIDDEN_TILE), lambda i: (0, 0, i)),
            pl.BlockSpec((1, HIDDEN_TILE), lambda i: (0, i)),
            pl.BlockSpec((1, HIDDEN_TILE, embed), lambda i: (0, i, 0)),
            pl.BlockSpec((1, embed), lambda i: (0, 0)),
            pl.BlockSpec((features // steps, embed), lambda i: (i, 0)),
        ],
    )(source, hidden, error, slope, summed)


def per_device(fields, patch_weight, trainer_of, lag_index, w_in, b_in, w_out, b_out):
    gx_n, gy_n = lax.axis_size("gx"), lax.axis_size("gy")
    devices, chips = gx_n * gy_n, gx_n // 2
    fields_n, size_x, size_y, size_z = fields.shape
    features, embed = patch_weight.shape
    hidden_n = w_in.shape[2]
    rows = lag_index.size
    blocks = rows // BLOCK_ROWS
    slot_rows = max(8, 2 * blocks // devices * BLOCK_ROWS)
    slots = devices * slot_rows
    columns = lag_index.shape[0] * lag_index.shape[1]
    part_rows = features // devices
    width = embed // CHUNKS
    bf16, f32 = jnp.bfloat16, jnp.float32
    dma = pltpu.SemaphoreType.DMA
    vmem = pltpu.VMEM
    whole = pl.BlockSpec(memory_space=pltpu.VMEM)
    anywhere = pl.BlockSpec(memory_space=pl.ANY)
    padded = (fields_n, size_x + 4, size_y + 2 * PAD, size_z)
    faces = (STEPS, 2, fields_n, size_x, 2, size_z)
    source_shape = (devices, slot_rows, embed)
    valid_shape = (devices, slot_rows, 128)
    feat_shape = (gx_n, gy_n, part_rows, rows)
    block_shape = (CHUNKS, gx_n, gy_n, part_rows, width)
    new_fields, summed, source, hidden, error, slope = pl.pallas_call(
        functools.partial(step_kernel, gx_n, gy_n),
        out_shape=[
            jax.ShapeDtypeStruct(fields.shape, f32),
            jax.ShapeDtypeStruct(block_shape, bf16),
            jax.ShapeDtypeStruct((slots, embed), bf16),
            jax.ShapeDtypeStruct((slots, hidden_n), bf16),
            jax.ShapeDtypeStruct((slots, embed), bf16),
            jax.ShapeDtypeStruct((slots, hidden_n), bf16),
        ],
        in_specs=[anywhere, anywhere, whole, whole, anywhere, whole, anywhere, whole],
        out_specs=[anywhere] * 6,
        scratch_shapes=[
            vmem(padded, f32),
            vmem(padded, f32),
            vmem(padded, f32),
            vmem(fields.shape, f32),
            vmem(block_shape, bf16),
            vmem(valid_shape, bf16),
            vmem(valid_shape, bf16),
            vmem(faces, f32),
            vmem(faces, f32),
            vmem((columns * size_z, PATCH * rows), bf16),
            vmem((features // PATCH, columns * size_z), bf16),
            vmem((features, rows), f32),
            vmem((slots, rows), bf16),
            vmem((features, embed), bf16),
            vmem((embed, hidden_n), bf16),
            vmem((hidden_n, embed), bf16),
            vmem(source_shape, bf16),
            vmem(source_shape, bf16),
            vmem(source_shape, bf16),
            vmem(source_shape, bf16),
            vmem(feat_shape, bf16),
            vmem(feat_shape, bf16),
            vmem((slots, embed), bf16),
            vmem((slots, hidden_n), bf16),
            vmem((slots, hidden_n), f32),
            vmem((slots, embed), bf16),
            vmem((slots, hidden_n), bf16),
            vmem((BACK_CHUNKS, devices, slot_rows, embed // BACK_CHUNKS), bf16),
            vmem((BACK_CHUNKS, devices, slot_rows, embed // BACK_CHUNKS), bf16),
            vmem((CHUNKS, gx_n, rows, width), bf16),
            vmem((CHUNKS, gy_n, part_rows, width), bf16),
            vmem((CHUNKS, gy_n, part_rows, width), bf16),
            dma((4,)),
            dma((5 + CHUNKS,)),
            dma((2,)),
            dma((STEPS, 4)),
            dma((STEPS, 4)),
            dma((2,)),
            dma((2,)),
            dma((gx_n,)),
            dma((gx_n,)),
            dma((BACK_CHUNKS, 2)),
            dma((CHUNKS, 2 * chips)),
            dma((CHUNKS, gx_n)),
            dma((CHUNKS, gy_n)),
            dma((CHUNKS, gy_n)),
            dma((CHUNKS, gy_n)),
            dma((CHUNKS, gy_n, chips)),
            dma((CHUNKS, gy_n, chips)),
            dma((CHUNKS, gx_n, gy_n)),
        ],
        compiler_params=pltpu.CompilerParams(
            collective_id=0, has_side_effects=True, vmem_limit_bytes=62 * 1024 * 1024
        ),
    )(fields, patch_weight, trainer_of.T, lag_index, w_in, b_in, w_out, b_out)
    first_grad, first_bias_grad, second_grad, second_bias_grad, patch_gradient = finish(
        source, hidden, error, slope, summed.reshape(CHUNKS, features, width)
    )
    return (
        new_fields,
        patch_gradient,
        first_grad,
        first_bias_grad,
        second_grad,
        second_bias_grad,
    )


def solution(mesh):
    in_specs = (
        P(None, "gx", "gy", None),
        P(),
        P(("gx", "gy"), None),
        P("gx", "gy", None),
        P(("gx", "gy"), None, None),
        P(("gx", "gy"), None),
        P(("gx", "gy"), None, None),
        P(("gx", "gy"), None),
    )
    out_specs = (
        P(None, "gx", "gy", None),
        P(),
        P(("gx", "gy"), None, None),
        P(("gx", "gy"), None),
        P(("gx", "gy"), None, None),
        P(("gx", "gy"), None),
    )
    return jax.shard_map(
        per_device, mesh=mesh, in_specs=in_specs, out_specs=out_specs, check_vma=False
    )
```

```python
import functools

import jax
import jax.numpy as jnp
from jax import lax
from jax.experimental import pallas as pl
from jax.experimental.pallas import tpu as pltpu
from jax.sharding import PartitionSpec as P

FIELDS = 5
PATCH = 8
STEPS = 3
BLOCK_ROWS = 2
PAD = 8
FACE_TYPE = jnp.float32
CHUNKS = 2
BACK_CHUNKS = 2
HIDDEN_TILE = 512


time_step = 0.2
viscosity = 0.5
drift_x = 0.6
drift_y = -0.4
drift_z = 0.3
error_weight = 0.0625


def contract_rows(left, right):
    return lax.dot_general(
        left, right, (((0,), (0,)), ((), ())), preferred_element_type=jnp.float32
    )


def contract_cols(left, right):
    return lax.dot_general(
        left, right, (((1,), (1,)), ((), ())), preferred_element_type=jnp.float32
    )


def my_place():
    return lax.axis_index("gx"), lax.axis_index("gy")


def across(place, step):
    bit = 1
    while bit <= step:
        if step & bit:
            place = place + bit - 2 * bit * lax.rem(place // bit, 2)
        bit *= 2
    return place


def remote(src, dst, send_sem, recv_sem, gx, gy):
    return pltpu.make_async_remote_copy(
        src_ref=src,
        dst_ref=dst,
        send_sem=send_sem,
        recv_sem=recv_sem,
        device_id=(gx, gy),
        device_id_type=pl.DeviceIdType.MESH,
    )


def step_kernel(
    gx_n,
    gy_n,
    fields_hbm,
    weight_hbm,
    owner_ref,
    lag_ref,
    first_hbm,
    first_bias_ref,
    second_hbm,
    second_bias_ref,
    fields_out_hbm,
    summed_hbm,
    source_hbm,
    hidden_hbm,
    error_hbm,
    slope_hbm,
    state_0,
    state_1,
    state_2,
    out_ref,
    summed_ref,
    valid_out,
    valid_in,
    side_out,
    side_in,
    face_out,
    face_in,
    swap,
    cells,
    turned,
    place,
    weight,
    first,
    second,
    source_out,
    source_in,
    target_out,
    target_in,
    feat_out,
    feats,
    source_rows,
    hidden,
    steep,
    error,
    slope,
    grad_out,
    back,
    shared,
    parts,
    landed,
    load_sem,
    save_sem,
    valid_sems,
    halo_send,
    halo_recv,
    source_sems,
    target_sems,
    feat_send,
    feat_recv,
    back_sems,
    share_send,
    share_recv,
    part_send,
    part_recv,
    line_send,
    plane_send,
    pair_send,
    out_recv,
):
    gx, gy = my_place()
    me = gx * gy_n + gy
    devices = gx_n * gy_n
    chips = gx_n // 2
    chip, core = gx // 2, lax.rem(gx, 2)
    partner = gx + 1 - 2 * core
    states = (state_0, state_1, state_2)
    _, size_x, size_y, size_z = fields_hbm.shape
    inner = pl.ds(PAD, size_y)
    embed = weight.shape[1]
    slot_rows = source_out.shape[1]
    count_x, count_y, count_z = lag_ref.shape
    columns = count_x * count_y
    kinds = FIELDS * PATCH * PATCH
    rows = turned.shape[1]
    hidden_n = hidden.shape[1]
    width = embed // CHUNKS
    f32, bf16 = jnp.float32, jnp.bfloat16

    loads = [
        pltpu.make_async_copy(
            fields_hbm, state_0.at[:, pl.ds(2, size_x), inner, :], load_sem.at[0]
        ),
        pltpu.make_async_copy(weight_hbm, weight, load_sem.at[1]),
        pltpu.make_async_copy(first_hbm.at[0], first, load_sem.at[2]),
        pltpu.make_async_copy(second_hbm.at[0], second, load_sem.at[3]),
    ]
    for load in loads:
        load.start()

    edges = ((gx > 0, 0), (gx < gx_n - 1, 1), (gy > 0, 2), (gy < gy_n - 1, 3))
    for state in states:
        for inside, side in edges:
            @pl.when(jnp.logical_not(inside))
            def _():
                if side < 2:
                    plane = pl.ds(0 if side == 0 else size_x + 2, 2)
                    state[:, plane, inner, :] = jnp.zeros((FIELDS, 2, size_y, size_z), jnp.float32)
                else:
                    strip = pl.ds(0 if side == 2 else PAD + size_y, PAD)
                    state[:, pl.ds(2, size_x), strip, :] = jnp.zeros(
                        (FIELDS, size_x, PAD, size_z), jnp.float32
                    )

    barrier = pltpu.get_barrier_semaphore()

    def greet(step, carry):
        other = lax.rem(me + step, devices)
        pl.semaphore_signal(
            barrier,
            inc=1,
            device_id=(other // gy_n, lax.rem(other, gy_n)),
            device_id_type=pl.DeviceIdType.MESH,
        )
        return carry

    lax.fori_loop(1, devices, greet, 0)
    pl.semaphore_wait(barrier, devices - 1)

    def halo_ends(side):
        if side < 2:
            return side_out, side_in, (gx - 1 if side == 0 else gx + 1, gy)
        return face_out, face_in, (gx, gy - 1 if side == 2 else gy + 1)

    def halo_copy(step, side):
        out, landing, target = halo_ends(side)
        return remote(
            out.at[step, side % 2],
            landing.at[step, 1 - side % 2],
            halo_send.at[step, side],
            halo_recv.at[step, side ^ 1],
            *target
        )

    def halo_start(step):
        state = states[step]
        for side, (inside, _) in enumerate(edges):
            @pl.when(inside)
            def _():
                if side < 2:
                    first = 2 if side == 0 else size_x
                    values = state[:, pl.ds(first, 2), inner, :]
                else:
                    first = PAD if side == 2 else PAD + size_y - 2
                    values = state[:, pl.ds(2, size_x), pl.ds(first, 2), :]
                out = halo_ends(side)[0]
                out[step, side % 2] = values.astype(out.dtype)
                halo_copy(step, side).start()

    def halo_wait(step):
        state = states[step]
        for side, (inside, _) in enumerate(edges):
            @pl.when(inside)
            def _():
                landing = halo_ends(side)[1]
                block = landing.at[step, side % 2]
                remote(
                    block, block, halo_send.at[step, side], halo_recv.at[step, side], gx, gy
                ).wait_recv()
                values = landing[step, side % 2].astype(jnp.float32)
                if side < 2:
                    state[:, pl.ds(0 if side == 0 else size_x + 2, 2), inner, :] = values
                else:
                    first = PAD - 2 if side == 2 else PAD + size_y
                    state[:, pl.ds(2, size_x), pl.ds(first, 2), :] = values

    def advance_part(step, first_plane, planes, pieces_of, count):
        state = states[step]
        lane = lax.broadcasted_iota(jnp.int32, (count, size_z), 1)

        def plane(i, carry):
            for ahead, first_row in pieces_of:
                piece(i + ahead, first_row)
            return carry

        def piece(i, first_row):
            here = pl.ds(PAD + first_row, count)

            def pieces(field):
                middle = state[field, i + 2, here, :]
                around = []
                around.append([state[field, i + k, here, :] for k in (0, 1, 3, 4)])
                around.append(
                    [state[field, i + 2, pl.ds(PAD + first_row + k, count), :] for k in (-2, -1, 1, 2)]
                )
                around.append(
                    [
                        jnp.where(lane < 2, 0.0, pltpu.roll(middle, 2, 1)),
                        jnp.where(lane < 1, 0.0, pltpu.roll(middle, 1, 1)),
                        jnp.where(lane >= size_z - 1, 0.0, pltpu.roll(middle, size_z - 1, 1)),
                        jnp.where(lane >= size_z - 2, 0.0, pltpu.roll(middle, size_z - 2, 1)),
                    ]
                )
                slopes = [(a - d) + 8.0 * (c - b) for a, b, c, d in around]
                near = sum(b + c for a, b, c, d in around)
                far = sum(a + d for a, b, c, d in around)
                change = viscosity * (16.0 * near - far - 90.0 * middle)
                change = change - (
                    drift_x * slopes[0] + drift_y * slopes[1] + drift_z * slopes[2]
                )
                return middle, slopes, change

            def put(field, value):
                if step < STEPS - 1:
                    states[step + 1][field, i + 2, here, :] = value
                else:
                    out_ref[field, i, pl.ds(first_row, count), :] = value

            scale = time_step / 12.0
            middle_p, slopes_p, change_p = pieces(4)
            spread = 0.0
            for axis in range(3):
                middle, slopes, change = pieces(1 + axis)
                spread = spread + slopes[axis]
                put(1 + axis, middle + scale * (change - slopes_p[axis]))
            put(4, middle_p + scale * (change_p - spread))
            middle, slopes, change = pieces(0)
            put(0, middle + scale * (change - spread))

        lax.fori_loop(first_plane, first_plane + planes, plane, 0)

    def advance_inside(step):
        advance_part(step, 2, size_x - 4, ((0, PAD),), size_y - 2 * PAD)

    def advance_edges(step):
        advance_part(step, 0, 2, ((0, 0), (size_x - 2, 0)), size_y)
        advance_part(step, 2, size_x - 4, ((0, 0), (0, size_y - PAD)), PAD)

    def column_cells(state, offset_x, offset_y, column):
        first_x = offset_x + column // count_y * PATCH
        first_y = offset_y + column % count_y * PATCH
        return state[:, pl.ds(first_x, PATCH), pl.ds(first_y, PATCH), :].reshape(kinds, size_z)

    def turn_cells():
        for offset in range(PATCH):
            turned[pl.ds(offset, kinds, stride=PATCH), :] = jnp.dot(
                cells[...],
                swap[:, pl.ds(offset * rows, rows)],
                preferred_element_type=f32,
            )

    def embed_rows():
        return contract_rows(turned[...].astype(bf16), weight[...]).astype(bf16)

    def scatter(step, stage, landing, sems):
        other = lax.rem(me + step, devices)
        return remote(
            stage.at[other],
            landing.at[me],
            sems.at[0],
            sems.at[1],
            other // gy_n,
            lax.rem(other, gy_n),
        )

    def scatter_start(stage, landing, sems):
        def start(step, carry):
            scatter(step, stage, landing, sems).start()
            return carry

        lax.fori_loop(1, devices, start, 0)
        landing[me] = stage[me]

    def scatter_all(stage, landing, sems):
        others = pl.ds(0, devices - 1)
        return remote(stage.at[others], landing.at[others], sems.at[0], sems.at[1], partner, gy)

    def scatter_wait(*args):
        scatter_all(*args).wait_recv()
        unsent.append(scatter_all(*args))

    unsent = []

    def put_rows(values, stage):
        packed = jnp.dot(place[...], values, preferred_element_type=f32)
        stage[...] = packed.reshape(stage.shape).astype(bf16)

    loads[0].wait()
    halo_start(0)
    place_of = lax.broadcasted_iota(jnp.int32, (1, PATCH * rows), 1)
    column_of = lax.rem(place_of, rows) // count_z
    cell_of = column_of * size_z + lax.rem(place_of, count_z) * PATCH + place_of // rows
    for column in range(columns):
        row_of = lax.broadcasted_iota(jnp.int32, (size_z, PATCH * rows), 0) + column * size_z
        swap[pl.ds(column * size_z, size_z), :] = jnp.where(row_of == cell_of, 1.0, 0.0).astype(
            jnp.bfloat16
        )

    owner = owner_ref[...].astype(f32)
    blocks = owner.shape[1]
    tall = lax.broadcasted_iota(jnp.int32, (devices, blocks), 0).astype(f32)
    onehot = jnp.where(owner == tall, 1.0, 0.0)
    before = jnp.where(
        lax.broadcasted_iota(jnp.int32, (blocks, blocks), 0)
        < lax.broadcasted_iota(jnp.int32, (blocks, blocks), 1),
        1.0,
        0.0,
    )
    ahead = jnp.dot(onehot.astype(bf16), before.astype(bf16), preferred_element_type=f32)
    rank = jnp.sum(ahead * onehot, axis=0, keepdims=True)
    block_slot = owner * float(slot_rows // BLOCK_ROWS) + rank
    slots = place.shape[0]
    slot_block = lax.broadcasted_iota(jnp.int32, (slots, blocks), 0) // BLOCK_ROWS
    block_place = jnp.where(block_slot == slot_block.astype(f32), 1.0, 0.0)
    spread_rows = jnp.where(
        lax.broadcasted_iota(jnp.int32, (blocks, rows), 1) // BLOCK_ROWS
        == lax.broadcasted_iota(jnp.int32, (blocks, rows), 0),
        1.0,
        0.0,
    )
    row_place = jnp.dot(
        block_place.astype(bf16), spread_rows.astype(bf16), preferred_element_type=f32
    )
    same = lax.rem(lax.broadcasted_iota(jnp.int32, (slots, rows), 0), BLOCK_ROWS) == lax.rem(
        lax.broadcasted_iota(jnp.int32, (slots, rows), 1), BLOCK_ROWS
    )
    place[...] = jnp.where(same, row_place, 0.0).astype(bf16)
    filled = jnp.sum(place[...].astype(f32), axis=1, keepdims=True)
    filled = jnp.broadcast_to(filled, (slots, valid_out.shape[2]))
    valid_out[...] = filled.reshape(valid_out.shape).astype(bf16)
    valid_args = (valid_out, valid_in, valid_sems)
    scatter_start(*valid_args)
    advance_inside(0)
    halo_wait(0)
    advance_edges(0)
    halo_start(1)
    advance_inside(1)
    halo_wait(1)
    advance_edges(1)
    halo_start(2)
    stretch = jnp.where(
        lax.broadcasted_iota(jnp.int32, (count_z, size_z), 1) // PATCH
        == lax.broadcasted_iota(jnp.int32, (count_z, size_z), 0),
        1.0,
        0.0,
    ).astype(bf16)
    for column_x in range(count_x):
        lag = lag_ref[column_x].astype(f32).astype(bf16)
        lag = jnp.dot(lag, stretch, preferred_element_type=f32)
        for column_y in range(count_y):
            column = column_x * count_y + column_y
            early = column_cells(state_1, 2, PAD, column)
            late = column_cells(state_2, 2, PAD, column)
            chosen = jnp.where(lag[column_y : column_y + 1, :] > 0.5, late, early)
            cells[:, pl.ds(column * size_z, size_z)] = chosen.astype(bf16)
    turn_cells()
    loads[1].wait()
    source = embed_rows()
    source_args = (source_out, source_in, source_sems)
    put_rows(source, source_out)
    scatter_start(*source_args)

    part_rows = feats.shape[2]
    for block in range(devices):
        feat_out[block // gy_n, block % gy_n] = turned[
            pl.ds(block * part_rows, part_rows), :
        ].astype(bf16)

    def feat_copy(step):
        other = lax.rem(gx + step, gx_n)
        return remote(
            feat_out.at[other], feats.at[gx], feat_send.at[step], feat_recv.at[step], other, gy
        )

    advance_inside(2)
    halo_wait(2)
    advance_edges(2)
    saves = [pltpu.make_async_copy(out_ref, fields_out_hbm, save_sem.at[4])]
    saves[0].start()
    for column in range(columns):
        cells[:, pl.ds(column * size_z, size_z)] = column_cells(out_ref, 0, 0, column).astype(bf16)
    turn_cells()
    target_args = (target_out, target_in, target_sems)
    put_rows(embed_rows(), target_out)
    scatter_start(*target_args)
    for step in range(1, gx_n):
        feat_copy(step).start()
    feats[gx] = feat_out[gx]

    scatter_wait(*source_args)
    source_rows[...] = source_in[...].astype(f32).reshape(slots, embed).astype(bf16)
    scatter_wait(*valid_args)
    valid = valid_in[...].astype(f32).reshape(slots, valid_in.shape[2])[:, 0:1]
    loads[2].wait()
    loads[3].wait()
    predict = jnp.zeros((slots, embed), f32) + second_bias_ref[...]
    for tile in range(0, hidden_n, HIDDEN_TILE):
        part = pl.ds(tile, HIDDEN_TILE)
        pre = jnp.dot(source_rows[...], first[:, part], preferred_element_type=f32)
        pre = pre + first_bias_ref[:, part]
        sigma = jax.nn.sigmoid(pre)
        units = (pre * sigma).astype(bf16)
        hidden[:, part] = units
        steep[:, part] = sigma * (1.0 + pre * (1.0 - sigma))
        predict = predict + jnp.dot(units, second[part, :], preferred_element_type=f32)
    scatter_wait(*target_args)
    wanted = target_in[...].astype(f32).reshape(slots, embed)
    error[...] = (error_weight * (predict - wanted) * valid).astype(bf16)
    for tile in range(0, hidden_n, HIDDEN_TILE):
        part = pl.ds(tile, HIDDEN_TILE)
        slope[:, part] = (contract_cols(error[...], second[part, :]) * steep[:, part]).astype(bf16)
    span = embed // BACK_CHUNKS
    for group in range(BACK_CHUNKS):
        grad = contract_cols(slope[...], first[pl.ds(group * span, span), :])
        grad_out[group] = grad.reshape(devices, slot_rows, span).astype(bf16)
        scatter_start(grad_out.at[group], back.at[group], back_sems.at[group])
    results = [
        pltpu.make_async_copy(source_rows, source_hbm, save_sem.at[0]),
        pltpu.make_async_copy(hidden, hidden_hbm, save_sem.at[1]),
        pltpu.make_async_copy(error, error_hbm, save_sem.at[2]),
        pltpu.make_async_copy(slope, slope_hbm, save_sem.at[3]),
    ]
    for save in results:
        save.start()
    saves = saves + results

    def chip_at(step):
        return across(chip, step) * 2 + core

    sends = []

    def send(copy):
        copy.start()
        sends.append(copy)

    def share_copy(chunk, origin, target, slot):
        block = shared.at[chunk, origin]
        return remote(
            block, block, share_send.at[chunk, slot], share_recv.at[chunk, origin], target, gy
        )

    def part_of(chunk, block):
        total = jnp.zeros((part_rows, width), f32)
        for origin in range(gx_n):
            total = total + jnp.dot(
                feats[origin, block], shared[chunk, origin], preferred_element_type=f32
            )
        return total

    def part_copy(chunk, step):
        other = across(gy, step)
        return remote(
            parts.at[chunk, other],
            landed.at[chunk, step],
            part_send.at[chunk, step],
            part_recv.at[chunk, step],
            gx,
            other,
        )

    def out_copy(chunk, block_x, block_y, send_sem, target_x, target_y):
        block = summed_ref.at[chunk, block_x, block_y]
        return remote(
            block, block, send_sem, out_recv.at[chunk, block_x, block_y], target_x, target_y
        )

    def out_wait(chunk, block_x, block_y):
        out_copy(chunk, block_x, block_y, line_send.at[0, 0], partner, gy).wait_recv()

    near = [chip_at(step) for step in range(1, chips)]
    own = {}

    def back_event(group):
        scatter_wait(grad_out.at[group], back.at[group], back_sems.at[group])
        packed = back[group].astype(f32).reshape(slots, span).astype(bf16)
        mine = contract_rows(place[...], packed).astype(bf16)
        for piece in range(span // width):
            chunk = group * (span // width) + piece
            shared[chunk, gx] = mine[:, piece * width : (piece + 1) * width]
            for step in range(1, chips):
                send(share_copy(chunk, gx, chip_at(step), step))
            send(share_copy(chunk, gx, partner, 0))

    def share_event(chunk):
        for step in range(1, chips):
            origin = chip_at(step)
            share_copy(chunk, origin, partner, chips + step).wait_recv()
            send(share_copy(chunk, origin, partner, chips + step))

    def part_event(chunk):
        for step in range(chips):
            share_copy(chunk, chip_at(step) + 1 - 2 * core, partner, 0).wait_recv()
        if chunk == 0:
            for step in range(1, gx_n):
                feat_copy(step).wait()
        for step in range(1, gy_n):
            other = across(gy, step)
            parts[chunk, other] = part_of(chunk, other).astype(bf16)
            part_copy(chunk, step).start()
        own[chunk] = part_of(chunk, gy)

    def spread(chunk, line):
        block_y = across(gy, line)
        for slot, target in enumerate(near):
            send(out_copy(chunk, gx, block_y, plane_send.at[chunk, line, slot], target, gy))
        send(out_copy(chunk, gx, block_y, pair_send.at[chunk, line, 0], partner, gy))

    def total_event(chunk):
        total = own[chunk]
        for step in range(1, gy_n):
            part_copy(chunk, step).wait()
            total = total + landed[chunk, step].astype(f32)
        summed_ref[chunk, gx, gy] = total.astype(bf16)
        for step in range(1, gy_n):
            other = across(gy, step)
            send(out_copy(chunk, gx, gy, line_send.at[chunk, step], gx, other))
        spread(chunk, 0)

    def line_event(chunk, line):
        out_wait(chunk, gx, across(gy, line))
        spread(chunk, line)

    def near_event(chunk, line):
        block_y = across(gy, line)
        for slot, block_x in enumerate(near):
            out_wait(chunk, block_x, block_y)
            send(
                out_copy(
                    chunk, block_x, block_y, pair_send.at[chunk, line, 1 + slot], partner, gy
                )
            )

    def pair_event(chunk):
        for line in range(gy_n):
            for step in range(chips):
                out_wait(chunk, chip_at(step) + 1 - 2 * core, line)
        save = pltpu.make_async_copy(
            summed_ref.at[chunk], summed_hbm.at[chunk], save_sem.at[5 + chunk]
        )
        save.start()
        saves.append(save)

    events = []
    for chunk in range(CHUNKS):
        if chunk * BACK_CHUNKS % CHUNKS == 0:
            group = chunk * BACK_CHUNKS // CHUNKS
            events.append((6.0 + 1.4 * chunk, back_event, group))
        events.append((9.8 + 1.6 * chunk, share_event, chunk))
        events.append((11.2 + 1.6 * chunk, part_event, chunk))
        base = 16.0 + 2.6 * chunk
        events.append((base, total_event, chunk))
        events.append((base + 3.2, near_event, chunk, 0))
        for line in range(1, gy_n):
            events.append((base + 3.0 + 0.5 * line, line_event, chunk, line))
            events.append((base + 6.0 + 0.5 * line, near_event, chunk, line))
        events.append((base + 12.0, pair_event, chunk))
    for event in sorted(events, key=lambda event: event[0]):
        event[1](*event[2:])
    for copy in sends + unsent:
        copy.wait_send()
    for step in range(STEPS):
        for inside, side in edges:
            @pl.when(inside)
            def _():
                halo_copy(step, side).wait_send()

    for save in saves:
        save.wait()


def finish_kernel(source_ref, hidden_ref, error_ref, slope_ref, summed_ref, *outs):
    first_ref, first_bias_ref, second_ref, second_bias_ref, patch_ref = outs
    error, slope = error_ref[...], slope_ref[...]
    first_ref[0] = contract_rows(source_ref[...], slope)
    first_bias_ref[...] = jnp.sum(slope.astype(jnp.float32), axis=0, keepdims=True)
    second_ref[0] = contract_rows(hidden_ref[...], error)
    second_bias_ref[...] = jnp.sum(error.astype(jnp.float32), axis=0, keepdims=True)
    width = summed_ref.shape[2]
    for chunk in range(summed_ref.shape[0]):
        patch_ref[:, chunk * width : (chunk + 1) * width] = summed_ref[chunk].astype(jnp.float32)


def finish(source, hidden, error, slope, summed):
    slots, embed = source.shape
    hidden_n = hidden.shape[1]
    features, width = summed.shape[1], summed.shape[2]
    steps = hidden_n // HIDDEN_TILE
    f32 = jnp.float32
    return pl.pallas_call(
        finish_kernel,
        grid=(steps,),
        out_shape=[
            jax.ShapeDtypeStruct((1, embed, hidden_n), f32),
            jax.ShapeDtypeStruct((1, hidden_n), f32),
            jax.ShapeDtypeStruct((1, hidden_n, embed), f32),
            jax.ShapeDtypeStruct((1, embed), f32),
            jax.ShapeDtypeStruct((features, embed), f32),
        ],
        in_specs=[
            pl.BlockSpec((slots, embed), lambda i: (0, 0)),
            pl.BlockSpec((slots, HIDDEN_TILE), lambda i: (0, i)),
            pl.BlockSpec((slots, embed), lambda i: (0, 0)),
            pl.BlockSpec((slots, HIDDEN_TILE), lambda i: (0, i)),
            pl.BlockSpec((CHUNKS, features // steps, width), lambda i: (0, i, 0)),
        ],
        out_specs=[
            pl.BlockSpec((1, embed, HIDDEN_TILE), lambda i: (0, 0, i)),
            pl.BlockSpec((1, HIDDEN_TILE), lambda i: (0, i)),
            pl.BlockSpec((1, HIDDEN_TILE, embed), lambda i: (0, i, 0)),
            pl.BlockSpec((1, embed), lambda i: (0, 0)),
            pl.BlockSpec((features // steps, embed), lambda i: (i, 0)),
        ],
    )(source, hidden, error, slope, summed)


def per_device(fields, patch_weight, trainer_of, lag_index, w_in, b_in, w_out, b_out):
    gx_n, gy_n = lax.axis_size("gx"), lax.axis_size("gy")
    devices, chips = gx_n * gy_n, gx_n // 2
    fields_n, size_x, size_y, size_z = fields.shape
    features, embed = patch_weight.shape
    hidden_n = w_in.shape[2]
    rows = lag_index.size
    blocks = rows // BLOCK_ROWS
    slot_rows = max(8, 2 * blocks // devices * BLOCK_ROWS)
    slots = devices * slot_rows
    columns = lag_index.shape[0] * lag_index.shape[1]
    part_rows = features // devices
    width = embed // CHUNKS
    bf16, f32 = jnp.bfloat16, jnp.float32
    dma = pltpu.SemaphoreType.DMA
    vmem = pltpu.VMEM
    whole = pl.BlockSpec(memory_space=pltpu.VMEM)
    anywhere = pl.BlockSpec(memory_space=pl.ANY)
    padded = (fields_n, size_x + 4, size_y + 2 * PAD, size_z)
    sides = (STEPS, 2, fields_n, 2, size_y, size_z)
    faces = (STEPS, 2, fields_n, size_x, 2, size_z)
    source_shape = (devices, slot_rows, embed)
    valid_shape = (devices, slot_rows, 128)
    feat_shape = (gx_n, gy_n, part_rows, rows)
    block_shape = (CHUNKS, gx_n, gy_n, part_rows, width)
    new_fields, summed, source, hidden, error, slope = pl.pallas_call(
        functools.partial(step_kernel, gx_n, gy_n),
        out_shape=[
            jax.ShapeDtypeStruct(fields.shape, f32),
            jax.ShapeDtypeStruct(block_shape, bf16),
            jax.ShapeDtypeStruct((slots, embed), bf16),
            jax.ShapeDtypeStruct((slots, hidden_n), bf16),
            jax.ShapeDtypeStruct((slots, embed), bf16),
            jax.ShapeDtypeStruct((slots, hidden_n), bf16),
        ],
        in_specs=[anywhere, anywhere, whole, whole, anywhere, whole, anywhere, whole],
        out_specs=[anywhere] * 6,
        scratch_shapes=[
            vmem(padded, f32),
            vmem(padded, f32),
            vmem(padded, f32),
            vmem(fields.shape, f32),
            vmem(block_shape, bf16),
            vmem(valid_shape, bf16),
            vmem(valid_shape, bf16),
            vmem(sides, bf16),
            vmem(sides, bf16),
            vmem(faces, FACE_TYPE),
            vmem(faces, FACE_TYPE),
            vmem((columns * size_z, PATCH * rows), bf16),
            vmem((features // PATCH, columns * size_z), bf16),
            vmem((features, rows), f32),
            vmem((slots, rows), bf16),
            vmem((features, embed), bf16),
            vmem((embed, hidden_n), bf16),
            vmem((hidden_n, embed), bf16),
            vmem(source_shape, bf16),
            vmem(source_shape, bf16),
            vmem(source_shape, bf16),
            vmem(source_shape, bf16),
            vmem(feat_shape, bf16),
            vmem(feat_shape, bf16),
            vmem((slots, embed), bf16),
            vmem((slots, hidden_n), bf16),
            vmem((slots, hidden_n), f32),
            vmem((slots, embed), bf16),
            vmem((slots, hidden_n), bf16),
            vmem((BACK_CHUNKS, devices, slot_rows, embed // BACK_CHUNKS), bf16),
            vmem((BACK_CHUNKS, devices, slot_rows, embed // BACK_CHUNKS), bf16),
            vmem((CHUNKS, gx_n, rows, width), bf16),
            vmem((CHUNKS, gy_n, part_rows, width), bf16),
            vmem((CHUNKS, gy_n, part_rows, width), bf16),
            dma((4,)),
            dma((5 + CHUNKS,)),
            dma((2,)),
            dma((STEPS, 4)),
            dma((STEPS, 4)),
            dma((2,)),
            dma((2,)),
            dma((gx_n,)),
            dma((gx_n,)),
            dma((BACK_CHUNKS, 2)),
            dma((CHUNKS, 2 * chips)),
            dma((CHUNKS, gx_n)),
            dma((CHUNKS, gy_n)),
            dma((CHUNKS, gy_n)),
            dma((CHUNKS, gy_n)),
            dma((CHUNKS, gy_n, chips)),
            dma((CHUNKS, gy_n, chips)),
            dma((CHUNKS, gx_n, gy_n)),
        ],
        compiler_params=pltpu.CompilerParams(
            collective_id=0, has_side_effects=True, vmem_limit_bytes=62 * 1024 * 1024
        ),
    )(fields, patch_weight, trainer_of.T, lag_index, w_in, b_in, w_out, b_out)
    first_grad, first_bias_grad, second_grad, second_bias_grad, patch_gradient = finish(
        source, hidden, error, slope, summed.reshape(CHUNKS, features, width)
    )
    return (
        new_fields,
        patch_gradient,
        first_grad,
        first_bias_grad,
        second_grad,
        second_bias_grad,
    )


def solution(mesh):
    in_specs = (
        P(None, "gx", "gy", None),
        P(),
        P(("gx", "gy"), None),
        P("gx", "gy", None),
        P(("gx", "gy"), None, None),
        P(("gx", "gy"), None),
        P(("gx", "gy"), None, None),
        P(("gx", "gy"), None),
    )
    out_specs = (
        P(None, "gx", "gy", None),
        P(),
        P(("gx", "gy"), None, None),
        P(("gx", "gy"), None),
        P(("gx", "gy"), None, None),
        P(("gx", "gy"), None),
    )
    return jax.shard_map(
        per_device, mesh=mesh, in_specs=in_specs, out_specs=out_specs, check_vma=False
    )
```

```python
import functools

import jax
import jax.numpy as jnp
from jax import lax
from jax.experimental import pallas as pl
from jax.experimental.pallas import tpu as pltpu
from jax.sharding import PartitionSpec as P

FIELDS = 5
PATCH = 8
STEPS = 3
BLOCK_ROWS = 2
PAD = 8
FACE_TYPE = jnp.float32
CHUNKS = 2
BACK_CHUNKS = 2
HIDDEN_TILE = 512
FINISH_STEPS = 4


time_step = 0.2
viscosity = 0.5
drift_x = 0.6
drift_y = -0.4
drift_z = 0.3
error_weight = 0.0625


def contract_rows(left, right):
    return lax.dot_general(
        left, right, (((0,), (0,)), ((), ())), preferred_element_type=jnp.float32
    )


def contract_cols(left, right):
    return lax.dot_general(
        left, right, (((1,), (1,)), ((), ())), preferred_element_type=jnp.float32
    )


def my_place():
    return lax.axis_index("gx"), lax.axis_index("gy")


def across(place, step):
    bit = 1
    while bit <= step:
        if step & bit:
            place = place + bit - 2 * bit * lax.rem(place // bit, 2)
        bit *= 2
    return place


def remote(src, dst, send_sem, recv_sem, gx, gy):
    return pltpu.make_async_remote_copy(
        src_ref=src,
        dst_ref=dst,
        send_sem=send_sem,
        recv_sem=recv_sem,
        device_id=(gx, gy),
        device_id_type=pl.DeviceIdType.MESH,
    )


def step_kernel(
    gx_n,
    gy_n,
    fields_hbm,
    weight_hbm,
    owner_hbm,
    lag_hbm,
    first_hbm,
    first_bias_hbm,
    second_hbm,
    second_bias_hbm,
    fields_out_hbm,
    summed_hbm,
    source_hbm,
    hidden_hbm,
    error_hbm,
    slope_hbm,
    state_0,
    state_1,
    state_2,
    out_ref,
    summed_ref,
    owner_ref,
    lag_ref,
    first_bias_ref,
    second_bias_ref,
    valid_out,
    valid_in,
    side_out,
    side_in,
    face_out,
    face_in,
    swap,
    cells,
    turned,
    place,
    weight,
    first,
    second,
    source_out,
    source_in,
    target_out,
    target_in,
    feat_out,
    feats,
    source_rows,
    source_turned,
    hidden,
    steep,
    error,
    slope,
    grad_out,
    back,
    shared,
    parts,
    landed,
    load_sem,
    save_sem,
    valid_sems,
    halo_send,
    halo_recv,
    source_sems,
    target_sems,
    feat_send,
    feat_recv,
    back_sems,
    share_send,
    share_recv,
    part_send,
    part_recv,
    line_send,
    plane_send,
    pair_send,
    out_recv,
):
    gx, gy = my_place()
    me = gx * gy_n + gy
    devices = gx_n * gy_n
    chips = gx_n // 2
    chip, core = gx // 2, lax.rem(gx, 2)
    partner = gx + 1 - 2 * core
    states = (state_0, state_1, state_2)
    _, size_x, size_y, size_z = fields_hbm.shape
    inner = pl.ds(PAD, size_y)
    embed = weight.shape[1]
    slot_rows = source_out.shape[1]
    count_x, count_y, count_z = lag_ref.shape
    columns = count_x * count_y
    kinds = FIELDS * PATCH * PATCH
    rows = turned.shape[1]
    hidden_n = hidden.shape[0]
    width = embed // CHUNKS
    f32, bf16 = jnp.float32, jnp.bfloat16

    barrier = pltpu.get_barrier_semaphore()

    def greet(step, carry):
        other = lax.rem(me + step, devices)
        pl.semaphore_signal(
            barrier,
            inc=1,
            device_id=(other // gy_n, lax.rem(other, gy_n)),
            device_id_type=pl.DeviceIdType.MESH,
        )
        return carry

    lax.fori_loop(1, devices, greet, 0)
    loads = [
        pltpu.make_async_copy(
            fields_hbm, state_0.at[:, pl.ds(2, size_x), inner, :], load_sem.at[0]
        ),
        pltpu.make_async_copy(weight_hbm, weight, load_sem.at[1]),
        pltpu.make_async_copy(first_hbm.at[0], first, load_sem.at[2]),
        pltpu.make_async_copy(second_hbm.at[0], second, load_sem.at[3]),
        pltpu.make_async_copy(owner_hbm, owner_ref, load_sem.at[4]),
        pltpu.make_async_copy(lag_hbm, lag_ref, load_sem.at[5]),
        pltpu.make_async_copy(first_bias_hbm, first_bias_ref, load_sem.at[6]),
        pltpu.make_async_copy(second_bias_hbm, second_bias_ref, load_sem.at[7]),
    ]
    for load in loads:
        load.start()

    edges = ((gx > 0, 0), (gx < gx_n - 1, 1), (gy > 0, 2), (gy < gy_n - 1, 3))
    pl.semaphore_wait(barrier, devices - 1)

    def halo_ends(side):
        if side < 2:
            return side_out, side_in, (gx - 1 if side == 0 else gx + 1, gy)
        return face_out, face_in, (gx, gy - 1 if side == 2 else gy + 1)

    def halo_copy(step, side):
        out, landing, target = halo_ends(side)
        return remote(
            out.at[step, side % 2],
            landing.at[step, 1 - side % 2],
            halo_send.at[step, side],
            halo_recv.at[step, side ^ 1],
            *target
        )

    def halo_start(step):
        state = states[step]
        for side, (inside, _) in enumerate(edges):
            @pl.when(inside)
            def _():
                if side < 2:
                    first = 2 if side == 0 else size_x
                    values = state[:, pl.ds(first, 2), inner, :]
                else:
                    first = PAD if side == 2 else PAD + size_y - 2
                    values = state[:, pl.ds(2, size_x), pl.ds(first, 2), :]
                out = halo_ends(side)[0]
                out[step, side % 2] = values.astype(out.dtype)
                halo_copy(step, side).start()

    def halo_wait(step):
        state = states[step]
        for side, (inside, _) in enumerate(edges):
            @pl.when(inside)
            def _():
                landing = halo_ends(side)[1]
                block = landing.at[step, side % 2]
                remote(
                    block, block, halo_send.at[step, side], halo_recv.at[step, side], gx, gy
                ).wait_recv()
                values = landing[step, side % 2].astype(jnp.float32)
                if side < 2:
                    state[:, pl.ds(0 if side == 0 else size_x + 2, 2), inner, :] = values
                else:
                    first = PAD - 2 if side == 2 else PAD + size_y
                    state[:, pl.ds(2, size_x), pl.ds(first, 2), :] = values

    def advance_part(step, first_plane, planes, pieces_of, count):
        state = states[step]
        lane = lax.broadcasted_iota(jnp.int32, (count, size_z), 1)

        def plane(i, carry):
            for ahead, first_row in pieces_of:
                piece(i + ahead, first_row)
            return carry

        def piece(i, first_row):
            here = pl.ds(PAD + first_row, count)

            def pieces(field):
                middle = state[field, i + 2, here, :]
                around = []
                around.append([state[field, i + k, here, :] for k in (0, 1, 3, 4)])
                around.append(
                    [state[field, i + 2, pl.ds(PAD + first_row + k, count), :] for k in (-2, -1, 1, 2)]
                )
                around.append(
                    [
                        jnp.where(lane < 2, 0.0, pltpu.roll(middle, 2, 1)),
                        jnp.where(lane < 1, 0.0, pltpu.roll(middle, 1, 1)),
                        jnp.where(lane >= size_z - 1, 0.0, pltpu.roll(middle, size_z - 1, 1)),
                        jnp.where(lane >= size_z - 2, 0.0, pltpu.roll(middle, size_z - 2, 1)),
                    ]
                )
                slopes = [(a - d) + 8.0 * (c - b) for a, b, c, d in around]
                near = sum(b + c for a, b, c, d in around)
                far = sum(a + d for a, b, c, d in around)
                change = viscosity * (16.0 * near - far - 90.0 * middle)
                change = change - (
                    drift_x * slopes[0] + drift_y * slopes[1] + drift_z * slopes[2]
                )
                return middle, slopes, change

            def put(field, value):
                if step < STEPS - 1:
                    states[step + 1][field, i + 2, here, :] = value
                else:
                    out_ref[field, i, pl.ds(first_row, count), :] = value

            scale = time_step / 12.0
            middle_p, slopes_p, change_p = pieces(4)
            spread = 0.0
            for axis in range(3):
                middle, slopes, change = pieces(1 + axis)
                spread = spread + slopes[axis]
                put(1 + axis, middle + scale * (change - slopes_p[axis]))
            put(4, middle_p + scale * (change_p - spread))
            middle, slopes, change = pieces(0)
            put(0, middle + scale * (change - spread))

        lax.fori_loop(first_plane, first_plane + planes, plane, 0)

    def advance_inside(step):
        advance_part(step, 2, size_x - 4, ((0, PAD),), size_y - 2 * PAD)

    def advance_edges(step):
        advance_part(step, 0, 2, ((0, 0), (size_x - 2, 0)), size_y)
        advance_part(step, 2, size_x - 4, ((0, 0), (0, size_y - PAD)), PAD)

    def column_cells(state, offset_x, offset_y, column):
        first_x = offset_x + column // count_y * PATCH
        first_y = offset_y + column % count_y * PATCH
        return state[:, pl.ds(first_x, PATCH), pl.ds(first_y, PATCH), :].reshape(kinds, size_z)

    def turn_cells():
        for offset in range(PATCH):
            turned[pl.ds(offset, kinds, stride=PATCH), :] = jnp.dot(
                cells[...],
                swap[:, pl.ds(offset * rows, rows)],
                preferred_element_type=f32,
            )

    def embed_rows():
        return contract_rows(turned[...].astype(bf16), weight[...]).astype(bf16)

    def scatter(step, stage, landing, sems):
        other = lax.rem(me + step, devices)
        return remote(
            stage.at[other],
            landing.at[me],
            sems.at[0],
            sems.at[1],
            other // gy_n,
            lax.rem(other, gy_n),
        )

    def scatter_start(stage, landing, sems):
        def start(step, carry):
            scatter(step, stage, landing, sems).start()
            return carry

        lax.fori_loop(1, devices, start, 0)
        landing[me] = stage[me]

    def scatter_all(stage, landing, sems):
        others = pl.ds(0, devices - 1)
        return remote(stage.at[others], landing.at[others], sems.at[0], sems.at[1], partner, gy)

    def scatter_wait(*args):
        scatter_all(*args).wait_recv()
        unsent.append(scatter_all(*args))

    unsent = []

    def put_rows(values, stage):
        packed = jnp.dot(place[...], values, preferred_element_type=f32)
        stage[...] = packed.reshape(stage.shape).astype(bf16)

    loads[0].wait()
    halo_start(0)
    for state in states:
        for inside, side in edges:
            @pl.when(jnp.logical_not(inside))
            def _():
                if side < 2:
                    plane = pl.ds(0 if side == 0 else size_x + 2, 2)
                    state[:, plane, inner, :] = jnp.zeros((FIELDS, 2, size_y, size_z), jnp.float32)
                else:
                    strip = pl.ds(0 if side == 2 else PAD + size_y, PAD)
                    state[:, pl.ds(2, size_x), strip, :] = jnp.zeros(
                        (FIELDS, size_x, PAD, size_z), jnp.float32
                    )

    place_of = lax.broadcasted_iota(jnp.int32, (1, PATCH * rows), 1)
    column_of = lax.rem(place_of, rows) // count_z
    cell_of = column_of * size_z + lax.rem(place_of, count_z) * PATCH + place_of // rows
    for column in range(columns):
        row_of = lax.broadcasted_iota(jnp.int32, (size_z, PATCH * rows), 0) + column * size_z
        swap[pl.ds(column * size_z, size_z), :] = jnp.where(row_of == cell_of, 1.0, 0.0).astype(
            jnp.bfloat16
        )

    loads[4].wait()
    owner = owner_ref[...].astype(f32)
    blocks = owner.shape[1]
    tall = lax.broadcasted_iota(jnp.int32, (devices, blocks), 0).astype(f32)
    onehot = jnp.where(owner == tall, 1.0, 0.0)
    before = jnp.where(
        lax.broadcasted_iota(jnp.int32, (blocks, blocks), 0)
        < lax.broadcasted_iota(jnp.int32, (blocks, blocks), 1),
        1.0,
        0.0,
    )
    ahead = jnp.dot(onehot.astype(bf16), before.astype(bf16), preferred_element_type=f32)
    rank = jnp.sum(ahead * onehot, axis=0, keepdims=True)
    block_slot = owner * float(slot_rows // BLOCK_ROWS) + rank
    slots = place.shape[0]
    slot_block = lax.broadcasted_iota(jnp.int32, (slots, blocks), 0) // BLOCK_ROWS
    block_place = jnp.where(block_slot == slot_block.astype(f32), 1.0, 0.0)
    spread_rows = jnp.where(
        lax.broadcasted_iota(jnp.int32, (blocks, rows), 1) // BLOCK_ROWS
        == lax.broadcasted_iota(jnp.int32, (blocks, rows), 0),
        1.0,
        0.0,
    )
    row_place = jnp.dot(
        block_place.astype(bf16), spread_rows.astype(bf16), preferred_element_type=f32
    )
    same = lax.rem(lax.broadcasted_iota(jnp.int32, (slots, rows), 0), BLOCK_ROWS) == lax.rem(
        lax.broadcasted_iota(jnp.int32, (slots, rows), 1), BLOCK_ROWS
    )
    place[...] = jnp.where(same, row_place, 0.0).astype(bf16)
    filled = jnp.sum(place[...].astype(f32), axis=1, keepdims=True)
    filled = jnp.broadcast_to(filled, (slots, valid_out.shape[2]))
    valid_out[...] = filled.reshape(valid_out.shape).astype(bf16)
    valid_args = (valid_out, valid_in, valid_sems)
    scatter_start(*valid_args)
    advance_inside(0)
    halo_wait(0)
    advance_edges(0)
    halo_start(1)
    advance_inside(1)
    halo_wait(1)
    advance_edges(1)
    halo_start(2)
    stretch = jnp.where(
        lax.broadcasted_iota(jnp.int32, (count_z, size_z), 1) // PATCH
        == lax.broadcasted_iota(jnp.int32, (count_z, size_z), 0),
        1.0,
        0.0,
    ).astype(bf16)
    loads[5].wait()
    for column_x in range(count_x):
        lag = lag_ref[column_x].astype(f32).astype(bf16)
        lag = jnp.dot(lag, stretch, preferred_element_type=f32)
        for column_y in range(count_y):
            column = column_x * count_y + column_y
            early = column_cells(state_1, 2, PAD, column)
            late = column_cells(state_2, 2, PAD, column)
            chosen = jnp.where(lag[column_y : column_y + 1, :] > 0.5, late, early)
            cells[:, pl.ds(column * size_z, size_z)] = chosen.astype(bf16)
    turn_cells()
    loads[1].wait()
    source = embed_rows()
    source_args = (source_out, source_in, source_sems)
    put_rows(source, source_out)
    scatter_start(*source_args)

    part_rows = feats.shape[2]
    for block in range(devices):
        feat_out[block // gy_n, block % gy_n] = turned[
            pl.ds(block * part_rows, part_rows), :
        ].astype(bf16)

    def feat_copy(step):
        other = lax.rem(gx + step, gx_n)
        return remote(
            feat_out.at[other], feats.at[gx], feat_send.at[step], feat_recv.at[step], other, gy
        )

    advance_inside(2)
    halo_wait(2)
    advance_edges(2)
    saves = [pltpu.make_async_copy(out_ref, fields_out_hbm, save_sem.at[4])]
    saves[0].start()
    for column in range(columns):
        cells[:, pl.ds(column * size_z, size_z)] = column_cells(out_ref, 0, 0, column).astype(bf16)
    turn_cells()
    target_args = (target_out, target_in, target_sems)
    put_rows(embed_rows(), target_out)
    scatter_start(*target_args)
    for step in range(1, gx_n):
        feat_copy(step).start()
    feats[gx] = feat_out[gx]

    scatter_wait(*source_args)
    source_rows[...] = source_in[...].astype(f32).reshape(slots, embed).astype(bf16)
    scatter_wait(*valid_args)
    valid = valid_in[...].astype(f32).reshape(slots, valid_in.shape[2])[:, 0:1]
    for load in (loads[2], loads[3], loads[6], loads[7]):
        load.wait()
    predict = jnp.zeros((slots, embed), f32) + second_bias_ref[...]
    for tile in range(0, hidden_n, HIDDEN_TILE):
        part = pl.ds(tile, HIDDEN_TILE)
        pre = jnp.dot(source_rows[...], first[:, part], preferred_element_type=f32)
        pre = pre + first_bias_ref[:, part]
        sigma = jax.nn.sigmoid(pre)
        units = (pre * sigma).astype(bf16)
        hidden[part, :] = units.T
        steep[:, part] = sigma * (1.0 + pre * (1.0 - sigma))
        predict = predict + jnp.dot(units, second[part, :], preferred_element_type=f32)
    source_turned[...] = source_rows[...].T
    scatter_wait(*target_args)
    wanted = target_in[...].astype(f32).reshape(slots, embed)
    error[...] = (error_weight * (predict - wanted) * valid).astype(bf16)
    for tile in range(0, hidden_n, HIDDEN_TILE):
        part = pl.ds(tile, HIDDEN_TILE)
        slope[:, part] = (contract_cols(error[...], second[part, :]) * steep[:, part]).astype(bf16)
    span = embed // BACK_CHUNKS
    for group in range(BACK_CHUNKS):
        grad = contract_cols(slope[...], first[pl.ds(group * span, span), :])
        grad_out[group] = grad.reshape(devices, slot_rows, span).astype(bf16)
        scatter_start(grad_out.at[group], back.at[group], back_sems.at[group])
    results = [
        pltpu.make_async_copy(source_turned, source_hbm, save_sem.at[0]),
        pltpu.make_async_copy(hidden, hidden_hbm, save_sem.at[1]),
        pltpu.make_async_copy(error, error_hbm, save_sem.at[2]),
        pltpu.make_async_copy(slope, slope_hbm, save_sem.at[3]),
    ]
    for save in results:
        save.start()
    saves = saves + results

    def chip_at(step):
        return across(chip, step) * 2 + core

    sends = []

    def send(copy):
        copy.start()
        sends.append(copy)

    def share_copy(chunk, origin, target, slot):
        block = shared.at[chunk, origin]
        return remote(
            block, block, share_send.at[chunk, slot], share_recv.at[chunk, origin], target, gy
        )

    def part_of(chunk, block):
        total = jnp.zeros((part_rows, width), f32)
        for origin in range(gx_n):
            total = total + jnp.dot(
                feats[origin, block], shared[chunk, origin], preferred_element_type=f32
            )
        return total

    def part_copy(chunk, step):
        other = across(gy, step)
        return remote(
            parts.at[chunk, other],
            landed.at[chunk, step],
            part_send.at[chunk, step],
            part_recv.at[chunk, step],
            gx,
            other,
        )

    def out_copy(chunk, block_x, block_y, send_sem, target_x, target_y):
        block = summed_ref.at[chunk, block_x, block_y]
        return remote(
            block, block, send_sem, out_recv.at[chunk, block_x, block_y], target_x, target_y
        )

    def out_wait(chunk, block_x, block_y):
        out_copy(chunk, block_x, block_y, line_send.at[0, 0], partner, gy).wait_recv()

    near = [chip_at(step) for step in range(1, chips)]
    own = {}

    def back_event(group):
        scatter_wait(grad_out.at[group], back.at[group], back_sems.at[group])
        packed = back[group].astype(f32).reshape(slots, span).astype(bf16)
        mine = contract_rows(place[...], packed).astype(bf16)
        for piece in range(span // width):
            chunk = group * (span // width) + piece
            shared[chunk, gx] = mine[:, piece * width : (piece + 1) * width]
            for step in range(1, chips):
                send(share_copy(chunk, gx, chip_at(step), step))
            send(share_copy(chunk, gx, partner, 0))

    def share_event(chunk):
        for step in range(1, chips):
            origin = chip_at(step)
            share_copy(chunk, origin, partner, chips + step).wait_recv()
            send(share_copy(chunk, origin, partner, chips + step))

    def part_event(chunk):
        for step in range(chips):
            share_copy(chunk, chip_at(step) + 1 - 2 * core, partner, 0).wait_recv()
        if chunk == 0:
            for step in range(1, gx_n):
                feat_copy(step).wait()
        for step in range(1, gy_n):
            other = across(gy, step)
            parts[chunk, other] = part_of(chunk, other).astype(bf16)
            part_copy(chunk, step).start()
        own[chunk] = part_of(chunk, gy)

    def spread(chunk, line):
        block_y = across(gy, line)
        for slot, target in enumerate(near):
            send(out_copy(chunk, gx, block_y, plane_send.at[chunk, line, slot], target, gy))
        send(out_copy(chunk, gx, block_y, pair_send.at[chunk, line, 0], partner, gy))

    def total_event(chunk):
        total = own[chunk]
        for step in range(1, gy_n):
            part_copy(chunk, step).wait()
            total = total + landed[chunk, step].astype(f32)
        summed_ref[chunk, gx, gy] = total.astype(bf16)
        for step in range(1, gy_n):
            other = across(gy, step)
            send(out_copy(chunk, gx, gy, line_send.at[chunk, step], gx, other))
        spread(chunk, 0)

    def line_event(chunk, line):
        out_wait(chunk, gx, across(gy, line))
        spread(chunk, line)

    def near_event(chunk, line):
        block_y = across(gy, line)
        for slot, block_x in enumerate(near):
            out_wait(chunk, block_x, block_y)
            send(
                out_copy(
                    chunk, block_x, block_y, pair_send.at[chunk, line, 1 + slot], partner, gy
                )
            )

    def pair_event(chunk):
        for line in range(gy_n):
            for step in range(chips):
                out_wait(chunk, chip_at(step) + 1 - 2 * core, line)
        save = pltpu.make_async_copy(
            summed_ref.at[chunk], summed_hbm.at[chunk], save_sem.at[5 + chunk]
        )
        save.start()
        saves.append(save)

    events = []
    for chunk in range(CHUNKS):
        if chunk * BACK_CHUNKS % CHUNKS == 0:
            group = chunk * BACK_CHUNKS // CHUNKS
            events.append((6.0 + 1.4 * chunk, back_event, group))
        events.append((9.8 + 1.6 * chunk, share_event, chunk))
        events.append((11.2 + 1.6 * chunk, part_event, chunk))
        base = 16.0 + 2.6 * chunk
        events.append((base, total_event, chunk))
        events.append((base + 3.2, near_event, chunk, 0))
        for line in range(1, gy_n):
            events.append((base + 3.0 + 0.5 * line, line_event, chunk, line))
            events.append((base + 6.0 + 0.5 * line, near_event, chunk, line))
        events.append((base + 12.0, pair_event, chunk))
    for event in sorted(events, key=lambda event: event[0]):
        event[1](*event[2:])
    for copy in sends + unsent:
        copy.wait_send()
    for step in range(STEPS):
        for inside, side in edges:
            @pl.when(inside)
            def _():
                halo_copy(step, side).wait_send()

    for save in saves:
        save.wait()


def finish_kernel(*refs):
    sources, results, landings, outs = refs[:5], refs[5:10], refs[10:15], refs[15:20]
    load_sem, save_sem = refs[20:]
    source, hidden, error, slope, summed = landings
    first, first_bias, second, second_bias, patch = outs
    f32 = jnp.float32
    saves = []

    def load(which, index, slot):
        copy = pltpu.make_async_copy(
            sources[which].at[index], landings[which].at[index], load_sem.at[slot]
        )
        copy.start()
        return copy

    def save(which, index):
        copy = pltpu.make_async_copy(
            outs[which].at[index], results[which].at[index], save_sem.at[len(saves)]
        )
        copy.start()
        saves.append(copy)

    def pieces(size):
        return [pl.ds(i * (size // FINISH_STEPS), size // FINISH_STEPS) for i in range(FINISH_STEPS)]

    everything = slice(None)
    hidden_pieces = pieces(hidden.shape[0])
    patch_pieces = pieces(patch.shape[0])
    error_load = load(2, everything, 0)
    hidden_loads = [load(1, piece, 1 + i) for i, piece in enumerate(hidden_pieces)]
    slope_load = load(3, everything, 1 + FINISH_STEPS)
    source_load = load(0, everything, 2 + FINISH_STEPS)
    summed_loads = [
        load(4, (everything, piece), 3 + FINISH_STEPS + i) for i, piece in enumerate(patch_pieces)
    ]
    error_load.wait()
    for piece, waiting in zip(hidden_pieces, hidden_loads):
        waiting.wait()
        second[0, piece, :] = jnp.dot(hidden[piece, :], error[...], preferred_element_type=f32)
        save(2, (0, piece))
    second_bias[...] = jnp.sum(error[...].astype(f32), axis=0, keepdims=True)
    save(3, everything)
    slope_load.wait()
    source_load.wait()
    for piece in pieces(source.shape[0]):
        first[0, piece, :] = jnp.dot(source[piece, :], slope[...], preferred_element_type=f32)
        save(0, (0, piece))
    first_bias[...] = jnp.sum(slope[...].astype(f32), axis=0, keepdims=True)
    save(1, everything)
    width = summed.shape[2]
    for piece, waiting in zip(patch_pieces, summed_loads):
        waiting.wait()
        for chunk in range(summed.shape[0]):
            patch[piece, chunk * width : (chunk + 1) * width] = summed[chunk, piece, :].astype(f32)
        save(4, piece)
    for waiting in saves:
        waiting.wait()


def finish(*values):
    embed, slots = values[0].shape
    hidden_n = values[1].shape[0]
    features = values[4].shape[1]
    f32 = jnp.float32
    shapes = [
        (1, embed, hidden_n),
        (1, hidden_n),
        (1, hidden_n, embed),
        (1, embed),
        (features, embed),
    ]
    anywhere = pl.BlockSpec(memory_space=pl.ANY)
    return pl.pallas_call(
        finish_kernel,
        out_shape=[jax.ShapeDtypeStruct(shape, f32) for shape in shapes],
        in_specs=[anywhere] * 5,
        out_specs=[anywhere] * 5,
        scratch_shapes=[pltpu.VMEM(value.shape, value.dtype) for value in values]
        + [pltpu.VMEM(shape, f32) for shape in shapes]
        + [
            pltpu.SemaphoreType.DMA((3 + 2 * FINISH_STEPS,)),
            pltpu.SemaphoreType.DMA((2 + 3 * FINISH_STEPS,)),
        ],
        compiler_params=pltpu.CompilerParams(vmem_limit_bytes=62 * 1024 * 1024),
    )(*values)


def per_device(fields, patch_weight, trainer_of, lag_index, w_in, b_in, w_out, b_out):
    gx_n, gy_n = lax.axis_size("gx"), lax.axis_size("gy")
    devices, chips = gx_n * gy_n, gx_n // 2
    fields_n, size_x, size_y, size_z = fields.shape
    features, embed = patch_weight.shape
    hidden_n = w_in.shape[2]
    rows = lag_index.size
    blocks = rows // BLOCK_ROWS
    slot_rows = max(8, 2 * blocks // devices * BLOCK_ROWS)
    slots = devices * slot_rows
    columns = lag_index.shape[0] * lag_index.shape[1]
    part_rows = features // devices
    width = embed // CHUNKS
    bf16, f32 = jnp.bfloat16, jnp.float32
    dma = pltpu.SemaphoreType.DMA
    vmem = pltpu.VMEM
    anywhere = pl.BlockSpec(memory_space=pl.ANY)
    padded = (fields_n, size_x + 4, size_y + 2 * PAD, size_z)
    sides = (STEPS, 2, fields_n, 2, size_y, size_z)
    faces = (STEPS, 2, fields_n, size_x, 2, size_z)
    source_shape = (devices, slot_rows, embed)
    valid_shape = (devices, slot_rows, 128)
    feat_shape = (gx_n, gy_n, part_rows, rows)
    block_shape = (CHUNKS, gx_n, gy_n, part_rows, width)
    new_fields, summed, source, hidden, error, slope = pl.pallas_call(
        functools.partial(step_kernel, gx_n, gy_n),
        out_shape=[
            jax.ShapeDtypeStruct(fields.shape, f32),
            jax.ShapeDtypeStruct(block_shape, bf16),
            jax.ShapeDtypeStruct((embed, slots), bf16),
            jax.ShapeDtypeStruct((hidden_n, slots), bf16),
            jax.ShapeDtypeStruct((slots, embed), bf16),
            jax.ShapeDtypeStruct((slots, hidden_n), bf16),
        ],
        in_specs=[anywhere] * 8,
        out_specs=[anywhere] * 6,
        scratch_shapes=[
            vmem(padded, f32),
            vmem(padded, f32),
            vmem(padded, f32),
            vmem(fields.shape, f32),
            vmem(block_shape, bf16),
            vmem((1, blocks), jnp.int32),
            vmem(lag_index.shape, jnp.int32),
            vmem(b_in.shape, f32),
            vmem(b_out.shape, f32),
            vmem(valid_shape, bf16),
            vmem(valid_shape, bf16),
            vmem(sides, bf16),
            vmem(sides, bf16),
            vmem(faces, FACE_TYPE),
            vmem(faces, FACE_TYPE),
            vmem((columns * size_z, PATCH * rows), bf16),
            vmem((features // PATCH, columns * size_z), bf16),
            vmem((features, rows), f32),
            vmem((slots, rows), bf16),
            vmem((features, embed), bf16),
            vmem((embed, hidden_n), bf16),
            vmem((hidden_n, embed), bf16),
            vmem(source_shape, bf16),
            vmem(source_shape, bf16),
            vmem(source_shape, bf16),
            vmem(source_shape, bf16),
            vmem(feat_shape, bf16),
            vmem(feat_shape, bf16),
            vmem((slots, embed), bf16),
            vmem((embed, slots), bf16),
            vmem((hidden_n, slots), bf16),
            vmem((slots, hidden_n), f32),
            vmem((slots, embed), bf16),
            vmem((slots, hidden_n), bf16),
            vmem((BACK_CHUNKS, devices, slot_rows, embed // BACK_CHUNKS), bf16),
            vmem((BACK_CHUNKS, devices, slot_rows, embed // BACK_CHUNKS), bf16),
            vmem((CHUNKS, gx_n, rows, width), bf16),
            vmem((CHUNKS, gy_n, part_rows, width), bf16),
            vmem((CHUNKS, gy_n, part_rows, width), bf16),
            dma((8,)),
            dma((5 + CHUNKS,)),
            dma((2,)),
            dma((STEPS, 4)),
            dma((STEPS, 4)),
            dma((2,)),
            dma((2,)),
            dma((gx_n,)),
            dma((gx_n,)),
            dma((BACK_CHUNKS, 2)),
            dma((CHUNKS, 2 * chips)),
            dma((CHUNKS, gx_n)),
            dma((CHUNKS, gy_n)),
            dma((CHUNKS, gy_n)),
            dma((CHUNKS, gy_n)),
            dma((CHUNKS, gy_n, chips)),
            dma((CHUNKS, gy_n, chips)),
            dma((CHUNKS, gx_n, gy_n)),
        ],
        compiler_params=pltpu.CompilerParams(
            collective_id=0, has_side_effects=True, vmem_limit_bytes=62 * 1024 * 1024
        ),
    )(fields, patch_weight, trainer_of.T, lag_index, w_in, b_in, w_out, b_out)
    first_grad, first_bias_grad, second_grad, second_bias_grad, patch_gradient = finish(
        source, hidden, error, slope, summed.reshape(CHUNKS, features, width)
    )
    return (
        new_fields,
        patch_gradient,
        first_grad,
        first_bias_grad,
        second_grad,
        second_bias_grad,
    )


def solution(mesh):
    in_specs = (
        P(None, "gx", "gy", None),
        P(),
        P(("gx", "gy"), None),
        P("gx", "gy", None),
        P(("gx", "gy"), None, None),
        P(("gx", "gy"), None),
        P(("gx", "gy"), None, None),
        P(("gx", "gy"), None),
    )
    out_specs = (
        P(None, "gx", "gy", None),
        P(),
        P(("gx", "gy"), None, None),
        P(("gx", "gy"), None),
        P(("gx", "gy"), None, None),
        P(("gx", "gy"), None),
    )
    return jax.shard_map(
        per_device, mesh=mesh, in_specs=in_specs, out_specs=out_specs, check_vma=False
    )
```

```python
import functools

import jax
import jax.numpy as jnp
from jax import lax
from jax.experimental import pallas as pl
from jax.experimental.pallas import tpu as pltpu
from jax.sharding import PartitionSpec as P

FIELDS = 5
PATCH = 8
STEPS = 3
BLOCK_ROWS = 2
PAD = 8
FACE_TYPE = jnp.float32
CHUNKS = 2
BACK_CHUNKS = 2
HIDDEN_TILE = 512
FINISH_STEPS = 4


time_step = 0.2
viscosity = 0.5
drift_x = 0.6
drift_y = -0.4
drift_z = 0.3
error_weight = 0.0625


def contract_rows(left, right):
    return lax.dot_general(
        left, right, (((0,), (0,)), ((), ())), preferred_element_type=jnp.float32
    )


def contract_cols(left, right):
    return lax.dot_general(
        left, right, (((1,), (1,)), ((), ())), preferred_element_type=jnp.float32
    )


def my_place():
    return lax.axis_index("gx"), lax.axis_index("gy")


def across(place, step):
    bit = 1
    while bit <= step:
        if step & bit:
            place = place + bit - 2 * bit * lax.rem(place // bit, 2)
        bit *= 2
    return place


def remote(src, dst, send_sem, recv_sem, gx, gy):
    return pltpu.make_async_remote_copy(
        src_ref=src,
        dst_ref=dst,
        send_sem=send_sem,
        recv_sem=recv_sem,
        device_id=(gx, gy),
        device_id_type=pl.DeviceIdType.MESH,
    )


def step_kernel(
    gx_n,
    gy_n,
    fields_hbm,
    weight_hbm,
    owner_hbm,
    lag_hbm,
    first_hbm,
    first_bias_hbm,
    second_hbm,
    second_bias_hbm,
    fields_out_hbm,
    summed_hbm,
    source_hbm,
    hidden_hbm,
    error_hbm,
    slope_hbm,
    state_0,
    state_1,
    state_2,
    out_ref,
    summed_ref,
    owner_ref,
    lag_ref,
    first_bias_ref,
    second_bias_ref,
    valid_out,
    valid_in,
    side_out,
    side_in,
    face_out,
    face_in,
    swap,
    cells,
    turned,
    turned_late,
    place,
    weight,
    first,
    second,
    source_out,
    source_in,
    target_out,
    target_in,
    feat_out,
    feats,
    source_rows,
    source_turned,
    hidden,
    steep,
    error,
    slope,
    grad_out,
    back,
    shared,
    parts,
    landed,
    load_sem,
    save_sem,
    valid_sems,
    halo_send,
    halo_recv,
    source_sems,
    target_sems,
    feat_send,
    feat_recv,
    back_sems,
    share_send,
    share_recv,
    part_send,
    part_recv,
    line_send,
    plane_send,
    pair_send,
    out_recv,
):
    gx, gy = my_place()
    me = gx * gy_n + gy
    devices = gx_n * gy_n
    chips = gx_n // 2
    chip, core = gx // 2, lax.rem(gx, 2)
    partner = gx + 1 - 2 * core
    states = (state_0, state_1, state_2)
    _, size_x, size_y, size_z = fields_hbm.shape
    inner = pl.ds(PAD, size_y)
    embed = weight.shape[1]
    slot_rows = source_out.shape[1]
    count_x, count_y, count_z = lag_ref.shape
    columns = count_x * count_y
    kinds = FIELDS * PATCH * PATCH
    rows = turned.shape[1]
    hidden_n = hidden.shape[0]
    width = embed // CHUNKS
    f32, bf16 = jnp.float32, jnp.bfloat16

    barrier = pltpu.get_barrier_semaphore()

    def greet(step, carry):
        other = lax.rem(me + step, devices)
        pl.semaphore_signal(
            barrier,
            inc=1,
            device_id=(other // gy_n, lax.rem(other, gy_n)),
            device_id_type=pl.DeviceIdType.MESH,
        )
        return carry

    lax.fori_loop(1, devices, greet, 0)
    loads = [
        pltpu.make_async_copy(
            fields_hbm, state_0.at[:, pl.ds(2, size_x), inner, :], load_sem.at[0]
        ),
        pltpu.make_async_copy(weight_hbm, weight, load_sem.at[1]),
        pltpu.make_async_copy(first_hbm.at[0], first, load_sem.at[2]),
        pltpu.make_async_copy(second_hbm.at[0], second, load_sem.at[3]),
        pltpu.make_async_copy(owner_hbm, owner_ref, load_sem.at[4]),
        pltpu.make_async_copy(lag_hbm, lag_ref, load_sem.at[5]),
        pltpu.make_async_copy(first_bias_hbm, first_bias_ref, load_sem.at[6]),
        pltpu.make_async_copy(second_bias_hbm, second_bias_ref, load_sem.at[7]),
    ]
    for load in loads:
        load.start()

    edges = ((gx > 0, 0), (gx < gx_n - 1, 1), (gy > 0, 2), (gy < gy_n - 1, 3))
    pl.semaphore_wait(barrier, devices - 1)

    def halo_ends(side):
        if side < 2:
            return side_out, side_in, (gx - 1 if side == 0 else gx + 1, gy)
        return face_out, face_in, (gx, gy - 1 if side == 2 else gy + 1)

    def halo_copy(step, side):
        out, landing, target = halo_ends(side)
        return remote(
            out.at[step, side % 2],
            landing.at[step, 1 - side % 2],
            halo_send.at[step, side],
            halo_recv.at[step, side ^ 1],
            *target
        )

    def halo_start(step):
        state = states[step]
        for side, (inside, _) in enumerate(edges):
            @pl.when(inside)
            def _():
                if side < 2:
                    first = 2 if side == 0 else size_x
                    values = state[:, pl.ds(first, 2), inner, :]
                else:
                    first = PAD if side == 2 else PAD + size_y - 2
                    values = state[:, pl.ds(2, size_x), pl.ds(first, 2), :]
                out = halo_ends(side)[0]
                out[step, side % 2] = values.astype(out.dtype)
                halo_copy(step, side).start()

    def halo_wait(step):
        state = states[step]
        for side, (inside, _) in enumerate(edges):
            @pl.when(inside)
            def _():
                landing = halo_ends(side)[1]
                block = landing.at[step, side % 2]
                remote(
                    block, block, halo_send.at[step, side], halo_recv.at[step, side], gx, gy
                ).wait_recv()
                values = landing[step, side % 2].astype(jnp.float32)
                if side < 2:
                    state[:, pl.ds(0 if side == 0 else size_x + 2, 2), inner, :] = values
                else:
                    first = PAD - 2 if side == 2 else PAD + size_y
                    state[:, pl.ds(2, size_x), pl.ds(first, 2), :] = values

    def advance_part(step, first_plane, planes, pieces_of, count):
        state = states[step]
        lane = lax.broadcasted_iota(jnp.int32, (count, size_z), 1)

        def plane(i, carry):
            for ahead, first_row in pieces_of:
                piece(i + ahead, first_row)
            return carry

        def piece(i, first_row):
            here = pl.ds(PAD + first_row, count)

            def pieces(field):
                middle = state[field, i + 2, here, :]
                around = []
                around.append([state[field, i + k, here, :] for k in (0, 1, 3, 4)])
                around.append(
                    [state[field, i + 2, pl.ds(PAD + first_row + k, count), :] for k in (-2, -1, 1, 2)]
                )
                around.append(
                    [
                        jnp.where(lane < 2, 0.0, pltpu.roll(middle, 2, 1)),
                        jnp.where(lane < 1, 0.0, pltpu.roll(middle, 1, 1)),
                        jnp.where(lane >= size_z - 1, 0.0, pltpu.roll(middle, size_z - 1, 1)),
                        jnp.where(lane >= size_z - 2, 0.0, pltpu.roll(middle, size_z - 2, 1)),
                    ]
                )
                slopes = [(a - d) + 8.0 * (c - b) for a, b, c, d in around]
                near = sum(b + c for a, b, c, d in around)
                far = sum(a + d for a, b, c, d in around)
                change = viscosity * (16.0 * near - far - 90.0 * middle)
                change = change - (
                    drift_x * slopes[0] + drift_y * slopes[1] + drift_z * slopes[2]
                )
                return middle, slopes, change

            def put(field, value):
                if step < STEPS - 1:
                    states[step + 1][field, i + 2, here, :] = value
                else:
                    out_ref[field, i, pl.ds(first_row, count), :] = value

            scale = time_step / 12.0
            middle_p, slopes_p, change_p = pieces(4)
            spread = 0.0
            for axis in range(3):
                middle, slopes, change = pieces(1 + axis)
                spread = spread + slopes[axis]
                put(1 + axis, middle + scale * (change - slopes_p[axis]))
            put(4, middle_p + scale * (change_p - spread))
            middle, slopes, change = pieces(0)
            put(0, middle + scale * (change - spread))

        lax.fori_loop(first_plane, first_plane + planes, plane, 0)

    def advance_inside(step):
        advance_part(step, 2, size_x - 4, ((0, PAD),), size_y - 2 * PAD)

    def advance_edges(step):
        advance_part(step, 0, 2, ((0, 0), (size_x - 2, 0)), size_y)
        advance_part(step, 2, size_x - 4, ((0, 0), (0, size_y - PAD)), PAD)

    def column_cells(state, offset_x, offset_y, column):
        first_x = offset_x + column // count_y * PATCH
        first_y = offset_y + column % count_y * PATCH
        return state[:, pl.ds(first_x, PATCH), pl.ds(first_y, PATCH), :].reshape(kinds, size_z)

    def turn_cells(turned):
        for offset in range(PATCH):
            turned[pl.ds(offset, kinds, stride=PATCH), :] = jnp.dot(
                cells[...],
                swap[:, pl.ds(offset * rows, rows)],
                preferred_element_type=f32,
            )

    def embed_rows(turned):
        return contract_rows(turned[...].astype(bf16), weight[...]).astype(bf16)

    def scatter(step, stage, landing, sems):
        other = lax.rem(me + step, devices)
        return remote(
            stage.at[other],
            landing.at[me],
            sems.at[0],
            sems.at[1],
            other // gy_n,
            lax.rem(other, gy_n),
        )

    def scatter_start(stage, landing, sems):
        def start(step, carry):
            scatter(step, stage, landing, sems).start()
            return carry

        lax.fori_loop(1, devices, start, 0)
        landing[me] = stage[me]

    def scatter_all(stage, landing, sems):
        others = pl.ds(0, devices - 1)
        return remote(stage.at[others], landing.at[others], sems.at[0], sems.at[1], partner, gy)

    def scatter_wait(*args):
        scatter_all(*args).wait_recv()
        unsent.append(scatter_all(*args))

    unsent = []

    def put_rows(values, stage):
        packed = jnp.dot(place[...], values, preferred_element_type=f32)
        stage[...] = packed.reshape(stage.shape).astype(bf16)

    loads[0].wait()
    halo_start(0)
    for state in states:
        for inside, side in edges:
            @pl.when(jnp.logical_not(inside))
            def _():
                if side < 2:
                    plane = pl.ds(0 if side == 0 else size_x + 2, 2)
                    state[:, plane, inner, :] = jnp.zeros((FIELDS, 2, size_y, size_z), jnp.float32)
                else:
                    strip = pl.ds(0 if side == 2 else PAD + size_y, PAD)
                    state[:, pl.ds(2, size_x), strip, :] = jnp.zeros(
                        (FIELDS, size_x, PAD, size_z), jnp.float32
                    )

    place_of = lax.broadcasted_iota(jnp.int32, (1, PATCH * rows), 1)
    column_of = lax.rem(place_of, rows) // count_z
    cell_of = column_of * size_z + lax.rem(place_of, count_z) * PATCH + place_of // rows
    for column in range(columns):
        row_of = lax.broadcasted_iota(jnp.int32, (size_z, PATCH * rows), 0) + column * size_z
        swap[pl.ds(column * size_z, size_z), :] = jnp.where(row_of == cell_of, 1.0, 0.0).astype(
            jnp.bfloat16
        )

    loads[4].wait()
    owner = owner_ref[...].astype(f32)
    blocks = owner.shape[1]
    tall = lax.broadcasted_iota(jnp.int32, (devices, blocks), 0).astype(f32)
    onehot = jnp.where(owner == tall, 1.0, 0.0)
    before = jnp.where(
        lax.broadcasted_iota(jnp.int32, (blocks, blocks), 0)
        < lax.broadcasted_iota(jnp.int32, (blocks, blocks), 1),
        1.0,
        0.0,
    )
    ahead = jnp.dot(onehot.astype(bf16), before.astype(bf16), preferred_element_type=f32)
    rank = jnp.sum(ahead * onehot, axis=0, keepdims=True)
    block_slot = owner * float(slot_rows // BLOCK_ROWS) + rank
    slots = place.shape[0]
    slot_block = lax.broadcasted_iota(jnp.int32, (slots, blocks), 0) // BLOCK_ROWS
    block_place = jnp.where(block_slot == slot_block.astype(f32), 1.0, 0.0)
    spread_rows = jnp.where(
        lax.broadcasted_iota(jnp.int32, (blocks, rows), 1) // BLOCK_ROWS
        == lax.broadcasted_iota(jnp.int32, (blocks, rows), 0),
        1.0,
        0.0,
    )
    row_place = jnp.dot(
        block_place.astype(bf16), spread_rows.astype(bf16), preferred_element_type=f32
    )
    same = lax.rem(lax.broadcasted_iota(jnp.int32, (slots, rows), 0), BLOCK_ROWS) == lax.rem(
        lax.broadcasted_iota(jnp.int32, (slots, rows), 1), BLOCK_ROWS
    )
    place[...] = jnp.where(same, row_place, 0.0).astype(bf16)
    filled = jnp.sum(place[...].astype(f32), axis=1, keepdims=True)
    filled = jnp.broadcast_to(filled, (slots, valid_out.shape[2]))
    valid_out[...] = filled.reshape(valid_out.shape).astype(bf16)
    valid_args = (valid_out, valid_in, valid_sems)
    scatter_start(*valid_args)
    advance_inside(0)
    halo_wait(0)
    advance_edges(0)
    halo_start(1)
    advance_inside(1)
    halo_wait(1)
    advance_edges(1)
    halo_start(2)
    stretch = jnp.where(
        lax.broadcasted_iota(jnp.int32, (count_z, size_z), 1) // PATCH
        == lax.broadcasted_iota(jnp.int32, (count_z, size_z), 0),
        1.0,
        0.0,
    ).astype(bf16)
    loads[5].wait()
    for column_x in range(count_x):
        lag = lag_ref[column_x].astype(f32).astype(bf16)
        lag = jnp.dot(lag, stretch, preferred_element_type=f32)
        for column_y in range(count_y):
            column = column_x * count_y + column_y
            early = column_cells(state_1, 2, PAD, column)
            late = column_cells(state_2, 2, PAD, column)
            chosen = jnp.where(lag[column_y : column_y + 1, :] > 0.5, late, early)
            cells[:, pl.ds(column * size_z, size_z)] = chosen.astype(bf16)
    turn_cells(turned)
    loads[1].wait()
    source = embed_rows(turned)
    source_args = (source_out, source_in, source_sems)
    put_rows(source, source_out)
    scatter_start(*source_args)

    def feat_copy(step):
        other = lax.rem(gx + step, gx_n)
        return remote(
            feat_out.at[other], feats.at[gx], feat_send.at[step], feat_recv.at[step], other, gy
        )

    advance_inside(2)
    halo_wait(2)
    advance_edges(2)
    saves = [pltpu.make_async_copy(out_ref, fields_out_hbm, save_sem.at[4])]
    saves[0].start()
    for column in range(columns):
        cells[:, pl.ds(column * size_z, size_z)] = column_cells(out_ref, 0, 0, column).astype(bf16)
    turn_cells(turned_late)
    target_args = (target_out, target_in, target_sems)
    put_rows(embed_rows(turned_late), target_out)
    scatter_start(*target_args)
    part_rows = feats.shape[2]
    for block in range(devices):
        feat_out[block // gy_n, block % gy_n] = turned[
            pl.ds(block * part_rows, part_rows), :
        ].astype(bf16)
    for step in range(1, gx_n):
        feat_copy(step).start()
    feats[gx] = feat_out[gx]

    scatter_wait(*source_args)
    source_rows[...] = source_in[...].astype(f32).reshape(slots, embed).astype(bf16)
    scatter_wait(*valid_args)
    valid = valid_in[...].astype(f32).reshape(slots, valid_in.shape[2])[:, 0:1]
    for load in (loads[2], loads[3], loads[6], loads[7]):
        load.wait()
    predict = jnp.zeros((slots, embed), f32) + second_bias_ref[...]
    for tile in range(0, hidden_n, HIDDEN_TILE):
        part = pl.ds(tile, HIDDEN_TILE)
        pre = jnp.dot(source_rows[...], first[:, part], preferred_element_type=f32)
        pre = pre + first_bias_ref[:, part]
        sigma = jax.nn.sigmoid(pre)
        units = (pre * sigma).astype(bf16)
        hidden[part, :] = units.T
        steep[:, part] = sigma * (1.0 + pre * (1.0 - sigma))
        predict = predict + jnp.dot(units, second[part, :], preferred_element_type=f32)
    source_turned[...] = source_rows[...].T
    scatter_wait(*target_args)
    wanted = target_in[...].astype(f32).reshape(slots, embed)
    error[...] = (error_weight * (predict - wanted) * valid).astype(bf16)
    for tile in range(0, hidden_n, HIDDEN_TILE):
        part = pl.ds(tile, HIDDEN_TILE)
        slope[:, part] = (contract_cols(error[...], second[part, :]) * steep[:, part]).astype(bf16)
    span = embed // BACK_CHUNKS
    for group in range(BACK_CHUNKS):
        grad = contract_cols(slope[...], first[pl.ds(group * span, span), :])
        grad_out[group] = grad.reshape(devices, slot_rows, span).astype(bf16)
        scatter_start(grad_out.at[group], back.at[group], back_sems.at[group])
    results = [
        pltpu.make_async_copy(source_turned, source_hbm, save_sem.at[0]),
        pltpu.make_async_copy(hidden, hidden_hbm, save_sem.at[1]),
        pltpu.make_async_copy(error, error_hbm, save_sem.at[2]),
        pltpu.make_async_copy(slope, slope_hbm, save_sem.at[3]),
    ]
    for save in results:
        save.start()
    saves = saves + results

    def chip_at(step):
        return across(chip, step) * 2 + core

    sends = []

    def send(copy):
        copy.start()
        sends.append(copy)

    def share_copy(chunk, origin, target, slot):
        block = shared.at[chunk, origin]
        return remote(
            block, block, share_send.at[chunk, slot], share_recv.at[chunk, origin], target, gy
        )

    def part_of(chunk, block):
        total = jnp.zeros((part_rows, width), f32)
        for origin in range(gx_n):
            total = total + jnp.dot(
                feats[origin, block], shared[chunk, origin], preferred_element_type=f32
            )
        return total

    def part_copy(chunk, step):
        other = across(gy, step)
        return remote(
            parts.at[chunk, other],
            landed.at[chunk, step],
            part_send.at[chunk, step],
            part_recv.at[chunk, step],
            gx,
            other,
        )

    def out_copy(chunk, block_x, block_y, send_sem, target_x, target_y):
        block = summed_ref.at[chunk, block_x, block_y]
        return remote(
            block, block, send_sem, out_recv.at[chunk, block_x, block_y], target_x, target_y
        )

    def out_wait(chunk, block_x, block_y):
        out_copy(chunk, block_x, block_y, line_send.at[0, 0], partner, gy).wait_recv()

    near = [chip_at(step) for step in range(1, chips)]
    own = {}

    def back_event(group):
        scatter_wait(grad_out.at[group], back.at[group], back_sems.at[group])
        packed = back[group].astype(f32).reshape(slots, span).astype(bf16)
        mine = contract_rows(place[...], packed).astype(bf16)
        for piece in range(span // width):
            chunk = group * (span // width) + piece
            shared[chunk, gx] = mine[:, piece * width : (piece + 1) * width]
            for step in range(1, chips):
                send(share_copy(chunk, gx, chip_at(step), step))
            send(share_copy(chunk, gx, partner, 0))

    def share_event(chunk):
        for step in range(1, chips):
            origin = chip_at(step)
            share_copy(chunk, origin, partner, chips + step).wait_recv()
            send(share_copy(chunk, origin, partner, chips + step))

    def part_event(chunk):
        for step in range(chips):
            share_copy(chunk, chip_at(step) + 1 - 2 * core, partner, 0).wait_recv()
        if chunk == 0:
            for step in range(1, gx_n):
                feat_copy(step).wait()
        for step in range(1, gy_n):
            other = across(gy, step)
            parts[chunk, other] = part_of(chunk, other).astype(bf16)
            part_copy(chunk, step).start()
        own[chunk] = part_of(chunk, gy)

    def spread(chunk, line):
        block_y = across(gy, line)
        for slot, target in enumerate(near):
            send(out_copy(chunk, gx, block_y, plane_send.at[chunk, line, slot], target, gy))
        send(out_copy(chunk, gx, block_y, pair_send.at[chunk, line, 0], partner, gy))

    def total_event(chunk):
        total = own[chunk]
        for step in range(1, gy_n):
            part_copy(chunk, step).wait()
            total = total + landed[chunk, step].astype(f32)
        summed_ref[chunk, gx, gy] = total.astype(bf16)
        for step in range(1, gy_n):
            other = across(gy, step)
            send(out_copy(chunk, gx, gy, line_send.at[chunk, step], gx, other))
        spread(chunk, 0)

    def line_event(chunk, line):
        out_wait(chunk, gx, across(gy, line))
        spread(chunk, line)

    def near_event(chunk, line):
        block_y = across(gy, line)
        for slot, block_x in enumerate(near):
            out_wait(chunk, block_x, block_y)
            send(
                out_copy(
                    chunk, block_x, block_y, pair_send.at[chunk, line, 1 + slot], partner, gy
                )
            )

    def pair_event(chunk):
        for line in range(gy_n):
            for step in range(chips):
                out_wait(chunk, chip_at(step) + 1 - 2 * core, line)
        save = pltpu.make_async_copy(
            summed_ref.at[chunk], summed_hbm.at[chunk], save_sem.at[5 + chunk]
        )
        save.start()
        saves.append(save)

    events = []
    for chunk in range(CHUNKS):
        if chunk * BACK_CHUNKS % CHUNKS == 0:
            group = chunk * BACK_CHUNKS // CHUNKS
            events.append((6.0 + 1.4 * chunk, back_event, group))
        events.append((9.8 + 1.6 * chunk, share_event, chunk))
        events.append((11.2 + 1.6 * chunk, part_event, chunk))
        base = 16.0 + 2.6 * chunk
        events.append((base, total_event, chunk))
        events.append((base + 3.2, near_event, chunk, 0))
        for line in range(1, gy_n):
            events.append((base + 3.0 + 0.5 * line, line_event, chunk, line))
            events.append((base + 6.0 + 0.5 * line, near_event, chunk, line))
        events.append((base + 12.0, pair_event, chunk))
    for event in sorted(events, key=lambda event: event[0]):
        event[1](*event[2:])
    for copy in sends + unsent:
        copy.wait_send()
    for step in range(STEPS):
        for inside, side in edges:
            @pl.when(inside)
            def _():
                halo_copy(step, side).wait_send()

    for save in saves:
        save.wait()


def finish_kernel(*refs):
    sources, results, landings, outs = refs[:5], refs[5:10], refs[10:15], refs[15:20]
    load_sem, save_sem = refs[20:]
    source, hidden, error, slope, summed = landings
    first, first_bias, second, second_bias, patch = outs
    f32 = jnp.float32
    saves = []

    def load(which, index, slot):
        copy = pltpu.make_async_copy(
            sources[which].at[index], landings[which].at[index], load_sem.at[slot]
        )
        copy.start()
        return copy

    def save(which, index):
        copy = pltpu.make_async_copy(
            outs[which].at[index], results[which].at[index], save_sem.at[len(saves)]
        )
        copy.start()
        saves.append(copy)

    def pieces(size):
        return [pl.ds(i * (size // FINISH_STEPS), size // FINISH_STEPS) for i in range(FINISH_STEPS)]

    everything = slice(None)
    hidden_pieces = pieces(hidden.shape[0])
    patch_pieces = pieces(patch.shape[0])
    error_load = load(2, everything, 0)
    hidden_loads = [load(1, piece, 1 + i) for i, piece in enumerate(hidden_pieces)]
    slope_load = load(3, everything, 1 + FINISH_STEPS)
    source_load = load(0, everything, 2 + FINISH_STEPS)
    summed_loads = [
        load(4, (everything, piece), 3 + FINISH_STEPS + i) for i, piece in enumerate(patch_pieces)
    ]
    error_load.wait()
    for piece, waiting in zip(hidden_pieces, hidden_loads):
        waiting.wait()
        second[0, piece, :] = jnp.dot(hidden[piece, :], error[...], preferred_element_type=f32)
        save(2, (0, piece))
    second_bias[...] = jnp.sum(error[...].astype(f32), axis=0, keepdims=True)
    save(3, everything)
    slope_load.wait()
    source_load.wait()
    for piece in pieces(source.shape[0]):
        first[0, piece, :] = jnp.dot(source[piece, :], slope[...], preferred_element_type=f32)
        save(0, (0, piece))
    first_bias[...] = jnp.sum(slope[...].astype(f32), axis=0, keepdims=True)
    save(1, everything)
    width = summed.shape[2]
    for piece, waiting in zip(patch_pieces, summed_loads):
        waiting.wait()
        for chunk in range(summed.shape[0]):
            patch[piece, chunk * width : (chunk + 1) * width] = summed[chunk, piece, :].astype(f32)
        save(4, piece)
    for waiting in saves:
        waiting.wait()


def finish(*values):
    embed, slots = values[0].shape
    hidden_n = values[1].shape[0]
    features = values[4].shape[1]
    f32 = jnp.float32
    shapes = [
        (1, embed, hidden_n),
        (1, hidden_n),
        (1, hidden_n, embed),
        (1, embed),
        (features, embed),
    ]
    anywhere = pl.BlockSpec(memory_space=pl.ANY)
    return pl.pallas_call(
        finish_kernel,
        out_shape=[jax.ShapeDtypeStruct(shape, f32) for shape in shapes],
        in_specs=[anywhere] * 5,
        out_specs=[anywhere] * 5,
        scratch_shapes=[pltpu.VMEM(value.shape, value.dtype) for value in values]
        + [pltpu.VMEM(shape, f32) for shape in shapes]
        + [
            pltpu.SemaphoreType.DMA((3 + 2 * FINISH_STEPS,)),
            pltpu.SemaphoreType.DMA((2 + 3 * FINISH_STEPS,)),
        ],
        compiler_params=pltpu.CompilerParams(vmem_limit_bytes=62 * 1024 * 1024),
    )(*values)


def per_device(fields, patch_weight, trainer_of, lag_index, w_in, b_in, w_out, b_out):
    gx_n, gy_n = lax.axis_size("gx"), lax.axis_size("gy")
    devices, chips = gx_n * gy_n, gx_n // 2
    fields_n, size_x, size_y, size_z = fields.shape
    features, embed = patch_weight.shape
    hidden_n = w_in.shape[2]
    rows = lag_index.size
    blocks = rows // BLOCK_ROWS
    slot_rows = max(8, 2 * blocks // devices * BLOCK_ROWS)
    slots = devices * slot_rows
    columns = lag_index.shape[0] * lag_index.shape[1]
    part_rows = features // devices
    width = embed // CHUNKS
    bf16, f32 = jnp.bfloat16, jnp.float32
    dma = pltpu.SemaphoreType.DMA
    vmem = pltpu.VMEM
    anywhere = pl.BlockSpec(memory_space=pl.ANY)
    padded = (fields_n, size_x + 4, size_y + 2 * PAD, size_z)
    sides = (STEPS, 2, fields_n, 2, size_y, size_z)
    faces = (STEPS, 2, fields_n, size_x, 2, size_z)
    source_shape = (devices, slot_rows, embed)
    valid_shape = (devices, slot_rows, 128)
    feat_shape = (gx_n, gy_n, part_rows, rows)
    block_shape = (CHUNKS, gx_n, gy_n, part_rows, width)
    new_fields, summed, source, hidden, error, slope = pl.pallas_call(
        functools.partial(step_kernel, gx_n, gy_n),
        out_shape=[
            jax.ShapeDtypeStruct(fields.shape, f32),
            jax.ShapeDtypeStruct(block_shape, bf16),
            jax.ShapeDtypeStruct((embed, slots), bf16),
            jax.ShapeDtypeStruct((hidden_n, slots), bf16),
            jax.ShapeDtypeStruct((slots, embed), bf16),
            jax.ShapeDtypeStruct((slots, hidden_n), bf16),
        ],
        in_specs=[anywhere] * 8,
        out_specs=[anywhere] * 6,
        scratch_shapes=[
            vmem(padded, f32),
            vmem(padded, f32),
            vmem(padded, f32),
            vmem(fields.shape, f32),
            vmem(block_shape, bf16),
            vmem((1, blocks), jnp.int32),
            vmem(lag_index.shape, jnp.int32),
            vmem(b_in.shape, f32),
            vmem(b_out.shape, f32),
            vmem(valid_shape, bf16),
            vmem(valid_shape, bf16),
            vmem(sides, bf16),
            vmem(sides, bf16),
            vmem(faces, FACE_TYPE),
            vmem(faces, FACE_TYPE),
            vmem((columns * size_z, PATCH * rows), bf16),
            vmem((features // PATCH, columns * size_z), bf16),
            vmem((features, rows), f32),
            vmem((features, rows), f32),
            vmem((slots, rows), bf16),
            vmem((features, embed), bf16),
            vmem((embed, hidden_n), bf16),
            vmem((hidden_n, embed), bf16),
            vmem(source_shape, bf16),
            vmem(source_shape, bf16),
            vmem(source_shape, bf16),
            vmem(source_shape, bf16),
            vmem(feat_shape, bf16),
            vmem(feat_shape, bf16),
            vmem((slots, embed), bf16),
            vmem((embed, slots), bf16),
            vmem((hidden_n, slots), bf16),
            vmem((slots, hidden_n), f32),
            vmem((slots, embed), bf16),
            vmem((slots, hidden_n), bf16),
            vmem((BACK_CHUNKS, devices, slot_rows, embed // BACK_CHUNKS), bf16),
            vmem((BACK_CHUNKS, devices, slot_rows, embed // BACK_CHUNKS), bf16),
            vmem((CHUNKS, gx_n, rows, width), bf16),
            vmem((CHUNKS, gy_n, part_rows, width), bf16),
            vmem((CHUNKS, gy_n, part_rows, width), bf16),
            dma((8,)),
            dma((5 + CHUNKS,)),
            dma((2,)),
            dma((STEPS, 4)),
            dma((STEPS, 4)),
            dma((2,)),
            dma((2,)),
            dma((gx_n,)),
            dma((gx_n,)),
            dma((BACK_CHUNKS, 2)),
            dma((CHUNKS, 2 * chips)),
            dma((CHUNKS, gx_n)),
            dma((CHUNKS, gy_n)),
            dma((CHUNKS, gy_n)),
            dma((CHUNKS, gy_n)),
            dma((CHUNKS, gy_n, chips)),
            dma((CHUNKS, gy_n, chips)),
            dma((CHUNKS, gx_n, gy_n)),
        ],
        compiler_params=pltpu.CompilerParams(
            collective_id=0, has_side_effects=True, vmem_limit_bytes=62 * 1024 * 1024
        ),
    )(fields, patch_weight, trainer_of.T, lag_index, w_in, b_in, w_out, b_out)
    first_grad, first_bias_grad, second_grad, second_bias_grad, patch_gradient = finish(
        source, hidden, error, slope, summed.reshape(CHUNKS, features, width)
    )
    return (
        new_fields,
        patch_gradient,
        first_grad,
        first_bias_grad,
        second_grad,
        second_bias_grad,
    )


def solution(mesh):
    in_specs = (
        P(None, "gx", "gy", None),
        P(),
        P(("gx", "gy"), None),
        P("gx", "gy", None),
        P(("gx", "gy"), None, None),
        P(("gx", "gy"), None),
        P(("gx", "gy"), None, None),
        P(("gx", "gy"), None),
    )
    out_specs = (
        P(None, "gx", "gy", None),
        P(),
        P(("gx", "gy"), None, None),
        P(("gx", "gy"), None),
        P(("gx", "gy"), None, None),
        P(("gx", "gy"), None),
    )
    return jax.shard_map(
        per_device, mesh=mesh, in_specs=in_specs, out_specs=out_specs, check_vma=False
    )
```
